128 devices in a mesh: pipe: 2 (over core), dp: 16 (over x, z), mp: 4 (over y).
Axes of the slice: x: 4, y: 4, z: 4, core: 2. Of those that a mesh axis runs over, the one named last changes fastest.
Arguments:
- hidden_states: bfloat16 [64, 64, 4096], P('dp'), may hold values from -6 to 6
- up_weight: bfloat16 [2, 4096, 7168], P('pipe', 'dp', 'mp'), may hold values from -0.09375 to 0.09375
- down_weight: bfloat16 [2, 7168, 4096], P('pipe', 'mp', 'dp'), may hold values from -0.0625 to 0.0625
- layer_gain: float32 [2, 4096], P('pipe'), may hold values from 0.5 to 1.5
- final_gain: float32 [4096], replicated, may hold values from 0.5 to 1.5
- unembedding: bfloat16 [32768, 4096], P(('pipe', 'mp')), may hold values from -32 to 32
- target_ids: int32 [64, 64], P('dp'), may hold values from 0 to 32767
- response_masks: int32 [64, 64], P('dp'), may hold values from 0 to 1, as said below
- anchor_logps: float32 [64, 64], P('dp'), may hold values from -14 to -10
- pairing: int32 [16, 4], P('dp'), may hold values from 0 to 3, each once within a row
Outputs:
- token_logps: float32 [64, 64], P('dp')
- seq_logps: float32 [64], P('dp')
- pair_losses: float32 [32], P('dp')
The draws below stay inside these ranges and needn't reach their ends.
Inputs may be any that keep to these rules, and one draw needn't show every extreme that they name: response_masks is 1 on one unbroken run of at least one position per sequence, starting at or after position 8, and 0 elsewhere.
All inputs are finite; a program needn't handle non-finite values.
Results may differ from the reference program's by a relative error of at most 0.0075.
Values may be sent and summed in bfloat16 or wider, within the bound.
A program may use at most 192 MiB of HBM per device.

```python
import math
import jax
import jax.numpy as jnp
import numpy as np
from jax import lax

D = 4096
VOCAB = 32768
FF = 7168
LEN = 64
SEQ_DEV = 4
SEQ_MB = 1
MICRO = 4
GROUPS = 16
SEQS = 64
PAIRS = 32
SECTIONS = 2


def draw_unembedding(key, part):
    values = jax.random.normal(key, (VOCAB, D), jnp.float32) * (2.0 * D ** (-0.5))
    values = jnp.clip(values, -12.0 * D ** (-0.5), 12.0 * D ** (-0.5))
    return values.astype(jnp.bfloat16)


def draw_response_masks(key, part):
    first_key, second_key = jax.random.split(key)
    starts = jax.random.randint(first_key, (SEQS, 1), LEN // 8, LEN // 2)
    spread = jax.random.randint(second_key, (SEQS, 1), 0, 1 << 20)
    spans = 1 + spread % (LEN - starts)
    positions = jnp.arange(LEN, dtype=jnp.int32)[None, :]
    return ((positions >= starts) & (positions < starts + spans)).astype(jnp.int32)


def set_ends(array, key, low, largest):
    spot = [jax.random.randint(jax.random.fold_in(key, axis), (), 0, length) for axis, length in enumerate(array.shape)]
    main_axis = array.shape.index(max(array.shape))
    next_to = spot[:main_axis] + [(spot[main_axis] + 1) % array.shape[main_axis]] + spot[main_axis + 1:]
    return array.at[tuple(spot)].set(low).at[tuple(next_to)].set(largest)


def steps_of(key, dims, cuts, low, largest):
    def one(axis_at, parts):
        heights = jax.random.uniform(jax.random.fold_in(jax.random.fold_in(key, 6), axis_at), (parts,), jnp.float32, low / len(cuts), largest / len(cuts))
        return jnp.repeat(jnp.exp(heights), dims[axis_at] // parts).reshape((-1,) + (1,) * (len(dims) - axis_at - 1))

    gain = one(*cuts[0])
    for cut in cuts[1:]:
        gain = gain * one(*cut)
    return gain


def rank_table(count, lean):
    portions = [(1 << 20) // math.isqrt(grade ** lean) + 1 for grade in range(1, count + 1)]
    scale = 1 + sum(portions) // (1 << 30)
    return np.cumsum(np.array([max(1, weight // scale) for weight in portions]))


def ranked_ids(rng, dims, amount, skew):
    table = rank_table(amount, skew)
    lot = jax.random.randint(jax.random.fold_in(rng, 1), dims, 0, int(table[amount - 1]))
    standing = jnp.searchsorted(jnp.asarray(table, jnp.int32), lot, side="right")
    return jax.random.permutation(jax.random.fold_in(rng, 2), amount)[standing].astype(jnp.int32)


def normal_values(own_key, dims, width, most, shards=(), kind=jnp.bfloat16):
    values = jax.random.normal(own_key, dims, jnp.float32) * width
    if len(shards) > 0:
        values = steps_of(own_key, dims, shards, -0.22, 0.18) * values
    return jnp.clip(values, min=-most, max=most).astype(kind)


def setup_inputs(seed: int = 0) -> dict:
    key_list = jax.random.split(jax.random.key(seed), 11)
    hidden_states = normal_values(key_list[0], (SEQS, LEN, D), 1.0, 6.0, ((0, 16),))
    up_weight = normal_values(key_list[1], (SECTIONS, D, FF), D ** -0.5, 0.09375, ((0, 2), (1, 16), (2, 4)))
    down_weight = normal_values(key_list[2], (SECTIONS, FF, D), FF ** -0.5, 0.0625, ((0, 2), (1, 4), (2, 16)))
    layer_gain = jnp.clip(1.0 + 0.1 * jax.random.normal(key_list[3], (SECTIONS, D), jnp.float32), 0.5, 1.5)
    final_gain = jnp.clip(1.0 + 0.1 * jax.random.normal(key_list[4], (D,), jnp.float32), 0.5, 1.5)
    unembedding = draw_unembedding(jax.random.fold_in(key_list[10], 71), 0)
    target_ids = set_ends(ranked_ids(key_list[6], (SEQS, LEN), VOCAB, 2), jax.random.fold_in(key_list[6], 3), 0, VOCAB - 1).astype(jnp.int32)
    response_masks = draw_response_masks(jax.random.fold_in(key_list[10], 71), 0)
    anchor_logps = jnp.clip(-14.0 + 4.0 * jax.random.uniform(key_list[8], (SEQS, LEN), jnp.float32) ** steps_of(key_list[8], (SEQS, LEN), ((0, 16),), -0.2, 0.2), -14.0, -10.0)
    pairing = jax.vmap(lambda own: jax.random.permutation(own, SEQ_DEV))(jax.random.split(key_list[9], GROUPS)).reshape((GROUPS, SEQ_DEV)).astype(jnp.int32)
    return dict(hidden_states=hidden_states, up_weight=up_weight, down_weight=down_weight, layer_gain=layer_gain, final_gain=final_gain, unembedding=unembedding, target_ids=target_ids, response_masks=response_masks, anchor_logps=anchor_logps, pairing=pairing)


epsilon = 1e-05
ipo_tau = 0.5

def rms_scale(values, gain_row):
    mean_square = lax.optimization_barrier(jnp.mean(values * values, axis=-1, keepdims=True))
    return values * lax.rsqrt(mean_square + epsilon) * gain_row.astype(jnp.float32)

def section_layer(states, gain_row, up_matrix, down_matrix):
    wide_states = states.astype(jnp.float32)
    normed = rms_scale(wide_states, gain_row).astype(jnp.bfloat16)
    active = jax.nn.silu(jnp.dot(normed, up_matrix, preferred_element_type=jnp.float32)).astype(jnp.bfloat16)
    summed = wide_states + jnp.dot(active, down_matrix, preferred_element_type=jnp.float32)
    return summed.astype(jnp.bfloat16)

def token_scores(finals, final_gain, unembedding, wanted_ids):
    normed = rms_scale(finals.astype(jnp.float32), final_gain).astype(jnp.bfloat16)
    logits = jnp.dot(normed, unembedding.T, preferred_element_type=jnp.float32)
    top_value = lax.optimization_barrier(jnp.max(logits, axis=1, keepdims=True))
    log_total = top_value[:, 0] + jnp.log(lax.optimization_barrier(jnp.sum(jnp.exp(logits - top_value), axis=1)))
    picked = jnp.take_along_axis(logits, wanted_ids[:, None], axis=1)[:, 0]
    return picked - log_total

def reference(hidden_states, up_weight, down_weight, layer_gain, final_gain, unembedding, target_ids, response_masks, anchor_logps, pairing):

    def one_group(group_items):
        states, wanted_ids = group_items
        flat_states = states.reshape(SEQ_DEV * LEN, D)
        for section_index in range(SECTIONS):
            flat_states = section_layer(flat_states, layer_gain[section_index], up_weight[section_index], down_weight[section_index])
        return token_scores(flat_states, final_gain, unembedding, wanted_ids.reshape(SEQ_DEV * LEN)).reshape(SEQ_DEV, LEN)
    token_logps = lax.map(one_group, (hidden_states.reshape(GROUPS, SEQ_DEV, LEN, D), target_ids.reshape(GROUPS, SEQ_DEV, LEN)))
    token_logps = token_logps.reshape(SEQS, LEN)
    mask_values = response_masks.astype(jnp.float32)
    counts = lax.optimization_barrier(jnp.sum(mask_values.reshape(GROUPS, MICRO, SEQ_MB * LEN), axis=(0, 2)))
    mean_length = counts / (GROUPS * SEQ_MB)
    divisor = jnp.tile(jnp.repeat(mean_length, SEQ_MB), GROUPS)
    policy = lax.optimization_barrier(jnp.sum(mask_values * token_logps, axis=1)) / divisor
    anchor = lax.optimization_barrier(jnp.sum(mask_values * anchor_logps, axis=1)) / divisor
    log_gaps = (policy - anchor).reshape(GROUPS, SEQ_DEV)
    chosen = jnp.take_along_axis(log_gaps, pairing[:, 0::2], axis=1)
    rejected = jnp.take_along_axis(log_gaps, pairing[:, 1::2], axis=1)
    losses = (chosen - rejected - 0.5 / ipo_tau) ** 2
    return (token_logps, policy, losses.reshape(PAIRS))
```

```python
import jax
import jax.numpy as jnp
from jax import lax
from jax.experimental import pallas as pl
from jax.experimental.pallas import tpu as pltpu
from jax.sharding import PartitionSpec as P

epsilon = 1e-05
ipo_tau = 0.5

NX, NY, NZ = 4, 4, 4
D = 4096
FF_DEV = 1792
BLK = 256
TILE_D = 4 * BLK
NH = 2
CHUNKS = ((0, 256), (256, 512), (768, 512), (1280, 512))
NC = len(CHUNKS)
UROWS = 512
NSLOT = 6
V_DEV = 4096
NU = V_DEV // UROWS
NSEM = 480

f32 = jnp.float32
bf16 = jnp.bfloat16


def body(
    hs, up, down, lgain, fgain, unemb, ids, mask,
    o_tok, o_cnt,
    wu, wd, xt, xg, pp, rz1, rz2, ag, yacc, yp, ry1, ry2, sh, xf, xn, ub,
    ssb, ssr, rcol, st, cx, cz, m_s, s_s, k_s,
    sems, usem, gate,
):
    p = lax.axis_index("pipe")
    dp = lax.axis_index("dp")
    y = lax.axis_index("mp")
    x = lax.div(dp, 4)
    z = lax.rem(dp, 4)

    def wrap(v):
        return lax.rem(v + 4, 4)

    xr = [wrap(x + d) for d in range(4)]
    yr = [wrap(y + d) for d in range(4)]
    zr = [wrap(z + d) for d in range(4)]

    def dev(pi, xi, zi, yi):
        return {"pipe": pi, "dp": xi * 4 + zi, "mp": yi}

    names = {}

    def sem(key):
        if key not in names:
            assert len(names) < NSEM
            names[key] = len(names)
        return sems.at[names[key]]

    pending = []

    def send(src, dst, key, to, cond=None):
        cp = pltpu.make_async_remote_copy(
            src_ref=src() if callable(src) else src, dst_ref=dst, send_sem=sem(("s", key)), recv_sem=sem(("r", key)),
            device_id=to, device_id_type=pl.DeviceIdType.MESH,
        )
        cp.start()
        pending.append((src, ("s", key), cond))

    def wait(dst, key):
        pltpu.make_async_copy(dst, dst, sem(("r", key))).wait()

    xp, xm, x2 = xr[1], xr[3], xr[2]
    zp, zm, z2 = zr[1], zr[3], zr[2]
    yq, ym, y2 = yr[1], yr[3], yr[2]
    other = 1 - p
    first = p == 0
    second = p == 1

    def ucopy(k):
        slot = lax.rem(k, NSLOT)
        return pltpu.make_async_copy(
            unemb.at[pl.ds(k * UROWS, UROWS)], ub.at[slot], usem.at[slot]
        )

    xrow = pl.ds(pl.multiple_of(x * BLK, BLK), BLK)
    lw = pltpu.make_async_copy(up, wu.at[xrow, :], sem("lwu"))
    lw.start()
    ld = pltpu.make_async_copy(down, wd.at[:, xrow], sem("lwd"))
    ld.start()

    cols_of = [
        [pl.ds(pl.multiple_of((xb * 4 + zr[d]) * BLK, BLK), BLK) for d in range(4)]
        for xb in range(4)
    ]

    def hcols(xb, d):
        return cols_of[xb][d]

    cx[...] = jnp.zeros_like(cx)
    cz[...] = jnp.zeros_like(cz)

    bar = pltpu.get_barrier_semaphore()
    peers = []
    for d in (1, 2, 3):
        peers.append(dev(p, xr[d], z, y))
        peers.append(dev(p, x, zr[d], y))
        peers.append(dev(p, x, z, yr[d]))
    for d in range(4):
        peers.append(dev(other, x, z, yr[d]))
    for peer in peers:
        pl.semaphore_signal(bar, inc=1, device_id=peer, device_id_type=pl.DeviceIdType.MESH)
    pl.semaphore_wait(bar, len(peers))

    items = [("u", c) for c in range(NC)] + [("d", c) for c in range(NC)]

    def own_weights(i):
        kind, c = items[i]
        o, w = CHUNKS[c]
        if kind == "u":
            src = up.at[:, pl.ds(o, w)]
            dst = wu.at[xrow, pl.ds(o, w)]
        else:
            src = down.at[pl.ds(o, w), :]
            dst = wd.at[pl.ds(o, w), xrow]
        return src, dst

    def wslice(i, xb, part=None):
        kind, c = items[i]
        o, w = CHUNKS[c]
        if kind == "u":
            n = BLK if part is None else BLK // 2
            s = xb * BLK + (0 if part is None else part * (BLK // 2))
            return wu.at[pl.ds(pl.multiple_of(s, n), n), pl.ds(o, w)]
        n = w if part is None else w // 2
        s = o + (0 if part is None else part * (w // 2))
        return wd.at[pl.ds(s, n), pl.ds(pl.multiple_of(xb * BLK, BLK), BLK)]

    def weights_own(i, cond=None):
        _, dst = own_weights(i)
        src = lambda: own_weights(i)[0]
        if cond is None:
            src = src()
        send(src, dst, ("w", i, 0), dev(p, xp, z, y), cond)
        send(src, dst, ("w", i, 1), dev(p, xm, z, y), cond)

    def weights_forward(i):
        a = wslice(i, xm)
        wait(a, ("w", i, 0))
        h = wslice(i, xm, 0)
        send(h, h, ("w", i, 2), dev(p, xp, z, y))
        b = wslice(i, xp)
        wait(b, ("w", i, 1))
        h = wslice(i, xp, 1)
        send(h, h, ("w", i, 3), dev(p, xm, z, y))
        if i + 2 < len(items):
            weights_own(i + 2)
        if i == len(items) - 3:
            @pl.when(first)
            def _():
                pl.semaphore_signal(gate, inc=1, device_id=dev(1, x, z, y),
                                    device_id_type=pl.DeviceIdType.MESH)

    def weights_last(i):
        wait(wslice(i, x2, 0), ("w", i, 2))
        wait(wslice(i, x2, 1), ("w", i, 3))

    @pl.when(first)
    def _():
        weights_own(0, first)
        weights_own(1, first)
        for h in range(NH):
            for d in (1, 3, 2):
                zt = zr[d]
                for xb in range(4):
                    send(
                        lambda h=h, d=d, xb=xb: hs.at[h, :, :, hcols(xb, d)],
                        xt.at[h, :, z, :, pl.ds(xb * BLK, BLK)],
                        ("x", h, d, xb), dev(0, x, zt, y), first,
                    )
            for xb in range(4):
                pltpu.make_async_copy(
                    hs.at[h, :, :, hcols(xb, 0)], xt.at[h, :, z, :, pl.ds(xb * BLK, BLK)],
                    sem(("xl", h, xb)),
                ).start()

    for k in range(NSLOT):
        ucopy(k).start()

    own = jnp.sum(mask[...].astype(f32), axis=1, keepdims=True)
    cx[x, 0:4, :] = jnp.broadcast_to(own, (4, 128))
    for d in (1, 2, 3):
        send(cx.at[x], cx.at[x], ("cx", d), dev(p, xr[d], z, y))

    @pl.when(second)
    def _():
        pl.semaphore_wait(gate, 1)
        weights_own(0, second)
        weights_own(1, second)

    gz = jnp.concatenate([lgain[:, hcols(xb, 0)] for xb in range(4)], axis=1)

    def tile_arrived(h):
        @pl.when(first)
        def _():
            for xb in range(4):
                pltpu.make_async_copy(
                    hs.at[h, :, :, hcols(xb, 0)], xt.at[h, :, z, :, pl.ds(xb * BLK, BLK)],
                    sem(("xl", h, xb)),
                ).wait()
            for d in (1, 3, 2):
                zs = zr[(4 - d) % 4]
                for xb in range(4):
                    wait(xt.at[h, :, zs, :, pl.ds(xb * BLK, BLK)], ("x", h, d, xb))

        @pl.when(second)
        def _():
            wait(xt.at[h, ym], ("g", h, 0))
            a = lambda: xt.at[h, ym, 0:2]
            send(a, a(), ("g", h, 3), dev(1, x, z, yq), second)
            wait(xt.at[h, yq], ("g", h, 1))
            b = lambda: xt.at[h, yq, 2:4]
            send(b, b(), ("g", h, 4), dev(1, x, z, ym), second)
            wait(xt.at[h, y], ("g", h, 2))
            wait(xt.at[h, y2, 0:2], ("g", h, 3))
            wait(xt.at[h, y2, 2:4], ("g", h, 4))

    def tile_ready(h):
        tile_arrived(h)
        ones = jnp.ones((8, TILE_D), bf16)
        for g in range(4):
            v = xt[h, :, g].reshape(128, TILE_D).astype(f32)
            xg[h, :, g] = (v * gz).astype(bf16).reshape(4, 32, TILE_D)
            sq = v * v
            hi = sq.astype(bf16)
            lo = (sq - hi.astype(f32)).astype(bf16)
            dn = (((1,), (1,)), ((), ()))
            ssb[h, g] = lax.dot_general(
                ones, hi, dn, preferred_element_type=f32
            ) + lax.dot_general(ones, lo, dn, preferred_element_type=f32)
        for d in (1, 3, 2):
            zt = zr[d]
            send(ssb.at[h, zt], ssr.at[h, d - 1], ("ss", h, d), dev(p, x, zt, y))

    def row_scale(h):
        for d in (1, 3, 2):
            wait(ssr.at[h, d - 1], ("ss", h, d))
        total = ssb[h, z] + ssr[h, 0] + ssr[h, 1] + ssr[h, 2]
        scale = lax.rsqrt(total * (1.0 / D) + epsilon)
        col = jnp.transpose(scale, (1, 0))[:, 0:1]
        rcol[h] = jnp.broadcast_to(col, (128, 128))

    def up_chunk(h, c):
        o, w = CHUNKS[c]
        lhs = xg[h].reshape(512, TILE_D)
        for n in range(o, o + w, 256):
            r = jnp.dot(lhs, wu[:, n : n + 256], preferred_element_type=f32)
            pp[h, :, :, :, n : n + 256] = r.astype(bf16).reshape(4, 4, 32, 256)
        cs = pl.ds(o, w)
        send(pp.at[h, 0:2, z2, :, cs], rz1.at[h, 0, :, :, cs], ("z1", h, c, 0), dev(p, x, zp, y))
        send(pp.at[h, 2:4, z2, :, cs], rz1.at[h, 1, :, :, cs], ("z1", h, c, 1), dev(p, x, zm, y))
        send(pp.at[h, 2:4, zp, :, cs], rz2.at[h, 0, 2:4, :, cs], ("z2", h, c, 0), dev(p, x, zp, y))
        send(pp.at[h, 0:2, zm, :, cs], rz2.at[h, 1, 0:2, :, cs], ("z2", h, c, 1), dev(p, x, zm, y))

    def reduce_one(h, c):
        o, w = CHUNKS[c]
        cs = pl.ds(o, w)
        wait(rz1.at[h, 0, :, :, cs], ("z1", h, c, 0))
        pp[h, 0:2, zp, :, cs] = (
            pp[h, 0:2, zp, :, cs].astype(f32) + rz1[h, 0, :, :, cs].astype(f32)
        ).astype(bf16)
        send(pp.at[h, 0:2, zp, :, cs], rz2.at[h, 0, 0:2, :, cs], ("z2", h, c, 2), dev(p, x, zp, y))
        wait(rz1.at[h, 1, :, :, cs], ("z1", h, c, 1))
        pp[h, 2:4, zm, :, cs] = (
            pp[h, 2:4, zm, :, cs].astype(f32) + rz1[h, 1, :, :, cs].astype(f32)
        ).astype(bf16)
        send(pp.at[h, 2:4, zm, :, cs], rz2.at[h, 1, 2:4, :, cs], ("z2", h, c, 3), dev(p, x, zm, y))

    def reduce_two(h, c):
        o, w = CHUNKS[c]
        cs = pl.ds(o, w)
        if c == 0:
            row_scale(h)
        wait(rz2.at[h, 0, 2:4, :, cs], ("z2", h, c, 0))
        wait(rz2.at[h, 1, 0:2, :, cs], ("z2", h, c, 1))
        wait(rz2.at[h, 0, 0:2, :, cs], ("z2", h, c, 2))
        wait(rz2.at[h, 1, 2:4, :, cs], ("z2", h, c, 3))
        s = (
            pp[h, :, z, :, cs].astype(f32)
            + rz2[h, 0, :, :, cs].astype(f32)
            + rz2[h, 1, :, :, cs].astype(f32)
        ).reshape(128, w)
        v = s * rcol[h][:, 0:1]
        act = v / (1.0 + jnp.exp(-v))
        ag[h, :, z, :, cs] = act.astype(bf16).reshape(4, 32, w)
        a = ag.at[h, :, z, :, cs]
        send(a, a, ("a", h, c, 0), dev(p, x, zp, y))
        send(a, a, ("a", h, c, 1), dev(p, x, zm, y))

    def gather_one(h, c):
        o, w = CHUNKS[c]
        cs = pl.ds(o, w)
        wait(ag.at[h, :, zm, :, cs], ("a", h, c, 0))
        a = ag.at[h, 0:2, zm, :, cs]
        send(a, a, ("a", h, c, 2), dev(p, x, zp, y))
        wait(ag.at[h, :, zp, :, cs], ("a", h, c, 1))
        b = ag.at[h, 2:4, zp, :, cs]
        send(b, b, ("a", h, c, 3), dev(p, x, zm, y))

    def down_chunk(h, c):
        o, w = CHUNKS[c]
        cs = pl.ds(o, w)
        wait(ag.at[h, 0:2, z2, :, cs], ("a", h, c, 2))
        wait(ag.at[h, 2:4, z2, :, cs], ("a", h, c, 3))
        lhs = ag[h, :, :, :, cs].reshape(512, w)
        for n in range(0, TILE_D, 256):
            r = jnp.dot(lhs, wd[cs, n : n + 256], preferred_element_type=f32)
            if c > 0:
                r = r + yacc[:, n : n + 256]
            if c == NC - 1:
                yp[h, :, :, :, n : n + 256] = r.astype(bf16).reshape(4, 4, 32, 256)
            else:
                yacc[:, n : n + 256] = r

    def y_start(h):
        send(yp.at[h, y2, 0:2], ry1.at[h, 0], ("y1", h, 0), dev(p, x, z, yq))
        send(yp.at[h, y2, 2:4], ry1.at[h, 1], ("y1", h, 1), dev(p, x, z, ym))
        send(yp.at[h, yq, 2:4], ry2.at[h, 0, 2:4], ("y2", h, 0), dev(p, x, z, yq))
        send(yp.at[h, ym, 0:2], ry2.at[h, 1, 0:2], ("y2", h, 1), dev(p, x, z, ym))

    def y_mid(h):
        wait(ry1.at[h, 0], ("y1", h, 0))
        yp[h, yq, 0:2] = (yp[h, yq, 0:2].astype(f32) + ry1[h, 0].astype(f32)).astype(bf16)
        send(yp.at[h, yq, 0:2], ry2.at[h, 0, 0:2], ("y2", h, 2), dev(p, x, z, yq))
        wait(ry1.at[h, 1], ("y1", h, 1))
        yp[h, ym, 2:4] = (yp[h, ym, 2:4].astype(f32) + ry1[h, 1].astype(f32)).astype(bf16)
        send(yp.at[h, ym, 2:4], ry2.at[h, 1, 2:4], ("y2", h, 3), dev(p, x, z, ym))

    def y_end(h):
        wait(ry2.at[h, 0, 2:4], ("y2", h, 0))
        wait(ry2.at[h, 1, 0:2], ("y2", h, 1))
        wait(ry2.at[h, 0, 0:2], ("y2", h, 2))
        wait(ry2.at[h, 1, 2:4], ("y2", h, 3))
        sh[h] = (
            xt[h, y].astype(f32) + yp[h, y].astype(f32) + ry2[h, 0].astype(f32) + ry2[h, 1].astype(f32)
        ).astype(bf16)

        @pl.when(first)
        def _():
            dst = xt.at[h, y]
            send(lambda: sh.at[h], dst, ("g", h, 0), dev(1, x, z, yq), first)
            send(lambda: sh.at[h], dst, ("g", h, 1), dev(1, x, z, ym), first)
            send(lambda: sh.at[h], dst, ("g", h, 2), dev(1, x, z, y), first)

        @pl.when(second)
        def _():
            for d in (1, 3, 2):
                zt = zr[d]
                for xb in range(4):
                    send(
                        lambda d=d, xb=xb: sh.at[h, zr[d], :, pl.ds(xb * BLK, BLK)],
                        xf.at[h, y, :, hcols(xb, 0)],
                        ("f", h, d, xb), dev(1, x, zt, y), second,
                    )
            for xb in range(4):
                xf[h, y, :, hcols(xb, 0)] = sh[h, z, :, xb * BLK : (xb + 1) * BLK]

    half_d = D // 2

    def finals_one(h):
        @pl.when(second)
        def _():
            for d in (1, 3, 2):
                zs = zr[(4 - d) % 4]
                for xb in range(4):
                    wait(xf.at[h, y, :, hcols(xb, (4 - d) % 4)], ("f", h, d, xb))
            a = lambda: xf.at[h, y]
            send(a, a(), ("q", h, 0), dev(1, x, z, yq), second)
            send(a, a(), ("q", h, 1), dev(1, x, z, ym), second)
            send(a, a(), ("q", h, 4), dev(0, x, z, y), second)

    def finals_two(h):
        @pl.when(second)
        def _():
            wait(xf.at[h, ym], ("q", h, 0))
            a = lambda: xf.at[h, ym, :, pl.ds(0, half_d)]
            send(a, a(), ("q", h, 2), dev(1, x, z, yq), second)
            wait(xf.at[h, yq], ("q", h, 1))
            b = lambda: xf.at[h, yq, :, pl.ds(half_d, half_d)]
            send(b, b(), ("q", h, 3), dev(1, x, z, ym), second)
            e = lambda: xf.at[h, ym]
            send(e, e(), ("q", h, 5), dev(0, x, z, y), second)
            f = lambda: xf.at[h, yq]
            send(f, f(), ("q", h, 6), dev(0, x, z, y), second)

    def finals_three(h):
        @pl.when(second)
        def _():
            wait(xf.at[h, y2, :, pl.ds(0, half_d)], ("q", h, 2))
            wait(xf.at[h, y2, :, pl.ds(half_d, half_d)], ("q", h, 3))
            a = lambda: xf.at[h, y2]
            send(a, a(), ("q", h, 7), dev(0, x, z, y), second)

        @pl.when(first)
        def _():
            wait(xf.at[h, y], ("q", h, 4))
            wait(xf.at[h, ym], ("q", h, 5))
            wait(xf.at[h, yq], ("q", h, 6))
            wait(xf.at[h, y2], ("q", h, 7))

    def final_norm(h):
        for q in range(4):
            v = xf[h, q].astype(f32)
            r = lax.rsqrt(jnp.mean(v * v, axis=1, keepdims=True) + epsilon)
            xn[pl.ds(h * 128 + q * 32, 32), :] = (v * r * fgain[...]).astype(bf16)

    steps = [(h, c) for h in range(NH) for c in range(NC)]
    lw.wait()
    ld.wait()

    def y_tail(h, stage):
        if stage == 0:
            y_start(h)
        elif stage == 1:
            y_mid(h)
        else:
            y_end(h)

    n = len(steps)
    y_events = {}
    for i in range(n + NC + 8):
        if i < len(items):
            weights_forward(i)
        if i - 1 >= 0 and i - 1 < n:
            reduce_one(*steps[i - 1])
        if i - 2 >= 0 and i - 2 < n:
            reduce_two(*steps[i - 2])
        if i - 3 >= 0 and i - 3 < n:
            gather_one(*steps[i - 3])
        if i < n:
            h, c = steps[i]
            if h == 0:
                weights_last(i)
            if c == 0:
                tile_ready(h)
            up_chunk(h, c)
        j = i - NC - 1
        if 0 <= j < n:
            h, c = steps[j]
            if h == 0:
                weights_last(NC + c)
            down_chunk(h, c)
            if c == NC - 1:
                y_start(h)
                y_events.setdefault(i + 1, []).append((y_mid, h))
                y_events.setdefault(i + 2, []).append((y_end, h))
                y_events.setdefault(i + 3, []).append((finals_one, h))
        for f, h in y_events.pop(i, []):
            f(h)
    assert not y_events
    for h in range(NH):
        finals_two(h)
        finals_three(h)
        final_norm(h)

    for d in (1, 2, 3):
        wait(cx.at[xr[(4 - d) % 4]], ("cx", d))
    cz[z] = cx[0] + cx[1] + cx[2] + cx[3]
    for d in (1, 2, 3):
        send(cz.at[z], cz.at[z], ("cz", d), dev(p, x, zr[d], y))

    m_s[...] = jnp.full_like(m_s, -jnp.inf)
    s_s[...] = jnp.zeros_like(s_s)
    k_s[...] = jnp.zeros_like(k_s)
    vocab_index = p * 4 + y

    def head(k, carry):
        slot = lax.rem(k, NSLOT)
        ucopy(k).wait()
        lt = lax.dot_general(
            ub[slot], xn[...], (((1,), (1,)), ((), ())), preferred_element_type=f32
        )
        m_old = m_s[0:1, :]
        m_new = jnp.maximum(m_old, jnp.max(lt, axis=0, keepdims=True))
        rows = lax.broadcasted_iota(jnp.int32, lt.shape, 0) + (vocab_index * V_DEV + k * UROWS)
        k_s[0:1, :] = k_s[0:1, :] + jnp.sum(
            jnp.where(rows == ids[...], lt, 0.0), axis=0, keepdims=True
        )
        s_s[0:1, :] = s_s[0:1, :] * jnp.exp(m_old - m_new) + jnp.sum(
            jnp.exp(lt - m_new), axis=0, keepdims=True
        )
        m_s[0:1, :] = m_new

        @pl.when(k + NSLOT < NU)
        def _():
            ucopy(k + NSLOT).start()

        return carry

    lax.fori_loop(0, NU, head, 0)

    st[vocab_index, 0:8] = m_s[...]
    st[vocab_index, 8:16] = s_s[...]
    st[vocab_index, 16:24] = k_s[...]
    mine = st.at[vocab_index]
    for d in range(4):
        yt = yr[d]
        if d > 0:
            send(mine, mine, ("st", 0, d), dev(p, x, z, yt))
        send(mine, mine, ("st", 1, d), dev(other, x, z, yt))
    for d in range(4):
        ys = yr[(4 - d) % 4]
        if d > 0:
            wait(st.at[p * 4 + ys], ("st", 0, d))
        wait(st.at[other * 4 + ys], ("st", 1, d))
    ms = [st[i, 0:8] for i in range(8)]
    top = ms[0]
    for i in range(1, 8):
        top = jnp.maximum(top, ms[i])
    tot = jnp.zeros_like(top)
    pick = jnp.zeros_like(top)
    for i in range(8):
        tot = tot + st[i, 8:16] * jnp.exp(ms[i] - top)
        pick = pick + st[i, 16:24]
    o_tok[...] = pick - top - jnp.log(tot)

    for d in (1, 2, 3):
        wait(cz.at[zr[(4 - d) % 4]], ("cz", d))
    o_cnt[...] = cz[0] + cz[1] + cz[2] + cz[3]

    for src, ssem, cond in pending:
        if cond is None:
            pltpu.make_async_copy(src, src, sem(ssem)).wait()
    for which in (first, second):
        @pl.when(which)
        def _():
            for src, ssem, cond in pending:
                if cond is which:
                    ref = src()
                    pltpu.make_async_copy(ref, ref, sem(ssem)).wait()


def run(hs, up, down, lgain, fgain, unemb, ids, mask):
    anyspace = pl.BlockSpec(memory_space=pltpu.HBM)
    vm = pl.BlockSpec(memory_space=pltpu.VMEM)
    V = pltpu.VMEM
    return pl.pallas_call(
        body,
        out_shape=(
            jax.ShapeDtypeStruct((8, 256), f32),
            jax.ShapeDtypeStruct((8, 128), f32),
        ),
        in_specs=[anyspace, anyspace, anyspace, vm, vm, anyspace, vm, vm],
        out_specs=(vm, vm),
        scratch_shapes=[
            V((TILE_D, FF_DEV), bf16),
            V((FF_DEV, TILE_D), bf16),
            V((NH, 4, 4, 32, TILE_D), bf16),
            V((NH, 4, 4, 32, TILE_D), bf16),
            V((NH, 4, 4, 32, FF_DEV), bf16),
            V((NH, 2, 2, 32, FF_DEV), bf16),
            V((NH, 2, 4, 32, FF_DEV), bf16),
            V((NH, 4, 4, 32, FF_DEV), bf16),
            V((512, TILE_D), f32),
            V((NH, 4, 4, 32, TILE_D), bf16),
            V((NH, 2, 2, 32, TILE_D), bf16),
            V((NH, 2, 4, 32, TILE_D), bf16),
            V((NH, 4, 32, TILE_D), bf16),
            V((NH, 4, 32, D), bf16),
            V((256, D), bf16),
            V((NSLOT, UROWS, D), bf16),
            V((NH, 4, 8, 128), f32),
            V((NH, 3, 8, 128), f32),
            V((NH, 128, 128), f32),
            V((8, 24, 256), f32),
            V((4, 8, 128), f32),
            V((4, 8, 128), f32),
            V((8, 256), f32),
            V((8, 256), f32),
            V((8, 256), f32),
            pltpu.SemaphoreType.DMA((NSEM,)),
            pltpu.SemaphoreType.DMA((NSLOT,)),
            pltpu.SemaphoreType.REGULAR,
        ],
        compiler_params=pltpu.CompilerParams(
            collective_id=0, has_side_effects=True, vmem_limit_bytes=66_000_000
        ),
        name="relay",
    )(hs, up, down, lgain, fgain, unemb, ids, mask)


def shards(
    hidden_states, up_weight, down_weight, layer_gain, final_gain, unembedding,
    target_ids, response_masks, anchor_logps, pairing,
):
    tok, cnt = run(
        hidden_states.reshape(NH, 4, 32, D),
        up_weight[0],
        down_weight[0],
        layer_gain,
        final_gain.reshape(1, D),
        unembedding,
        target_ids.reshape(1, 256),
        response_masks,
    )
    token_logps = tok[0].reshape(4, 64)
    counts = cnt[0:4, 0]
    mask_values = response_masks.astype(f32)
    divisor = counts / 16.0
    policy = jnp.sum(mask_values * token_logps, axis=1) / divisor
    anchor = jnp.sum(mask_values * anchor_logps, axis=1) / divisor
    log_gaps = policy - anchor
    positions = jnp.arange(4, dtype=jnp.int32)
    chosen = jnp.sum(
        jnp.where(pairing[0, 0::2][:, None] == positions[None, :], log_gaps[None, :], 0.0), axis=1
    )
    rejected = jnp.sum(
        jnp.where(pairing[0, 1::2][:, None] == positions[None, :], log_gaps[None, :], 0.0), axis=1
    )
    losses = (chosen - rejected - 0.5 / ipo_tau) ** 2
    return (token_logps, policy, losses)


def solution(mesh):
    return jax.shard_map(
        shards,
        mesh=mesh,
        in_specs=(
            P("dp", None, None),
            P("pipe", "dp", "mp"),
            P("pipe", "mp", "dp"),
            P("pipe", None),
            P(),
            P(("pipe", "mp"), None),
            P("dp", None),
            P("dp", None),
            P("dp", None),
            P("dp", None),
        ),
        out_specs=(P("dp", None), P("dp"), P("dp")),
        check_vma=False,
    )
```

```python
import jax
import jax.numpy as jnp
from jax import lax
from jax.experimental import pallas as pl
from jax.experimental.pallas import tpu as pltpu
from jax.sharding import PartitionSpec as P

epsilon = 1e-05
ipo_tau = 0.5

NX, NY, NZ = 4, 4, 4
D = 4096
FF_DEV = 1792
BLK = 256
TILE_D = 4 * BLK
NH = 4
R = 32 // (NH // 2)
AHEAD = 2
WF_SLOT = (-1, 0, 2, 4, 6, 8, 10, 12)
GATE = 0
PRE = 4
CHUNKS = ((0, 256), (256, 512), (768, 512), (1280, 512))
LAG = 2
NC = len(CHUNKS)
UROWS = 512
NSLOT = 6
V_DEV = 4096
NU = V_DEV // UROWS
NS = 1
SUB = TILE_D // NS
XB = 4 // NS
NSEM = 1200

f32 = jnp.float32
bf16 = jnp.bfloat16


def body(
    hs, up, down, lgain, fgain, unemb, ids, mask,
    o_tok, o_cnt,
    wu, wd, xt, xg, pp, rz1, rz2, ag, yacc, yp, ry1, ry2, sh, xf, xn, ub,
    ssb, ssr, rcol, st, cx, cz, m_s, s_s, k_s,
    sems, usem, gate,
):
    p = lax.axis_index("pipe")
    dp = lax.axis_index("dp")
    y = lax.axis_index("mp")
    x = lax.div(dp, 4)
    z = lax.rem(dp, 4)

    def wrap(v):
        return lax.rem(v + 4, 4)

    xr = [wrap(x + d) for d in range(4)]
    yr = [wrap(y + d) for d in range(4)]
    zr = [wrap(z + d) for d in range(4)]

    def dev(pi, xi, zi, yi):
        return {"pipe": pi, "dp": xi * 4 + zi, "mp": yi}

    names = {}

    def sem(key):
        if key not in names:
            assert len(names) < NSEM
            names[key] = len(names)
        return sems.at[names[key]]

    pending = []

    def send(src, dst, key, to, cond=None):
        cp = pltpu.make_async_remote_copy(
            src_ref=src() if callable(src) else src, dst_ref=dst, send_sem=sem(("s", key)), recv_sem=sem(("r", key)),
            device_id=to, device_id_type=pl.DeviceIdType.MESH,
        )
        cp.start()
        pending.append((src, ("s", key), cond))

    def wait(dst, key):
        pltpu.make_async_copy(dst, dst, sem(("r", key))).wait()

    xp, xm, x2 = xr[1], xr[3], xr[2]
    zp, zm, z2 = zr[1], zr[3], zr[2]
    yq, ym, y2 = yr[1], yr[3], yr[2]
    other = 1 - p
    first = p == 0
    second = p == 1

    def ucopy(k):
        slot = lax.rem(k, NSLOT)
        return pltpu.make_async_copy(
            unemb.at[pl.ds(k * UROWS, UROWS)], ub.at[slot], usem.at[slot]
        )

    xrow = pl.ds(pl.multiple_of(x * BLK, BLK), BLK)
    lw = pltpu.make_async_copy(up, wu.at[xrow, :], sem("lwu"))
    lw.start()
    ld = pltpu.make_async_copy(down, wd.at[:, xrow], sem("lwd"))

    cols_of = [
        [pl.ds(pl.multiple_of((xb * 4 + zr[d]) * BLK, BLK), BLK) for d in range(4)]
        for xb in range(4)
    ]

    def hcols(xb, d):
        return cols_of[xb][d]

    cx[...] = jnp.zeros_like(cx)
    cz[...] = jnp.zeros_like(cz)
    ssb[...] = jnp.zeros_like(ssb)

    bar = pltpu.get_barrier_semaphore()
    peers = []
    for d in (1, 2, 3):
        peers.append(dev(p, xr[d], z, y))
        peers.append(dev(p, x, zr[d], y))
        peers.append(dev(p, x, z, yr[d]))
    for d in range(4):
        peers.append(dev(other, x, z, yr[d]))
    for peer in peers:
        pl.semaphore_signal(bar, inc=1, device_id=peer, device_id_type=pl.DeviceIdType.MESH)
    with jax.named_scope("barrier"):
        pl.semaphore_wait(bar, len(peers))

    items = [("u", c) for c in range(NC)] + [("d", c) for c in range(NC)]

    def own_weights(i):
        kind, c = items[i]
        o, w = CHUNKS[c]
        if kind == "u":
            src = up.at[:, pl.ds(o, w)]
            dst = wu.at[xrow, pl.ds(o, w)]
        else:
            src = down.at[pl.ds(o, w), :]
            dst = wd.at[pl.ds(o, w), xrow]
        return src, dst

    def wslice(i, xb, part=None):
        kind, c = items[i]
        o, w = CHUNKS[c]
        if kind == "u":
            n = BLK if part is None else BLK // 2
            s = xb * BLK + (0 if part is None else part * (BLK // 2))
            return wu.at[pl.ds(pl.multiple_of(s, n), n), pl.ds(o, w)]
        n = w if part is None else w // 2
        s = o + (0 if part is None else part * (w // 2))
        return wd.at[pl.ds(s, n), pl.ds(pl.multiple_of(xb * BLK, BLK), BLK)]

    def weights_own(i, cond=None):
        _, dst = own_weights(i)
        src = lambda: own_weights(i)[0]
        if cond is None:
            src = src()
        send(src, dst, ("w", i, 0), dev(p, xp, z, y), cond)
        send(src, dst, ("w", i, 1), dev(p, xm, z, y), cond)

    def weights_forward(i, cond):
        @pl.when(cond)
        def _():
            wait(wslice(i, xm), ("w", i, 0))
            a = lambda: wslice(i, xm, 0)
            send(a, a(), ("w", i, 2), dev(p, xp, z, y), cond)
            wait(wslice(i, xp), ("w", i, 1))
            b = lambda: wslice(i, xp, 1)
            send(b, b(), ("w", i, 3), dev(p, xm, z, y), cond)
            if cond is first and i == 0:
                for k in range(2, AHEAD):
                    weights_own(k, cond)
            if i + AHEAD < len(items):
                weights_own(i + AHEAD, cond)
            if cond is first and i == len(items) - 1 - GATE:
                pl.semaphore_signal(gate, inc=1, device_id=dev(1, x, z, y),
                                    device_id_type=pl.DeviceIdType.MESH)

    def weights_last(i):
        wait(wslice(i, x2, 0), ("w", i, 2))
        wait(wslice(i, x2, 1), ("w", i, 3))

    def far_tokens(h):
        for xb in range(4):
            send(
                lambda h=h, xb=xb: hs.at[h, y, :, hcols(xb, 2)],
                xt.at[h, y, z, :, pl.ds(xb * BLK, BLK)],
                ("x", h, 2, xb), dev(0, x, z2, y), first,
            )

    def near_tokens(h):
        for d in (1, 3):
            for xb in range(4):
                send(
                    lambda h=h, d=d, xb=xb: hs.at[h, :, :, hcols(xb, d)],
                    xt.at[h, :, z, :, pl.ds(xb * BLK, BLK)],
                    ("x", h, d, xb), dev(0, x, zr[d], y), first,
                )
        for xb in range(4):
            pltpu.make_async_copy(
                hs.at[h, :, :, hcols(xb, 0)], xt.at[h, :, z, :, pl.ds(xb * BLK, BLK)],
                sem(("xl", h, xb)),
            ).start()

    def near_later(h):
        @pl.when(first)
        def _():
            near_tokens(h)

    @pl.when(first)
    def _():
        weights_own(0, first)
        weights_own(1, first)
        for h in range(NH):
            far_tokens(h)
            if h < 2:
                near_tokens(h)

    own = jnp.sum(mask[...].astype(f32), axis=1, keepdims=True)
    cx[x, 0:4, :] = jnp.broadcast_to(own, (4, 128))
    for d in (1, 2, 3):
        send(cx.at[x], cx.at[x], ("cx", d), dev(p, xr[d], z, y))

    @pl.when(second)
    def _():
        pl.semaphore_wait(gate, 1)
        for i in range(AHEAD):
            weights_own(i, second)

    gz = jnp.concatenate([lgain[:, hcols(xb, 0)] for xb in range(4)], axis=1)

    def tile_arrived(h):
        @pl.when(first)
        def _():
            for xb in range(4):
                pltpu.make_async_copy(
                    hs.at[h, :, :, hcols(xb, 0)], xt.at[h, :, z, :, pl.ds(xb * BLK, BLK)],
                    sem(("xl", h, xb)),
                ).wait()
            for d in (1, 3):
                zs = zr[(4 - d) % 4]
                for xb in range(4):
                    wait(xt.at[h, :, zs, :, pl.ds(xb * BLK, BLK)], ("x", h, d, xb))
            for d in (1, 3, 2):
                wait(xt.at[h, yr[(4 - d) % 4], z2], ("xy", h, d))

        @pl.when(second)
        def _():
            for e in range(NS):
                es = pl.ds(e * SUB, SUB)
                wait(xt.at[h, y, :, :, es], ("g", h, e, 2))
                wait(xt.at[h, y2, 0:2, :, es], ("g", h, e, 3))
                wait(xt.at[h, y2, 2:4, :, es], ("g", h, e, 4))

    def tile_relay_first(h):
        @pl.when(first)
        def _():
            for xb in range(4):
                wait(xt.at[h, y, z2, :, pl.ds(xb * BLK, BLK)], ("x", h, 2, xb))
            a = lambda: xt.at[h, y, z2]
            for d in (1, 3, 2):
                send(a, a(), ("xy", h, d), dev(0, x, z, yr[d]), first)

    def tile_relay(h):
        @pl.when(second)
        def _():
            for e in range(NS):
                es = pl.ds(e * SUB, SUB)
                wait(xt.at[h, ym, :, :, es], ("g", h, e, 0))
                a = lambda es=es: xt.at[h, ym, 0:2, :, es]
                send(a, a(), ("g", h, e, 3), dev(1, x, z, yq), second)
                wait(xt.at[h, yq, :, :, es], ("g", h, e, 1))
                b = lambda es=es: xt.at[h, yq, 2:4, :, es]
                send(b, b(), ("g", h, e, 4), dev(1, x, z, ym), second)

    def tile_ready(h):
        tile_arrived(h)
        ones = jnp.ones((8, TILE_D), bf16)
        for g in range(4):
            v = xt[h, :, g].reshape(4 * R, TILE_D).astype(f32)
            xg[h, :, g] = (v * gz).astype(bf16).reshape(4, R, TILE_D)
            sq = v * v
            hi = sq.astype(bf16)
            lo = (sq - hi.astype(f32)).astype(bf16)
            dn = (((1,), (1,)), ((), ()))
            ssb[h, g, :, 0 : 4 * R] = lax.dot_general(
                ones, hi, dn, preferred_element_type=f32
            ) + lax.dot_general(ones, lo, dn, preferred_element_type=f32)
        for d in (1, 3, 2):
            zt = zr[d]
            send(ssb.at[h, zt], ssr.at[h, d - 1], ("ss", h, d), dev(p, x, zt, y))

    def row_scale(h):
        for d in (1, 3, 2):
            wait(ssr.at[h, d - 1], ("ss", h, d))
        total = ssb[h, z] + ssr[h, 0] + ssr[h, 1] + ssr[h, 2]
        scale = lax.rsqrt(total * (1.0 / D) + epsilon)
        col = jnp.transpose(scale, (1, 0))[0 : 4 * R, 0:1]
        rcol[h] = jnp.broadcast_to(col, (4 * R, 128))

    def up_chunk(h, c):
        o, w = CHUNKS[c]
        lhs = xg[h].reshape(16 * R, TILE_D)
        r = jnp.dot(lhs, wu[:, o : o + w], preferred_element_type=f32)
        pp[h, :, :, :, o : o + w] = r.astype(bf16).reshape(4, 4, R, w)
        cs = pl.ds(o, w)
        send(pp.at[h, 0:2, z2, :, cs], rz1.at[h, 0, :, :, cs], ("z1", h, c, 0), dev(p, x, zp, y))
        send(pp.at[h, 2:4, z2, :, cs], rz1.at[h, 1, :, :, cs], ("z1", h, c, 1), dev(p, x, zm, y))
        send(pp.at[h, 2:4, zp, :, cs], rz2.at[h, 0, 2:4, :, cs], ("z2", h, c, 0), dev(p, x, zp, y))
        send(pp.at[h, 0:2, zm, :, cs], rz2.at[h, 1, 0:2, :, cs], ("z2", h, c, 1), dev(p, x, zm, y))

    def reduce_one(h, c):
        o, w = CHUNKS[c]
        cs = pl.ds(o, w)
        wait(rz1.at[h, 0, :, :, cs], ("z1", h, c, 0))
        pp[h, 0:2, zp, :, cs] = (
            pp[h, 0:2, zp, :, cs].astype(f32) + rz1[h, 0, :, :, cs].astype(f32)
        ).astype(bf16)
        send(pp.at[h, 0:2, zp, :, cs], rz2.at[h, 0, 0:2, :, cs], ("z2", h, c, 2), dev(p, x, zp, y))
        wait(rz1.at[h, 1, :, :, cs], ("z1", h, c, 1))
        pp[h, 2:4, zm, :, cs] = (
            pp[h, 2:4, zm, :, cs].astype(f32) + rz1[h, 1, :, :, cs].astype(f32)
        ).astype(bf16)
        send(pp.at[h, 2:4, zm, :, cs], rz2.at[h, 1, 2:4, :, cs], ("z2", h, c, 3), dev(p, x, zm, y))

    def reduce_two(h, c):
        o, w = CHUNKS[c]
        cs = pl.ds(o, w)
        if c == 0:
            row_scale(h)
        wait(rz2.at[h, 0, 2:4, :, cs], ("z2", h, c, 0))
        wait(rz2.at[h, 1, 0:2, :, cs], ("z2", h, c, 1))
        wait(rz2.at[h, 0, 0:2, :, cs], ("z2", h, c, 2))
        wait(rz2.at[h, 1, 2:4, :, cs], ("z2", h, c, 3))
        s = (
            pp[h, :, z, :, cs].astype(f32)
            + rz2[h, 0, :, :, cs].astype(f32)
            + rz2[h, 1, :, :, cs].astype(f32)
        ).reshape(4 * R, w)
        v = s * rcol[h][:, 0:1]
        act = v / (1.0 + jnp.exp(-v))
        ag[h, :, z, :, cs] = act.astype(bf16).reshape(4, R, w)
        a = ag.at[h, :, z, :, cs]
        send(a, a, ("a", h, c, 0), dev(p, x, zp, y))
        send(a, a, ("a", h, c, 1), dev(p, x, zm, y))

    def gather_one(h, c):
        o, w = CHUNKS[c]
        cs = pl.ds(o, w)
        wait(ag.at[h, :, zm, :, cs], ("a", h, c, 0))
        a = ag.at[h, 0:2, zm, :, cs]
        send(a, a, ("a", h, c, 2), dev(p, x, zp, y))
        wait(ag.at[h, :, zp, :, cs], ("a", h, c, 1))
        b = ag.at[h, 2:4, zp, :, cs]
        send(b, b, ("a", h, c, 3), dev(p, x, zm, y))

    def down_arrived(h, c):
        cs = pl.ds(*CHUNKS[c])
        wait(ag.at[h, 0:2, z2, :, cs], ("a", h, c, 2))
        wait(ag.at[h, 2:4, z2, :, cs], ("a", h, c, 3))

    def down_chunk(h, c, e=None):
        o, w = CHUNKS[c]
        cs = pl.ds(o, w)
        if e is None:
            down_arrived(h, c)
        lhs = ag[h, :, :, :, cs].reshape(16 * R, w)
        for n in range(0 if e is None else e * SUB, TILE_D if e is None else (e + 1) * SUB, 256):
            r = jnp.dot(lhs, wd[cs, n : n + 256], preferred_element_type=f32)
            if c > 0:
                r = r + yacc[h, :, n : n + 256]
            if c == NC - 1:
                yp[h, :, :, :, n : n + 256] = r.astype(bf16).reshape(4, 4, R, 256)
            else:
                yacc[h, :, n : n + 256] = r

    def y_start(h, e):
        es = pl.ds(e * SUB, SUB)
        send(yp.at[h, y2, 0:2, :, es], ry1.at[h, 0, :, :, es], ("y1", h, e, 0), dev(p, x, z, yq))
        send(yp.at[h, y2, 2:4, :, es], ry1.at[h, 1, :, :, es], ("y1", h, e, 1), dev(p, x, z, ym))
        send(yp.at[h, yq, 2:4, :, es], ry2.at[h, 0, 2:4, :, es], ("y2", h, e, 0), dev(p, x, z, yq))
        send(yp.at[h, ym, 0:2, :, es], ry2.at[h, 1, 0:2, :, es], ("y2", h, e, 1), dev(p, x, z, ym))

    def y_mid(h, e):
        es = pl.ds(e * SUB, SUB)
        wait(ry1.at[h, 0, :, :, es], ("y1", h, e, 0))
        yp[h, yq, 0:2, :, es] = (
            yp[h, yq, 0:2, :, es].astype(f32) + ry1[h, 0, :, :, es].astype(f32)
        ).astype(bf16)
        send(yp.at[h, yq, 0:2, :, es], ry2.at[h, 0, 0:2, :, es], ("y2", h, e, 2), dev(p, x, z, yq))
        wait(ry1.at[h, 1, :, :, es], ("y1", h, e, 1))
        yp[h, ym, 2:4, :, es] = (
            yp[h, ym, 2:4, :, es].astype(f32) + ry1[h, 1, :, :, es].astype(f32)
        ).astype(bf16)
        send(yp.at[h, ym, 2:4, :, es], ry2.at[h, 1, 2:4, :, es], ("y2", h, e, 3), dev(p, x, z, ym))

    def y_end(h, e):
        es = pl.ds(e * SUB, SUB)
        wait(ry2.at[h, 0, 2:4, :, es], ("y2", h, e, 0))
        wait(ry2.at[h, 1, 0:2, :, es], ("y2", h, e, 1))
        wait(ry2.at[h, 0, 0:2, :, es], ("y2", h, e, 2))
        wait(ry2.at[h, 1, 2:4, :, es], ("y2", h, e, 3))
        sh[h, :, :, es] = (
            xt[h, y, :, :, es].astype(f32)
            + yp[h, y, :, :, es].astype(f32)
            + ry2[h, 0, :, :, es].astype(f32)
            + ry2[h, 1, :, :, es].astype(f32)
        ).astype(bf16)

        @pl.when(first)
        def _():
            dst = xt.at[h, y, :, :, es]
            src = lambda: sh.at[h, :, :, es]
            send(src, dst, ("g", h, e, 0), dev(1, x, z, yq), first)
            send(src, dst, ("g", h, e, 1), dev(1, x, z, ym), first)
            send(src, dst, ("g", h, e, 2), dev(1, x, z, y), first)

        @pl.when(second)
        def _():
            for d in (1, 3, 2):
                for xb in range(e * XB, (e + 1) * XB):
                    send(
                        lambda d=d, xb=xb: sh.at[h, zr[d], :, pl.ds(xb * BLK, BLK)],
                        xf.at[h, y, :, hcols(xb, 0)],
                        ("f", h, d, xb), dev(1, x, zr[d], y), second,
                    )
            for xb in range(e * XB, (e + 1) * XB):
                xf[h, y, :, hcols(xb, 0)] = sh[h, z, :, xb * BLK : (xb + 1) * BLK]

    FW = D // NS

    def fcols(e, part=None):
        if part is None:
            return pl.ds(e * FW, FW)
        return pl.ds(e * FW + part * (FW // 2), FW // 2)

    def finals_one(h, e):
        @pl.when(second)
        def _():
            for d in (1, 3, 2):
                for xb in range(e * XB, (e + 1) * XB):
                    wait(xf.at[h, y, :, hcols(xb, (4 - d) % 4)], ("f", h, d, xb))
            a = lambda: xf.at[h, y, :, fcols(e)]
            send(a, a(), ("q", h, e, 0), dev(1, x, z, yq), second)
            send(a, a(), ("q", h, e, 1), dev(1, x, z, ym), second)
            send(a, a(), ("q", h, e, 4), dev(0, x, z, y), second)

    def finals_two(h, e):
        @pl.when(second)
        def _():
            wait(xf.at[h, ym, :, fcols(e)], ("q", h, e, 0))
            a = lambda: xf.at[h, ym, :, fcols(e, 0)]
            send(a, a(), ("q", h, e, 2), dev(1, x, z, yq), second)
            wait(xf.at[h, yq, :, fcols(e)], ("q", h, e, 1))
            b = lambda: xf.at[h, yq, :, fcols(e, 1)]
            send(b, b(), ("q", h, e, 3), dev(1, x, z, ym), second)
            a2 = lambda: xf.at[h, ym, :, fcols(e)]
            send(a2, a2(), ("q", h, e, 5), dev(0, x, z, y), second)
            b2 = lambda: xf.at[h, yq, :, fcols(e)]
            send(b2, b2(), ("q", h, e, 6), dev(0, x, z, y), second)

    def finals_three(h, e):
        @pl.when(second)
        def _():
            wait(xf.at[h, y2, :, fcols(e, 0)], ("q", h, e, 2))
            wait(xf.at[h, y2, :, fcols(e, 1)], ("q", h, e, 3))
            a = lambda: xf.at[h, y2, :, fcols(e)]
            send(a, a(), ("q", h, e, 7), dev(0, x, z, y), second)

    def finals_here(h):
        @pl.when(first)
        def _():
            for e in range(NS):
                wait(xf.at[h, y, :, fcols(e)], ("q", h, e, 4))
                wait(xf.at[h, ym, :, fcols(e)], ("q", h, e, 5))
                wait(xf.at[h, yq, :, fcols(e)], ("q", h, e, 6))
                wait(xf.at[h, y2, :, fcols(e)], ("q", h, e, 7))

    def final_norm(h, cond):
        def work():
            for q in range(4):
                v = xf[h, q].astype(f32)
                r = lax.rsqrt(jnp.mean(v * v, axis=1, keepdims=True) + epsilon)
                xn[pl.ds((h * 4 + q) * R, R), :] = (v * r * fgain[...]).astype(bf16)

        if cond is None:
            work()
        else:
            pl.when(cond)(work)

    steps = [(h, c) for c in range(NC) for h in range(2)]
    steps += [(h, c) for h in range(2, NH) for c in range(NC)]
    with jax.named_scope("local_weights"):
        ld.start()
        lw.wait()

    n = len(steps)
    slots = {}

    def prefetch(a, b):
        for k in range(a, b):
            ucopy(k).start()


    def at(slot, prio, fn, *args):
        slots.setdefault(slot, []).append((prio, len(slots[slot]) if slot in slots else 0, fn, args))

    for k in range(PRE):
        at(-1, 0, weights_forward, k, second)
    at(-1, 1, tile_relay_first, 0)
    at(-1, 1, tile_relay_first, 1)
    at(3, 8, ld.wait)
    at(3, 9, prefetch, 0, NSLOT)
    at(-1, 1, tile_relay, 0)
    at(1, 9, tile_relay, 1)
    for h in range(2, NH):
        at(h, 3, near_later, h)
        at(h + 2, 3, tile_relay_first, h)
        at(steps.index((h, 0)) - 1, 9, tile_relay, h)
    for k in range(2 * NC):
        at(WF_SLOT[k], 0 if k == 0 else 2, weights_forward, k, first)
    for k in range(PRE, 2 * NC):
        at(1 + 2 * (k - PRE), 2, weights_forward, k, second)
    last = {}
    for i, (h, c) in enumerate(steps):
        u = i + 1
        if h == 0:
            at(u, 2, weights_last, c)
        if c == 0:
            at(u, 2, tile_ready, h)
        at(u, 2, up_chunk, h, c)
        at(u + LAG, 3, reduce_one, h, c)
        at(u + 2 * LAG, 4, reduce_two, h, c)
        at(u + 3 * LAG, 5, gather_one, h, c)
        slot = max(u + 4 * LAG, WF_SLOT[NC + c] + 2 + h)
        if h == 0:
            at(slot, 6, weights_last, NC + c)
        if c < NC - 1 or NS == 1:
            at(slot, 6, down_chunk, h, c)
        else:
            at(slot, 6, down_arrived, h, c)
        if c == NC - 1:
            for e in range(NS):
                if NS > 1:
                    at(slot, 7, down_chunk, h, c, e)
                at(slot, 7, y_start, h, e)
        last[h] = slot
    for h in range(NH):
        slot = last[h]
        lags = (1, 2, 4, 6, 7) if h < NH - 1 else (1, 2, 3, 4, 5)
        for e in range(NS):
            for lag, fn in zip(lags, (y_mid, y_end, finals_one, finals_two, finals_three)):
                at(slot + lag, 8, fn, h, e)
        if h < NH - 1:
            at(slot + 8, 13, final_norm, h, second)
    end = max(slots) + 1
    for h in range(NH):
        at(end, h, finals_here, h)
        if h < NH - 1:
            at(end, h, final_norm, h, first)
        else:
            at(end, h, final_norm, h, None)
    for slot in sorted(slots):
        for _, _, fn, args in sorted(slots[slot], key=lambda e: e[:2]):
            with jax.named_scope(getattr(fn, "__name__", "copy")):
                fn(*args)

    for d in (1, 2, 3):
        wait(cx.at[xr[(4 - d) % 4]], ("cx", d))
    cz[z] = cx[0] + cx[1] + cx[2] + cx[3]
    for d in (1, 2, 3):
        send(cz.at[z], cz.at[z], ("cz", d), dev(p, x, zr[d], y))

    m_s[...] = jnp.full_like(m_s, -jnp.inf)
    s_s[...] = jnp.zeros_like(s_s)
    k_s[...] = jnp.zeros_like(k_s)
    vocab_index = p * 4 + y

    def head(k, carry):
        slot = lax.rem(k, NSLOT)
        ucopy(k).wait()
        lt = lax.dot_general(
            ub[slot], xn[...], (((1,), (1,)), ((), ())), preferred_element_type=f32
        )
        m_old = m_s[0:1, :]
        m_new = jnp.maximum(m_old, jnp.max(lt, axis=0, keepdims=True))
        rows = lax.broadcasted_iota(jnp.int32, lt.shape, 0) + (vocab_index * V_DEV + k * UROWS)
        k_s[0:1, :] = k_s[0:1, :] + jnp.sum(
            jnp.where(rows == ids[...], lt, 0.0), axis=0, keepdims=True
        )
        s_s[0:1, :] = s_s[0:1, :] * jnp.exp(m_old - m_new) + jnp.sum(
            jnp.exp(lt - m_new), axis=0, keepdims=True
        )
        m_s[0:1, :] = m_new

        @pl.when(k + NSLOT < NU)
        def _():
            ucopy(k + NSLOT).start()

        return carry

    with jax.named_scope("head"):
        lax.fori_loop(0, NU, head, 0)

    st[vocab_index, 0:8] = m_s[...]
    st[vocab_index, 8:16] = s_s[...]
    st[vocab_index, 16:24] = k_s[...]
    mine = st.at[vocab_index]
    for d in range(4):
        yt = yr[d]
        if d > 0:
            send(mine, mine, ("st", 0, d), dev(p, x, z, yt))
        send(mine, mine, ("st", 1, d), dev(other, x, z, yt))
    stat = jax.named_scope("stats_wait")
    stat.__enter__()
    for d in range(4):
        ys = yr[(4 - d) % 4]
        if d > 0:
            wait(st.at[p * 4 + ys], ("st", 0, d))
        wait(st.at[other * 4 + ys], ("st", 1, d))
    stat.__exit__(None, None, None)
    ms = [st[i, 0:8] for i in range(8)]
    top = ms[0]
    for i in range(1, 8):
        top = jnp.maximum(top, ms[i])
    tot = jnp.zeros_like(top)
    pick = jnp.zeros_like(top)
    for i in range(8):
        tot = tot + st[i, 8:16] * jnp.exp(ms[i] - top)
        pick = pick + st[i, 16:24]
    o_tok[...] = pick - top - jnp.log(tot)

    for d in (1, 2, 3):
        wait(cz.at[zr[(4 - d) % 4]], ("cz", d))
    o_cnt[...] = cz[0] + cz[1] + cz[2] + cz[3]

    for src, ssem, cond in pending:
        if cond is None:
            pltpu.make_async_copy(src, src, sem(ssem)).wait()
    for which in (first, second):
        @pl.when(which)
        def _():
            for src, ssem, cond in pending:
                if cond is which:
                    ref = src()
                    pltpu.make_async_copy(ref, ref, sem(ssem)).wait()


def run(hs, up, down, lgain, fgain, unemb, ids, mask):
    anyspace = pl.BlockSpec(memory_space=pltpu.HBM)
    vm = pl.BlockSpec(memory_space=pltpu.VMEM)
    V = pltpu.VMEM
    return pl.pallas_call(
        body,
        out_shape=(
            jax.ShapeDtypeStruct((8, 256), f32),
            jax.ShapeDtypeStruct((8, 128), f32),
        ),
        in_specs=[anyspace, anyspace, anyspace, vm, vm, anyspace, vm, vm],
        out_specs=(vm, vm),
        scratch_shapes=[
            V((TILE_D, FF_DEV), bf16),
            V((FF_DEV, TILE_D), bf16),
            V((NH, 4, 4, R, TILE_D), bf16),
            V((NH, 4, 4, R, TILE_D), bf16),
            V((NH, 4, 4, R, FF_DEV), bf16),
            V((NH, 2, 2, R, FF_DEV), bf16),
            V((NH, 2, 4, R, FF_DEV), bf16),
            V((NH, 4, 4, R, FF_DEV), bf16),
            V((NH, 16 * R, TILE_D), f32),
            V((NH, 4, 4, R, TILE_D), bf16),
            V((NH, 2, 2, R, TILE_D), bf16),
            V((NH, 2, 4, R, TILE_D), bf16),
            V((NH, 4, R, TILE_D), bf16),
            V((NH, 4, R, D), bf16),
            V((256, D), bf16),
            V((NSLOT, UROWS, D), bf16),
            V((NH, 4, 8, 128), f32),
            V((NH, 3, 8, 128), f32),
            V((NH, 4 * R, 128), f32),
            V((8, 24, 256), f32),
            V((4, 8, 128), f32),
            V((4, 8, 128), f32),
            V((8, 256), f32),
            V((8, 256), f32),
            V((8, 256), f32),
            pltpu.SemaphoreType.DMA((NSEM,)),
            pltpu.SemaphoreType.DMA((NSLOT,)),
            pltpu.SemaphoreType.REGULAR,
        ],
        compiler_params=pltpu.CompilerParams(
            collective_id=0, has_side_effects=True, vmem_limit_bytes=66_000_000
        ),
        name="relay",
    )(hs, up, down, lgain, fgain, unemb, ids, mask)


def shards(
    hidden_states, up_weight, down_weight, layer_gain, final_gain, unembedding,
    target_ids, response_masks, anchor_logps, pairing,
):
    tok, cnt = run(
        hidden_states.reshape(NH, 4, R, D),
        up_weight[0],
        down_weight[0],
        layer_gain,
        final_gain.reshape(1, D),
        unembedding,
        target_ids.reshape(1, 256),
        response_masks,
    )
    token_logps = tok[0].reshape(4, 64)
    counts = cnt[0:4, 0]
    mask_values = response_masks.astype(f32)
    divisor = counts / 16.0
    policy = jnp.sum(mask_values * token_logps, axis=1) / divisor
    anchor = jnp.sum(mask_values * anchor_logps, axis=1) / divisor
    log_gaps = policy - anchor
    positions = jnp.arange(4, dtype=jnp.int32)
    chosen = jnp.sum(
        jnp.where(pairing[0, 0::2][:, None] == positions[None, :], log_gaps[None, :], 0.0), axis=1
    )
    rejected = jnp.sum(
        jnp.where(pairing[0, 1::2][:, None] == positions[None, :], log_gaps[None, :], 0.0), axis=1
    )
    losses = (chosen - rejected - 0.5 / ipo_tau) ** 2
    return (token_logps, policy, losses)


def solution(mesh):
    return jax.shard_map(
        shards,
        mesh=mesh,
        in_specs=(
            P("dp", None, None),
            P("pipe", "dp", "mp"),
            P("pipe", "mp", "dp"),
            P("pipe", None),
            P(),
            P(("pipe", "mp"), None),
            P("dp", None),
            P("dp", None),
            P("dp", None),
            P("dp", None),
        ),
        out_specs=(P("dp", None), P("dp"), P("dp")),
        check_vma=False,
    )
```

```python
import jax
import jax.numpy as jnp
from jax import lax
from jax.experimental import pallas as pl
from jax.experimental.pallas import tpu as pltpu
from jax.sharding import PartitionSpec as P

epsilon = 1e-05
ipo_tau = 0.5

NX, NY, NZ = 4, 4, 4
D = 4096
FF_DEV = 1792
BLK = 256
TILE_D = 4 * BLK
NH = 4
R = 32 // (NH // 2)
AHEAD = 2
END = ((2, 3, 4, 6), (1, 2, 3, 4))
LAGS = ((2, 4, 6, 7, 8), (2, 4, 5, 6, 7), (2, 3, 4, 5, 6), (1, 2, 3, 4, 5))
ORDER = (8, 8.1, 8.3, 8.2)
WF_SLOT = (-1, 0, 2, 4, 6, 8, 10, 12)
GATE = 0
PRE = 4
CHUNKS = ((0, 256), (256, 512), (768, 512), (1280, 512))
LAG = 2
NC = len(CHUNKS)
UROWS = 1024
NSLOT = 3
V_DEV = 4096
NU = V_DEV // UROWS
NS = 1
SUB = TILE_D // NS
XB = 4 // NS
NSEM = 1200

f32 = jnp.float32
bf16 = jnp.bfloat16


def body(
    hs, up, down, lgain, fgain, unemb, ids, mask, anchor, pairing,
    out,
    wu, wd, xt, xg, pp, rz1, rz2, ag, yacc, yp, ry1, ry2, sh, xf, xn, ub,
    ssb, ssr, rcol, st, cx, cz, m_s, s_s, k_s,
    sems, usem, gate,
):
    p = lax.axis_index("pipe")
    dp = lax.axis_index("dp")
    y = lax.axis_index("mp")
    x = lax.div(dp, 4)
    z = lax.rem(dp, 4)

    def wrap(v):
        return lax.rem(v + 4, 4)

    xr = [wrap(x + d) for d in range(4)]
    yr = [wrap(y + d) for d in range(4)]
    zr = [wrap(z + d) for d in range(4)]

    def dev(pi, xi, zi, yi):
        return {"pipe": pi, "dp": xi * 4 + zi, "mp": yi}

    names = {}

    def sem(key):
        if key not in names:
            assert len(names) < NSEM
            names[key] = len(names)
        return sems.at[names[key]]

    pending = []
    recorded = set()
    turn = [None]

    def when(core):
        if turn[0] is None:
            return pl.when(core)
        return (lambda fn: fn()) if turn[0] is core else (lambda fn: None)

    def send(src, dst, key, to, cond=None):
        cp = pltpu.make_async_remote_copy(
            src_ref=src() if callable(src) else src, dst_ref=dst, send_sem=sem(("s", key)), recv_sem=sem(("r", key)),
            device_id=to, device_id_type=pl.DeviceIdType.MESH,
        )
        cp.start()
        if (key, id(cond)) not in recorded:
            recorded.add((key, id(cond)))
            pending.append((src, ("s", key), cond))

    def wait(dst, key):
        pltpu.make_async_copy(dst, dst, sem(("r", key))).wait()

    xp, xm, x2 = xr[1], xr[3], xr[2]
    zp, zm, z2 = zr[1], zr[3], zr[2]
    yq, ym, y2 = yr[1], yr[3], yr[2]
    other = 1 - p
    first = p == 0
    second = p == 1

    def ucopy(k):
        slot = lax.rem(k, NSLOT)
        return pltpu.make_async_copy(
            unemb.at[pl.ds(k * UROWS, UROWS)], ub.at[slot], usem.at[slot]
        )

    xrow = pl.ds(pl.multiple_of(x * BLK, BLK), BLK)
    lw = pltpu.make_async_copy(up, wu.at[xrow, :], sem("lwu"))
    lw.start()
    ld = pltpu.make_async_copy(down, wd.at[:, xrow], sem("lwd"))

    cols_of = [
        [pl.ds(pl.multiple_of((xb * 4 + zr[d]) * BLK, BLK), BLK) for d in range(4)]
        for xb in range(4)
    ]

    def hcols(xb, d):
        return cols_of[xb][d]

    cx[...] = jnp.zeros_like(cx)
    cz[...] = jnp.zeros_like(cz)
    st[...] = jnp.zeros_like(st)
    ssb[...] = jnp.zeros_like(ssb)

    bar = pltpu.get_barrier_semaphore()
    peers = []
    for d in (1, 2, 3):
        peers.append(dev(p, xr[d], z, y))
        peers.append(dev(p, x, zr[d], y))
        peers.append(dev(p, x, z, yr[d]))
    for d in range(4):
        peers.append(dev(other, x, z, yr[d]))
    for peer in peers:
        pl.semaphore_signal(bar, inc=1, device_id=peer, device_id_type=pl.DeviceIdType.MESH)
    with jax.named_scope("barrier"):
        pl.semaphore_wait(bar, len(peers))

    items = [("u", c) for c in range(NC)] + [("d", c) for c in range(NC)]

    def own_weights(i):
        kind, c = items[i]
        o, w = CHUNKS[c]
        if kind == "u":
            src = up.at[:, pl.ds(o, w)]
            dst = wu.at[xrow, pl.ds(o, w)]
        else:
            src = down.at[pl.ds(o, w), :]
            dst = wd.at[pl.ds(o, w), xrow]
        return src, dst

    def wslice(i, xb, part=None):
        kind, c = items[i]
        o, w = CHUNKS[c]
        if kind == "u":
            n = BLK if part is None else BLK // 2
            s = xb * BLK + (0 if part is None else part * (BLK // 2))
            return wu.at[pl.ds(pl.multiple_of(s, n), n), pl.ds(o, w)]
        n = w if part is None else w // 2
        s = o + (0 if part is None else part * (w // 2))
        return wd.at[pl.ds(s, n), pl.ds(pl.multiple_of(xb * BLK, BLK), BLK)]

    def weights_own(i, cond=None):
        _, dst = own_weights(i)
        src = lambda: own_weights(i)[0]
        if cond is None:
            src = src()
        send(src, dst, ("w", i, 0), dev(p, xp, z, y), cond)
        send(src, dst, ("w", i, 1), dev(p, xm, z, y), cond)

    def weights_forward(i, cond):
        @pl.when(cond)
        def _():
            wait(wslice(i, xm), ("w", i, 0))
            a = lambda: wslice(i, xm, 0)
            send(a, a(), ("w", i, 2), dev(p, xp, z, y), cond)
            wait(wslice(i, xp), ("w", i, 1))
            b = lambda: wslice(i, xp, 1)
            send(b, b(), ("w", i, 3), dev(p, xm, z, y), cond)
            if cond is first and i == 0:
                for k in range(2, AHEAD):
                    weights_own(k, cond)
            if i + AHEAD < len(items):
                weights_own(i + AHEAD, cond)
            if cond is first and i == len(items) - 1 - GATE:
                pl.semaphore_signal(gate, inc=1, device_id=dev(1, x, z, y),
                                    device_id_type=pl.DeviceIdType.MESH)

    def weights_last(i):
        wait(wslice(i, x2, 0), ("w", i, 2))
        wait(wslice(i, x2, 1), ("w", i, 3))

    def far_tokens(h):
        for xb in range(4):
            part = slice(None) if h == 0 else y
            send(
                lambda h=h, xb=xb, part=part: hs.at[h, part, :, hcols(xb, 2)],
                xt.at[h, part, z, :, pl.ds(xb * BLK, BLK)],
                ("x", h, 2, xb), dev(0, x, z2, y), first,
            )

    def near_tokens(h):
        for d in (1, 3):
            for xb in range(4):
                send(
                    lambda h=h, d=d, xb=xb: hs.at[h, :, :, hcols(xb, d)],
                    xt.at[h, :, z, :, pl.ds(xb * BLK, BLK)],
                    ("x", h, d, xb), dev(0, x, zr[d], y), first,
                )
        for xb in range(4):
            pltpu.make_async_copy(
                hs.at[h, :, :, hcols(xb, 0)], xt.at[h, :, z, :, pl.ds(xb * BLK, BLK)],
                sem(("xl", h, xb)),
            ).start()

    def near_later(h):
        @pl.when(first)
        def _():
            near_tokens(h)

    @pl.when(first)
    def _():
        weights_own(0, first)
        weights_own(1, first)
        far_tokens(0)
        near_tokens(0)
        for h in range(1, NH):
            far_tokens(h)

    own = jnp.sum(mask[...].astype(f32), axis=1, keepdims=True)
    cx[x, 0:4, :] = jnp.broadcast_to(own, (4, 128))
    for d in (1, 2, 3):
        send(cx.at[x], cx.at[x], ("cx", d), dev(p, xr[d], z, y))

    @pl.when(second)
    def _():
        pl.semaphore_wait(gate, 1)
        for i in range(AHEAD):
            weights_own(i, second)

    gz = jnp.concatenate([lgain[:, hcols(xb, 0)] for xb in range(4)], axis=1)

    def tile_arrived(h):
        @pl.when(first)
        def _():
            for xb in range(4):
                pltpu.make_async_copy(
                    hs.at[h, :, :, hcols(xb, 0)], xt.at[h, :, z, :, pl.ds(xb * BLK, BLK)],
                    sem(("xl", h, xb)),
                ).wait()
            for d in (1, 3):
                zs = zr[(4 - d) % 4]
                for xb in range(4):
                    wait(xt.at[h, :, zs, :, pl.ds(xb * BLK, BLK)], ("x", h, d, xb))
            if h == 0:
                for xb in range(4):
                    wait(xt.at[h, :, z2, :, pl.ds(xb * BLK, BLK)], ("x", h, 2, xb))
            else:
                for d in (1, 3, 2):
                    wait(xt.at[h, yr[(4 - d) % 4], z2], ("xy", h, d))

        @pl.when(second)
        def _():
            for e in range(NS):
                es = pl.ds(e * SUB, SUB)
                wait(xt.at[h, y, :, :, es], ("g", h, e, 2))
                wait(xt.at[h, y2, 0:2, :, es], ("g", h, e, 3))
                wait(xt.at[h, y2, 2:4, :, es], ("g", h, e, 4))

    def tile_relay_first(h):
        @pl.when(first)
        def _():
            for xb in range(4):
                wait(xt.at[h, y, z2, :, pl.ds(xb * BLK, BLK)], ("x", h, 2, xb))
            a = lambda: xt.at[h, y, z2]
            for d in (1, 3, 2):
                send(a, a(), ("xy", h, d), dev(0, x, z, yr[d]), first)

    def tile_relay(h):
        @pl.when(second)
        def _():
            for e in range(NS):
                es = pl.ds(e * SUB, SUB)
                wait(xt.at[h, ym, :, :, es], ("g", h, e, 0))
                a = lambda es=es: xt.at[h, ym, 0:2, :, es]
                send(a, a(), ("g", h, e, 3), dev(1, x, z, yq), second)
                wait(xt.at[h, yq, :, :, es], ("g", h, e, 1))
                b = lambda es=es: xt.at[h, yq, 2:4, :, es]
                send(b, b(), ("g", h, e, 4), dev(1, x, z, ym), second)

    def tile_ready(h):
        tile_arrived(h)
        ones = jnp.ones((8, TILE_D), bf16)
        for g in range(4):
            v = xt[h, :, g].reshape(4 * R, TILE_D).astype(f32)
            xg[h, :, g] = (v * gz).astype(bf16).reshape(4, R, TILE_D)
            sq = v * v
            hi = sq.astype(bf16)
            lo = (sq - hi.astype(f32)).astype(bf16)
            dn = (((1,), (1,)), ((), ()))
            ssb[h, g, :, 0 : 4 * R] = lax.dot_general(
                ones, hi, dn, preferred_element_type=f32
            ) + lax.dot_general(ones, lo, dn, preferred_element_type=f32)
        for d in (1, 3, 2):
            zt = zr[d]
            send(ssb.at[h, zt], ssr.at[h, d - 1], ("ss", h, d), dev(p, x, zt, y))

    def row_scale(h):
        for d in (1, 3, 2):
            wait(ssr.at[h, d - 1], ("ss", h, d))
        total = ssb[h, z] + ssr[h, 0] + ssr[h, 1] + ssr[h, 2]
        scale = lax.rsqrt(total * (1.0 / D) + epsilon)
        col = jnp.transpose(scale, (1, 0))[0 : 4 * R, 0:1]
        rcol[h] = jnp.broadcast_to(col, (4 * R, 128))

    def up_chunk(h, c):
        o, w = CHUNKS[c]
        lhs = xg[h].reshape(16 * R, TILE_D)
        r = jnp.dot(lhs, wu[:, o : o + w], preferred_element_type=f32)
        pp[h, :, :, :, o : o + w] = r.astype(bf16).reshape(4, 4, R, w)
        cs = pl.ds(o, w)
        send(pp.at[h, 0:2, z2, :, cs], rz1.at[h, 0, :, :, cs], ("z1", h, c, 0), dev(p, x, zp, y))
        send(pp.at[h, 2:4, z2, :, cs], rz1.at[h, 1, :, :, cs], ("z1", h, c, 1), dev(p, x, zm, y))
        send(pp.at[h, 2:4, zp, :, cs], rz2.at[h, 0, 2:4, :, cs], ("z2", h, c, 0), dev(p, x, zp, y))
        send(pp.at[h, 0:2, zm, :, cs], rz2.at[h, 1, 0:2, :, cs], ("z2", h, c, 1), dev(p, x, zm, y))

    def reduce_one(h, c):
        o, w = CHUNKS[c]
        cs = pl.ds(o, w)
        wait(rz1.at[h, 0, :, :, cs], ("z1", h, c, 0))
        pp[h, 0:2, zp, :, cs] = (
            pp[h, 0:2, zp, :, cs].astype(f32) + rz1[h, 0, :, :, cs].astype(f32)
        ).astype(bf16)
        send(pp.at[h, 0:2, zp, :, cs], rz2.at[h, 0, 0:2, :, cs], ("z2", h, c, 2), dev(p, x, zp, y))
        wait(rz1.at[h, 1, :, :, cs], ("z1", h, c, 1))
        pp[h, 2:4, zm, :, cs] = (
            pp[h, 2:4, zm, :, cs].astype(f32) + rz1[h, 1, :, :, cs].astype(f32)
        ).astype(bf16)
        send(pp.at[h, 2:4, zm, :, cs], rz2.at[h, 1, 2:4, :, cs], ("z2", h, c, 3), dev(p, x, zm, y))

    def reduce_two(h, c):
        o, w = CHUNKS[c]
        cs = pl.ds(o, w)
        if c == 0:
            row_scale(h)
        wait(rz2.at[h, 0, 2:4, :, cs], ("z2", h, c, 0))
        wait(rz2.at[h, 1, 0:2, :, cs], ("z2", h, c, 1))
        wait(rz2.at[h, 0, 0:2, :, cs], ("z2", h, c, 2))
        wait(rz2.at[h, 1, 2:4, :, cs], ("z2", h, c, 3))
        s = (
            pp[h, :, z, :, cs].astype(f32)
            + rz2[h, 0, :, :, cs].astype(f32)
            + rz2[h, 1, :, :, cs].astype(f32)
        ).reshape(4 * R, w)
        v = s * rcol[h][:, 0:1]
        act = v / (1.0 + jnp.exp(-v))
        ag[h, :, z, :, cs] = act.astype(bf16).reshape(4, R, w)
        a = ag.at[h, :, z, :, cs]
        send(a, a, ("a", h, c, 0), dev(p, x, zp, y))
        send(a, a, ("a", h, c, 1), dev(p, x, zm, y))

    def gather_one(h, c):
        o, w = CHUNKS[c]
        cs = pl.ds(o, w)
        wait(ag.at[h, :, zm, :, cs], ("a", h, c, 0))
        a = ag.at[h, 0:2, zm, :, cs]
        send(a, a, ("a", h, c, 2), dev(p, x, zp, y))
        wait(ag.at[h, :, zp, :, cs], ("a", h, c, 1))
        b = ag.at[h, 2:4, zp, :, cs]
        send(b, b, ("a", h, c, 3), dev(p, x, zm, y))

    def down_arrived(h, c):
        cs = pl.ds(*CHUNKS[c])
        wait(ag.at[h, 0:2, z2, :, cs], ("a", h, c, 2))
        wait(ag.at[h, 2:4, z2, :, cs], ("a", h, c, 3))

    def down_chunk(h, c, e=None):
        o, w = CHUNKS[c]
        cs = pl.ds(o, w)
        if e is None:
            down_arrived(h, c)
        lhs = ag[h, :, :, :, cs].reshape(16 * R, w)
        for n in range(0 if e is None else e * SUB, TILE_D if e is None else (e + 1) * SUB, 256):
            r = jnp.dot(lhs, wd[cs, n : n + 256], preferred_element_type=f32)
            if c > 0:
                r = r + yacc[h, :, n : n + 256]
            if c == NC - 1:
                yp[h, :, :, :, n : n + 256] = r.astype(bf16).reshape(4, 4, R, 256)
            else:
                yacc[h, :, n : n + 256] = r

    def y_start(h, e):
        es = pl.ds(e * SUB, SUB)
        send(yp.at[h, y2, 0:2, :, es], ry1.at[h, 0, :, :, es], ("y1", h, e, 0), dev(p, x, z, yq))
        send(yp.at[h, y2, 2:4, :, es], ry1.at[h, 1, :, :, es], ("y1", h, e, 1), dev(p, x, z, ym))
        send(yp.at[h, yq, 2:4, :, es], ry2.at[h, 0, 2:4, :, es], ("y2", h, e, 0), dev(p, x, z, yq))
        send(yp.at[h, ym, 0:2, :, es], ry2.at[h, 1, 0:2, :, es], ("y2", h, e, 1), dev(p, x, z, ym))

    def y_mid(h, e):
        es = pl.ds(e * SUB, SUB)
        wait(ry1.at[h, 0, :, :, es], ("y1", h, e, 0))
        yp[h, yq, 0:2, :, es] = (
            yp[h, yq, 0:2, :, es].astype(f32) + ry1[h, 0, :, :, es].astype(f32)
        ).astype(bf16)
        send(lambda: yp.at[h, yq, 0:2, :, es], ry2.at[h, 0, 0:2, :, es], ("y2", h, e, 2), dev(p, x, z, yq))
        wait(ry1.at[h, 1, :, :, es], ("y1", h, e, 1))
        yp[h, ym, 2:4, :, es] = (
            yp[h, ym, 2:4, :, es].astype(f32) + ry1[h, 1, :, :, es].astype(f32)
        ).astype(bf16)
        send(lambda: yp.at[h, ym, 2:4, :, es], ry2.at[h, 1, 2:4, :, es], ("y2", h, e, 3), dev(p, x, z, ym))

    def y_end(h, e):
        es = pl.ds(e * SUB, SUB)
        wait(ry2.at[h, 0, 2:4, :, es], ("y2", h, e, 0))
        wait(ry2.at[h, 1, 0:2, :, es], ("y2", h, e, 1))
        wait(ry2.at[h, 0, 0:2, :, es], ("y2", h, e, 2))
        wait(ry2.at[h, 1, 2:4, :, es], ("y2", h, e, 3))
        sh[h, :, :, es] = (
            xt[h, y, :, :, es].astype(f32)
            + yp[h, y, :, :, es].astype(f32)
            + ry2[h, 0, :, :, es].astype(f32)
            + ry2[h, 1, :, :, es].astype(f32)
        ).astype(bf16)

        @when(first)
        def _():
            dst = xt.at[h, y, :, :, es]
            src = lambda: sh.at[h, :, :, es]
            send(src, dst, ("g", h, e, 0), dev(1, x, z, yq), first)
            send(src, dst, ("g", h, e, 1), dev(1, x, z, ym), first)
            send(src, dst, ("g", h, e, 2), dev(1, x, z, y), first)

        @when(second)
        def _():
            for d in (1, 3, 2):
                for xb in range(e * XB, (e + 1) * XB):
                    send(
                        lambda d=d, xb=xb: sh.at[h, zr[d], :, pl.ds(xb * BLK, BLK)],
                        xf.at[h, y, :, hcols(xb, 0)],
                        ("f", h, d, xb), dev(1, x, zr[d], y), second,
                    )
            for xb in range(e * XB, (e + 1) * XB):
                xf[h, y, :, hcols(xb, 0)] = sh[h, z, :, xb * BLK : (xb + 1) * BLK]

    FW = D // NS

    def fcols(e, part=None):
        if part is None:
            return pl.ds(e * FW, FW)
        return pl.ds(e * FW + part * (FW // 2), FW // 2)

    def finals_one(h, e):
        @when(second)
        def _():
            for d in (1, 3, 2):
                for xb in range(e * XB, (e + 1) * XB):
                    wait(xf.at[h, y, :, hcols(xb, (4 - d) % 4)], ("f", h, d, xb))
            a = lambda: xf.at[h, y, :, fcols(e)]
            send(a, a(), ("q", h, e, 0), dev(1, x, z, yq), second)
            send(a, a(), ("q", h, e, 1), dev(1, x, z, ym), second)
            send(a, a(), ("q", h, e, 4), dev(0, x, z, y), second)

    def finals_two(h, e):
        @when(second)
        def _():
            wait(xf.at[h, ym, :, fcols(e)], ("q", h, e, 0))
            a = lambda: xf.at[h, ym, :, fcols(e, 0)]
            send(a, a(), ("q", h, e, 2), dev(1, x, z, yq), second)
            wait(xf.at[h, yq, :, fcols(e)], ("q", h, e, 1))
            b = lambda: xf.at[h, yq, :, fcols(e, 1)]
            send(b, b(), ("q", h, e, 3), dev(1, x, z, ym), second)
            a2 = lambda: xf.at[h, ym, :, fcols(e)]
            send(a2, a2(), ("q", h, e, 5), dev(0, x, z, y), second)
            b2 = lambda: xf.at[h, yq, :, fcols(e)]
            send(b2, b2(), ("q", h, e, 6), dev(0, x, z, y), second)

    def finals_three(h, e):
        @when(second)
        def _():
            wait(xf.at[h, y2, :, fcols(e, 0)], ("q", h, e, 2))
            wait(xf.at[h, y2, :, fcols(e, 1)], ("q", h, e, 3))
            a = lambda: xf.at[h, y2, :, fcols(e)]
            send(a, a(), ("q", h, e, 7), dev(0, x, z, y), second)

    def finals_here(h):
        @pl.when(first)
        def _():
            for e in range(NS):
                wait(xf.at[h, y, :, fcols(e)], ("q", h, e, 4))
                wait(xf.at[h, ym, :, fcols(e)], ("q", h, e, 5))
                wait(xf.at[h, yq, :, fcols(e)], ("q", h, e, 6))
                wait(xf.at[h, y2, :, fcols(e)], ("q", h, e, 7))

    def final_norm(h, cond):
        def work():
            for q in range(4):
                v = xf[h, q].astype(f32)
                r = lax.rsqrt(jnp.mean(v * v, axis=1, keepdims=True) + epsilon)
                xn[pl.ds((h * 4 + q) * R, R), :] = (v * r * fgain[...]).astype(bf16)

        if cond is None:
            work()
        else:
            pl.when(cond)(work)

    steps = [(h, c) for c in range(NC) for h in range(2)]
    steps += [(h, c) for h in range(2, NH) for c in range(NC)]
    with jax.named_scope("local_weights"):
        ld.start()
        lw.wait()

    n = len(steps)
    slots = {}

    def prefetch(a, b):
        for k in range(a, b):
            ucopy(k).start()


    def at(slot, prio, fn, *args):
        entry = (prio, len(slots.get(slot, ())), fn, args, None)
        slots.setdefault(slot, []).append(entry)

    def at_core(core, slot, prio, fn, *args):
        entry = (prio, len(slots.get(slot, ())), fn, args, core)
        slots.setdefault(slot, []).append(entry)

    for k in range(PRE):
        at(-1, 0, weights_forward, k, second)
    at(-1, 1, near_later, 1)
    at(0, 1, tile_relay_first, 1)
    at(3, 8, ld.wait)
    at(3, 9, prefetch, 0, NSLOT)
    at(-1, 1, tile_relay, 0)
    at(1, 9, tile_relay, 1)
    for h in range(2, NH):
        at(h, 3, near_later, h)
        at(h + 2, 3, tile_relay_first, h)
        at(steps.index((h, 0)) - 1, 9, tile_relay, h)
    for k in range(2 * NC):
        at(WF_SLOT[k], 0 if k == 0 else 2, weights_forward, k, first)
    for k in range(PRE, 2 * NC):
        at(1 + 2 * (k - PRE), 2, weights_forward, k, second)
    last = {}
    for i, (h, c) in enumerate(steps):
        u = i + 1
        if h == 0:
            at(u, 2, weights_last, c)
        if c == 0:
            at(u, 2, tile_ready, h)
        at(u, 2, up_chunk, h, c)
        stage = [u + k * LAG for k in range(1, 5)]
        if h >= NH - 2:
            end = steps.index((h, NC - 1)) + 1
            cap = END[h - NH + 2]
            stage = [min(t, end + d) for t, d in zip(stage, cap)]
        at(stage[0], 3, reduce_one, h, c)
        at(stage[1], 4, reduce_two, h, c)
        at(stage[2], 5, gather_one, h, c)
        slot = max(stage[3], WF_SLOT[NC + c] + 2 + h)
        if h == 0:
            at(slot, 6, weights_last, NC + c)
        if c < NC - 1 or NS == 1:
            at(slot, 6, down_chunk, h, c)
        else:
            at(slot, 6, down_arrived, h, c)
        if c == NC - 1:
            for e in range(NS):
                if NS > 1:
                    at(slot, 7, down_chunk, h, c, e)
                at(slot, 7, y_start, h, e)
        last[h] = slot
    for h in range(NH):
        slot = last[h]
        at_core(first, slot + 1, 8, y_mid, h, 0)
        at_core(first, slot + 2, 8, y_end, h, 0)
        fns = (y_mid, y_end, finals_one, finals_two, finals_three)
        for lag, fn in zip(LAGS[h], fns):
            at_core(second, slot + lag, ORDER[h], fn, h, 0)
        if h < NH - 1:
            at(slot + LAGS[h][-1], 13, final_norm, h, second)
    end = max(slots) + 1
    for h in range(NH):
        at(end, h, finals_here, h)
        if h < NH - 1:
            at(end, h, final_norm, h, first)
        else:
            at(end, h, final_norm, h, None)
    for slot in sorted(slots):
        for _, _, fn, args, core in sorted(slots[slot], key=lambda e: e[:2]):
            with jax.named_scope(getattr(fn, "__name__", "copy")):
                if core is None:
                    fn(*args)
                else:
                    turn[0] = core
                    pl.when(core)(lambda: fn(*args))
                    turn[0] = None

    for d in (1, 2, 3):
        wait(cx.at[xr[(4 - d) % 4]], ("cx", d))
    cz[z] = cx[0] + cx[1] + cx[2] + cx[3]
    for d in (1, 2, 3):
        send(cz.at[z], cz.at[z], ("cz", d), dev(p, x, zr[d], y))

    vocab_index = p * 4 + y
    lanes = lax.broadcasted_iota(jnp.int32, (64, 256), 1)
    spread = (lanes % 64 == lax.broadcasted_iota(jnp.int32, (64, 256), 0)).astype(bf16)
    own_row = lax.broadcasted_iota(jnp.int32, (8, 256), 1) // 64 == lax.broadcasted_iota(
        jnp.int32, (8, 256), 0
    )

    def to_row(v):
        r = jnp.dot(v, spread, preferred_element_type=f32)
        return jnp.sum(jnp.where(own_row, r, 0.0), axis=0, keepdims=True)

    idp = jnp.concatenate([ids[...], jnp.zeros((4, 64), jnp.int32)], axis=0)
    high = to_row((idp // 256).astype(f32).astype(bf16))
    low = to_row((idp % 256).astype(f32).astype(bf16))
    id_row = (high * 256.0 + low).astype(jnp.int32) - vocab_index * V_DEV

    m_s[...] = jnp.full_like(m_s, -jnp.inf)
    s_s[...] = jnp.zeros_like(s_s)
    k_s[...] = jnp.zeros_like(k_s)

    def head(k, carry):
        slot = lax.rem(k, NSLOT)
        ucopy(k).wait()
        lt = lax.dot_general(
            ub[slot], xn[...], (((1,), (1,)), ((), ())), preferred_element_type=f32
        )
        m_old = m_s[...]
        m_new = jnp.maximum(m_old, jnp.max(lt, axis=0, keepdims=True))
        rows = lax.broadcasted_iota(jnp.int32, lt.shape, 0) + k * UROWS
        k_s[...] = k_s[...] + jnp.sum(jnp.where(rows == id_row, lt, 0.0), axis=0, keepdims=True)
        s_s[...] = s_s[...] * jnp.exp(m_old - m_new) + jnp.sum(
            jnp.exp(lt - m_new), axis=0, keepdims=True
        )
        m_s[...] = m_new

        @pl.when(k + NSLOT < NU)
        def _():
            ucopy(k + NSLOT).start()

        return carry

    with jax.named_scope("head"):
        lax.fori_loop(0, NU, head, 0)

    st[vocab_index, 0:1] = m_s[...]
    st[vocab_index, 1:2] = s_s[...]
    st[vocab_index, 2:3] = k_s[...]
    mine = st.at[vocab_index]
    for d in range(4):
        yt = yr[d]
        if d > 0:
            send(mine, mine, ("st", 0, d), dev(p, x, z, yt))
        send(mine, mine, ("st", 1, d), dev(other, x, z, yt))
    stat = jax.named_scope("stats_wait")
    stat.__enter__()
    for d in range(4):
        ys = yr[(4 - d) % 4]
        if d > 0:
            wait(st.at[p * 4 + ys], ("st", 0, d))
        wait(st.at[other * 4 + ys], ("st", 1, d))
    stat.__exit__(None, None, None)
    ms = [st[i, 0:1] for i in range(8)]
    top = ms[0]
    for i in range(1, 8):
        top = jnp.maximum(top, ms[i])
    tot = jnp.zeros_like(top)
    pick = jnp.zeros_like(top)
    for i in range(8):
        tot = tot + st[i, 1:2] * jnp.exp(ms[i] - top)
        pick = pick + st[i, 2:3]
    row = pick - top - jnp.log(tot)
    for d in (1, 2, 3):
        wait(cz.at[zr[(4 - d) % 4]], ("cz", d))
    counts = (cz[0] + cz[1] + cz[2] + cz[3])[0:4, 0:1]
    divisor = counts / 16.0
    mv = mask[...].astype(f32)
    tok = jnp.concatenate([row[:, 64 * i : 64 * i + 64] for i in range(4)], axis=0)
    policy = jnp.sum(mv * tok, axis=1, keepdims=True) / divisor
    gaps = policy - jnp.sum(mv * anchor[...], axis=1, keepdims=True) / divisor
    place = lax.broadcasted_iota(jnp.int32, (4, 1), 0)
    side = lax.broadcasted_iota(jnp.int32, (4, 64), 1)
    extra = jnp.broadcast_to(policy, (4, 64))
    for i in range(2):
        chosen = jnp.sum(jnp.where(place == pairing[0, 2 * i], gaps, 0.0))
        rejected = jnp.sum(jnp.where(place == pairing[0, 2 * i + 1], gaps, 0.0))
        diff = chosen - rejected - 0.5 / ipo_tau
        extra = jnp.where(side == i + 1, diff * diff, extra)
    out[0:4, :] = jnp.concatenate([tok, extra], axis=1)
    out[4:8, :] = jnp.zeros((4, 128), f32)

    for src, ssem, cond in pending:
        if cond is None:
            ref = src() if callable(src) else src
            pltpu.make_async_copy(ref, ref, sem(ssem)).wait()
    for which in (first, second):
        @pl.when(which)
        def _():
            for src, ssem, cond in pending:
                if cond is which:
                    ref = src()
                    pltpu.make_async_copy(ref, ref, sem(ssem)).wait()


def run(hs, up, down, lgain, fgain, unemb, ids, mask, anchor, pairing):
    anyspace = pl.BlockSpec(memory_space=pltpu.HBM)
    vm = pl.BlockSpec(memory_space=pltpu.VMEM)
    sm = pl.BlockSpec(memory_space=pltpu.SMEM)
    V = pltpu.VMEM
    return pl.pallas_call(
        body,
        out_shape=(
            jax.ShapeDtypeStruct((8, 128), f32)
        ),
        in_specs=[anyspace, anyspace, anyspace, vm, vm, anyspace, vm, vm, vm, sm],
        out_specs=vm,
        scratch_shapes=[
            V((TILE_D, FF_DEV), bf16),
            V((FF_DEV, TILE_D), bf16),
            V((NH, 4, 4, R, TILE_D), bf16),
            V((NH, 4, 4, R, TILE_D), bf16),
            V((NH, 4, 4, R, FF_DEV), bf16),
            V((NH, 2, 2, R, FF_DEV), bf16),
            V((NH, 2, 4, R, FF_DEV), bf16),
            V((NH, 4, 4, R, FF_DEV), bf16),
            V((NH, 16 * R, TILE_D), f32),
            V((NH, 4, 4, R, TILE_D), bf16),
            V((NH, 2, 2, R, TILE_D), bf16),
            V((NH, 2, 4, R, TILE_D), bf16),
            V((NH, 4, R, TILE_D), bf16),
            V((NH, 4, R, D), bf16),
            V((256, D), bf16),
            V((NSLOT, UROWS, D), bf16),
            V((NH, 4, 8, 128), f32),
            V((NH, 3, 8, 128), f32),
            V((NH, 4 * R, 128), f32),
            V((8, 8, 256), f32),
            V((4, 8, 128), f32),
            V((4, 8, 128), f32),
            V((1, 256), f32),
            V((1, 256), f32),
            V((1, 256), f32),
            pltpu.SemaphoreType.DMA((NSEM,)),
            pltpu.SemaphoreType.DMA((NSLOT,)),
            pltpu.SemaphoreType.REGULAR,
        ],
        compiler_params=pltpu.CompilerParams(
            collective_id=0, has_side_effects=True, vmem_limit_bytes=66_000_000
        ),
        name="relay",
    )(hs, up, down, lgain, fgain, unemb, ids, mask, anchor, pairing)


def unpack(rows, tok, policy, losses):
    tok[...] = rows[0:4, 0:64]
    for i in range(4):
        policy[i] = rows[i, 64]
    for i in range(2):
        losses[i] = rows[0, 65 + i]


def shards(
    hidden_states, up_weight, down_weight, layer_gain, final_gain, unembedding,
    target_ids, response_masks, anchor_logps, pairing,
):
    out = run(
        hidden_states.reshape(NH, 4, R, D),
        up_weight[0],
        down_weight[0],
        layer_gain,
        final_gain.reshape(1, D),
        unembedding,
        target_ids,
        response_masks,
        anchor_logps,
        pairing,
    )
    vm = pl.BlockSpec(memory_space=pltpu.VMEM)
    sm = pl.BlockSpec(memory_space=pltpu.SMEM)
    return pl.pallas_call(
        unpack,
        out_shape=(
            jax.ShapeDtypeStruct((4, 64), f32),
            jax.ShapeDtypeStruct((4,), f32),
            jax.ShapeDtypeStruct((2,), f32),
        ),
        in_specs=[vm],
        out_specs=(vm, sm, sm),
        name="unpack",
    )(out)


def solution(mesh):
    return jax.shard_map(
        shards,
        mesh=mesh,
        in_specs=(
            P("dp", None, None),
            P("pipe", "dp", "mp"),
            P("pipe", "mp", "dp"),
            P("pipe", None),
            P(),
            P(("pipe", "mp"), None),
            P("dp", None),
            P("dp", None),
            P("dp", None),
            P("dp", None),
        ),
        out_specs=(P("dp", None), P("dp"), P("dp")),
        check_vma=False,
    )
```

```python
import jax
import jax.numpy as jnp
from jax import lax
from jax.experimental import pallas as pl
from jax.experimental.pallas import tpu as pltpu
from jax.sharding import PartitionSpec as P

epsilon = 1e-05
ipo_tau = 0.5

NX, NY, NZ = 4, 4, 4
D = 4096
FF_DEV = 1792
BLK = 256
TILE_D = 4 * BLK
NH = 4
R = 32 // (NH // 2)
AHEAD = 2
END = ((2, 3, 4, 6), (1, 2, 3, 4))
LAGS = ((2, 4, 6, 7, 8), (2, 4, 5, 6, 7), (2, 3, 4, 5, 6), (1, 2, 3, 4, 5))
ORDER = (8, 8.1, 7.9, 7.5)
WF_SLOT = (-1, 0, 2, 4, 6, 8, 10, 12)
GATE = 0
PRE = 4
CHUNKS = ((0, 384), (384, 512), (896, 512), (1408, 384))
LAG = 2
NC = len(CHUNKS)
UROWS = 1024
NSLOT = 3
V_DEV = 4096
NU = V_DEV // UROWS
NS = 1
SUB = TILE_D // NS
XB = 4 // NS
NSEM = 1200

f32 = jnp.float32
bf16 = jnp.bfloat16


def body(
    hs, up, down, lgain, fgain, unemb, ids, mask, anchor, pairing,
    out,
    wu, wd, xt, xg, pp, rz1, rz2, ag, yacc, yp, ry1, ry2, sh, xf, xn, ub,
    ssb, ssr, rcol, st, cx, cz, m_s, s_s, k_s,
    sems, usem, gate,
):
    p = lax.axis_index("pipe")
    dp = lax.axis_index("dp")
    y = lax.axis_index("mp")
    x = lax.div(dp, 4)
    z = lax.rem(dp, 4)

    def wrap(v):
        return lax.rem(v + 4, 4)

    xr = [wrap(x + d) for d in range(4)]
    yr = [wrap(y + d) for d in range(4)]
    zr = [wrap(z + d) for d in range(4)]

    def dev(pi, xi, zi, yi):
        return {"pipe": pi, "dp": xi * 4 + zi, "mp": yi}

    names = {}

    def sem(key):
        if key not in names:
            assert len(names) < NSEM
            names[key] = len(names)
        return sems.at[names[key]]

    pending = []
    recorded = set()
    turn = [None]

    def when(core):
        if turn[0] is None:
            return pl.when(core)
        return (lambda fn: fn()) if turn[0] is core else (lambda fn: None)

    def send(src, dst, key, to, cond=None):
        cp = pltpu.make_async_remote_copy(
            src_ref=src() if callable(src) else src, dst_ref=dst, send_sem=sem(("s", key)), recv_sem=sem(("r", key)),
            device_id=to, device_id_type=pl.DeviceIdType.MESH,
        )
        cp.start()
        if (key, id(cond)) not in recorded:
            recorded.add((key, id(cond)))
            pending.append((src, ("s", key), cond))

    def wait(dst, key):
        pltpu.make_async_copy(dst, dst, sem(("r", key))).wait()

    xp, xm, x2 = xr[1], xr[3], xr[2]
    zp, zm, z2 = zr[1], zr[3], zr[2]
    yq, ym, y2 = yr[1], yr[3], yr[2]
    other = 1 - p
    first = p == 0
    second = p == 1

    def ucopy(k):
        slot = lax.rem(k, NSLOT)
        return pltpu.make_async_copy(
            unemb.at[pl.ds(k * UROWS, UROWS)], ub.at[slot], usem.at[slot]
        )

    xrow = pl.ds(pl.multiple_of(x * BLK, BLK), BLK)
    lw = pltpu.make_async_copy(up, wu.at[xrow, :], sem("lwu"))
    lw.start()
    ld = pltpu.make_async_copy(down, wd.at[:, xrow], sem("lwd"))

    cols_of = [
        [pl.ds(pl.multiple_of((xb * 4 + zr[d]) * BLK, BLK), BLK) for d in range(4)]
        for xb in range(4)
    ]

    def hcols(xb, d):
        return cols_of[xb][d]

    cx[...] = jnp.zeros_like(cx)
    cz[...] = jnp.zeros_like(cz)
    st[...] = jnp.zeros_like(st)
    ssb[...] = jnp.zeros_like(ssb)

    bar = pltpu.get_barrier_semaphore()
    peers = []
    for d in (1, 2, 3):
        peers.append(dev(p, xr[d], z, y))
        peers.append(dev(p, x, zr[d], y))
        peers.append(dev(p, x, z, yr[d]))
    for d in range(4):
        peers.append(dev(other, x, z, yr[d]))
    for peer in peers:
        pl.semaphore_signal(bar, inc=1, device_id=peer, device_id_type=pl.DeviceIdType.MESH)
    with jax.named_scope("barrier"):
        pl.semaphore_wait(bar, len(peers))

    items = [("u", c) for c in range(NC)] + [("d", c) for c in range(NC)]

    def own_weights(i):
        kind, c = items[i]
        o, w = CHUNKS[c]
        if kind == "u":
            src = up.at[:, pl.ds(o, w)]
            dst = wu.at[xrow, pl.ds(o, w)]
        else:
            src = down.at[pl.ds(o, w), :]
            dst = wd.at[pl.ds(o, w), xrow]
        return src, dst

    def wslice(i, xb, part=None):
        kind, c = items[i]
        o, w = CHUNKS[c]
        if kind == "u":
            n = BLK if part is None else BLK // 2
            s = xb * BLK + (0 if part is None else part * (BLK // 2))
            return wu.at[pl.ds(pl.multiple_of(s, n), n), pl.ds(o, w)]
        n = w if part is None else w // 2
        s = o + (0 if part is None else part * (w // 2))
        return wd.at[pl.ds(s, n), pl.ds(pl.multiple_of(xb * BLK, BLK), BLK)]

    def weights_own(i, cond=None):
        _, dst = own_weights(i)
        src = lambda: own_weights(i)[0]
        if cond is None:
            src = src()
        send(src, dst, ("w", i, 0), dev(p, xp, z, y), cond)
        send(src, dst, ("w", i, 1), dev(p, xm, z, y), cond)

    def weights_forward(i, cond):
        @pl.when(cond)
        def _():
            wait(wslice(i, xm), ("w", i, 0))
            a = lambda: wslice(i, xm, 0)
            send(a, a(), ("w", i, 2), dev(p, xp, z, y), cond)
            wait(wslice(i, xp), ("w", i, 1))
            b = lambda: wslice(i, xp, 1)
            send(b, b(), ("w", i, 3), dev(p, xm, z, y), cond)
            if cond is first and i == 0:
                for k in range(2, AHEAD):
                    weights_own(k, cond)
            if i + AHEAD < len(items):
                weights_own(i + AHEAD, cond)
            if cond is first and i == len(items) - 1 - GATE:
                pl.semaphore_signal(gate, inc=1, device_id=dev(1, x, z, y),
                                    device_id_type=pl.DeviceIdType.MESH)

    def weights_last(i):
        wait(wslice(i, x2, 0), ("w", i, 2))
        wait(wslice(i, x2, 1), ("w", i, 3))

    def far_tokens(h):
        for xb in range(4):
            part = slice(None) if h == 0 else y
            send(
                lambda h=h, xb=xb, part=part: hs.at[h, part, :, hcols(xb, 2)],
                xt.at[h, part, z, :, pl.ds(xb * BLK, BLK)],
                ("x", h, 2, xb), dev(0, x, z2, y), first,
            )

    def near_tokens(h):
        for d in (1, 3):
            for xb in range(4):
                send(
                    lambda h=h, d=d, xb=xb: hs.at[h, :, :, hcols(xb, d)],
                    xt.at[h, :, z, :, pl.ds(xb * BLK, BLK)],
                    ("x", h, d, xb), dev(0, x, zr[d], y), first,
                )
        for xb in range(4):
            pltpu.make_async_copy(
                hs.at[h, :, :, hcols(xb, 0)], xt.at[h, :, z, :, pl.ds(xb * BLK, BLK)],
                sem(("xl", h, xb)),
            ).start()

    def near_later(h):
        @pl.when(first)
        def _():
            near_tokens(h)

    @pl.when(first)
    def _():
        weights_own(0, first)
        weights_own(1, first)
        far_tokens(0)
        near_tokens(0)
        for h in range(1, NH):
            far_tokens(h)

    own = jnp.sum(mask[...].astype(f32), axis=1, keepdims=True)
    cx[x, 0:4, :] = jnp.broadcast_to(own, (4, 128))
    for d in (1, 2, 3):
        send(cx.at[x], cx.at[x], ("cx", d), dev(p, xr[d], z, y))

    @pl.when(second)
    def _():
        pl.semaphore_wait(gate, 1)
        for i in range(AHEAD):
            weights_own(i, second)

    gz = jnp.concatenate([lgain[:, hcols(xb, 0)] for xb in range(4)], axis=1)

    def tile_arrived(h):
        @pl.when(first)
        def _():
            for xb in range(4):
                pltpu.make_async_copy(
                    hs.at[h, :, :, hcols(xb, 0)], xt.at[h, :, z, :, pl.ds(xb * BLK, BLK)],
                    sem(("xl", h, xb)),
                ).wait()
            for d in (1, 3):
                zs = zr[(4 - d) % 4]
                for xb in range(4):
                    wait(xt.at[h, :, zs, :, pl.ds(xb * BLK, BLK)], ("x", h, d, xb))
            if h == 0:
                for xb in range(4):
                    wait(xt.at[h, :, z2, :, pl.ds(xb * BLK, BLK)], ("x", h, 2, xb))
            else:
                for d in (1, 3, 2):
                    wait(xt.at[h, yr[(4 - d) % 4], z2], ("xy", h, d))

        @pl.when(second)
        def _():
            for e in range(NS):
                es = pl.ds(e * SUB, SUB)
                wait(xt.at[h, y, :, :, es], ("g", h, e, 2))
                wait(xt.at[h, y2, 0:2, :, es], ("g", h, e, 3))
                wait(xt.at[h, y2, 2:4, :, es], ("g", h, e, 4))

    def tile_relay_first(h):
        @pl.when(first)
        def _():
            for xb in range(4):
                wait(xt.at[h, y, z2, :, pl.ds(xb * BLK, BLK)], ("x", h, 2, xb))
            a = lambda: xt.at[h, y, z2]
            for d in (1, 3, 2):
                send(a, a(), ("xy", h, d), dev(0, x, z, yr[d]), first)

    def tile_relay(h):
        @pl.when(second)
        def _():
            for e in range(NS):
                es = pl.ds(e * SUB, SUB)
                wait(xt.at[h, ym, :, :, es], ("g", h, e, 0))
                a = lambda es=es: xt.at[h, ym, 0:2, :, es]
                send(a, a(), ("g", h, e, 3), dev(1, x, z, yq), second)
                wait(xt.at[h, yq, :, :, es], ("g", h, e, 1))
                b = lambda es=es: xt.at[h, yq, 2:4, :, es]
                send(b, b(), ("g", h, e, 4), dev(1, x, z, ym), second)

    def tile_ready(h):
        tile_arrived(h)
        ones = jnp.ones((8, TILE_D), bf16)
        for g in range(4):
            v = xt[h, :, g].reshape(4 * R, TILE_D).astype(f32)
            xg[h, :, g] = (v * gz).astype(bf16).reshape(4, R, TILE_D)
            sq = v * v
            hi = sq.astype(bf16)
            lo = (sq - hi.astype(f32)).astype(bf16)
            dn = (((1,), (1,)), ((), ()))
            ssb[h, g, :, 0 : 4 * R] = lax.dot_general(
                ones, hi, dn, preferred_element_type=f32
            ) + lax.dot_general(ones, lo, dn, preferred_element_type=f32)
        for d in (1, 3, 2):
            zt = zr[d]
            send(ssb.at[h, zt], ssr.at[h, d - 1], ("ss", h, d), dev(p, x, zt, y))

    def row_scale(h):
        for d in (1, 3, 2):
            wait(ssr.at[h, d - 1], ("ss", h, d))
        total = ssb[h, z] + ssr[h, 0] + ssr[h, 1] + ssr[h, 2]
        scale = lax.rsqrt(total * (1.0 / D) + epsilon)
        col = jnp.transpose(scale, (1, 0))[0 : 4 * R, 0:1]
        rcol[h] = jnp.broadcast_to(col, (4 * R, 128))

    def up_chunk(h, c):
        o, w = CHUNKS[c]
        lhs = xg[h].reshape(16 * R, TILE_D)
        r = jnp.dot(lhs, wu[:, o : o + w], preferred_element_type=f32)
        pp[h, :, :, :, o : o + w] = r.astype(bf16).reshape(4, 4, R, w)
        cs = pl.ds(o, w)
        send(pp.at[h, 0:2, z2, :, cs], rz1.at[h, 0, :, :, cs], ("z1", h, c, 0), dev(p, x, zp, y))
        send(pp.at[h, 2:4, z2, :, cs], rz1.at[h, 1, :, :, cs], ("z1", h, c, 1), dev(p, x, zm, y))
        send(pp.at[h, 2:4, zp, :, cs], rz2.at[h, 0, 2:4, :, cs], ("z2", h, c, 0), dev(p, x, zp, y))
        send(pp.at[h, 0:2, zm, :, cs], rz2.at[h, 1, 0:2, :, cs], ("z2", h, c, 1), dev(p, x, zm, y))

    def reduce_one(h, c):
        o, w = CHUNKS[c]
        cs = pl.ds(o, w)
        wait(rz1.at[h, 0, :, :, cs], ("z1", h, c, 0))
        pp[h, 0:2, zp, :, cs] = (
            pp[h, 0:2, zp, :, cs].astype(f32) + rz1[h, 0, :, :, cs].astype(f32)
        ).astype(bf16)
        send(pp.at[h, 0:2, zp, :, cs], rz2.at[h, 0, 0:2, :, cs], ("z2", h, c, 2), dev(p, x, zp, y))
        wait(rz1.at[h, 1, :, :, cs], ("z1", h, c, 1))
        pp[h, 2:4, zm, :, cs] = (
            pp[h, 2:4, zm, :, cs].astype(f32) + rz1[h, 1, :, :, cs].astype(f32)
        ).astype(bf16)
        send(pp.at[h, 2:4, zm, :, cs], rz2.at[h, 1, 2:4, :, cs], ("z2", h, c, 3), dev(p, x, zm, y))

    def reduce_two(h, c):
        o, w = CHUNKS[c]
        cs = pl.ds(o, w)
        if c == 0:
            row_scale(h)
        wait(rz2.at[h, 0, 2:4, :, cs], ("z2", h, c, 0))
        wait(rz2.at[h, 1, 0:2, :, cs], ("z2", h, c, 1))
        wait(rz2.at[h, 0, 0:2, :, cs], ("z2", h, c, 2))
        wait(rz2.at[h, 1, 2:4, :, cs], ("z2", h, c, 3))
        s = (
            pp[h, :, z, :, cs].astype(f32)
            + rz2[h, 0, :, :, cs].astype(f32)
            + rz2[h, 1, :, :, cs].astype(f32)
        ).reshape(4 * R, w)
        v = s * rcol[h][:, 0:1]
        act = v / (1.0 + jnp.exp(-v))
        ag[h, :, z, :, cs] = act.astype(bf16).reshape(4, R, w)
        a = ag.at[h, :, z, :, cs]
        send(a, a, ("a", h, c, 0), dev(p, x, zp, y))
        send(a, a, ("a", h, c, 1), dev(p, x, zm, y))

    def gather_one(h, c):
        o, w = CHUNKS[c]
        cs = pl.ds(o, w)
        wait(ag.at[h, :, zm, :, cs], ("a", h, c, 0))
        a = ag.at[h, 0:2, zm, :, cs]
        send(a, a, ("a", h, c, 2), dev(p, x, zp, y))
        wait(ag.at[h, :, zp, :, cs], ("a", h, c, 1))
        b = ag.at[h, 2:4, zp, :, cs]
        send(b, b, ("a", h, c, 3), dev(p, x, zm, y))

    def down_arrived(h, c):
        cs = pl.ds(*CHUNKS[c])
        wait(ag.at[h, 0:2, z2, :, cs], ("a", h, c, 2))
        wait(ag.at[h, 2:4, z2, :, cs], ("a", h, c, 3))

    def down_chunk(h, c, e=None):
        o, w = CHUNKS[c]
        cs = pl.ds(o, w)
        if e is None:
            down_arrived(h, c)
        lhs = ag[h, :, :, :, cs].reshape(16 * R, w)
        for n in range(0 if e is None else e * SUB, TILE_D if e is None else (e + 1) * SUB, 256):
            r = jnp.dot(lhs, wd[cs, n : n + 256], preferred_element_type=f32)
            if c > 0:
                r = r + yacc[h, :, n : n + 256]
            if c == NC - 1:
                yp[h, :, :, :, n : n + 256] = r.astype(bf16).reshape(4, 4, R, 256)
            else:
                yacc[h, :, n : n + 256] = r

    def y_start(h, e):
        es = pl.ds(e * SUB, SUB)
        send(yp.at[h, y2, 0:2, :, es], ry1.at[h, 0, :, :, es], ("y1", h, e, 0), dev(p, x, z, yq))
        send(yp.at[h, y2, 2:4, :, es], ry1.at[h, 1, :, :, es], ("y1", h, e, 1), dev(p, x, z, ym))
        send(yp.at[h, yq, 2:4, :, es], ry2.at[h, 0, 2:4, :, es], ("y2", h, e, 0), dev(p, x, z, yq))
        send(yp.at[h, ym, 0:2, :, es], ry2.at[h, 1, 0:2, :, es], ("y2", h, e, 1), dev(p, x, z, ym))

    def y_mid(h, e):
        es = pl.ds(e * SUB, SUB)
        wait(ry1.at[h, 0, :, :, es], ("y1", h, e, 0))
        yp[h, yq, 0:2, :, es] = (
            yp[h, yq, 0:2, :, es].astype(f32) + ry1[h, 0, :, :, es].astype(f32)
        ).astype(bf16)
        send(lambda: yp.at[h, yq, 0:2, :, es], ry2.at[h, 0, 0:2, :, es], ("y2", h, e, 2), dev(p, x, z, yq))
        wait(ry1.at[h, 1, :, :, es], ("y1", h, e, 1))
        yp[h, ym, 2:4, :, es] = (
            yp[h, ym, 2:4, :, es].astype(f32) + ry1[h, 1, :, :, es].astype(f32)
        ).astype(bf16)
        send(lambda: yp.at[h, ym, 2:4, :, es], ry2.at[h, 1, 2:4, :, es], ("y2", h, e, 3), dev(p, x, z, ym))

    def y_end(h, e):
        es = pl.ds(e * SUB, SUB)
        wait(ry2.at[h, 0, 2:4, :, es], ("y2", h, e, 0))
        wait(ry2.at[h, 1, 0:2, :, es], ("y2", h, e, 1))
        wait(ry2.at[h, 0, 0:2, :, es], ("y2", h, e, 2))
        wait(ry2.at[h, 1, 2:4, :, es], ("y2", h, e, 3))
        sh[h, :, :, es] = (
            xt[h, y, :, :, es].astype(f32)
            + yp[h, y, :, :, es].astype(f32)
            + ry2[h, 0, :, :, es].astype(f32)
            + ry2[h, 1, :, :, es].astype(f32)
        ).astype(bf16)

        @when(first)
        def _():
            dst = xt.at[h, y, :, :, es]
            src = lambda: sh.at[h, :, :, es]
            send(src, dst, ("g", h, e, 0), dev(1, x, z, yq), first)
            send(src, dst, ("g", h, e, 1), dev(1, x, z, ym), first)
            send(src, dst, ("g", h, e, 2), dev(1, x, z, y), first)

        @when(second)
        def _():
            for d in (1, 3, 2):
                for xb in range(e * XB, (e + 1) * XB):
                    send(
                        lambda d=d, xb=xb: sh.at[h, zr[d], :, pl.ds(xb * BLK, BLK)],
                        xf.at[h, y, :, hcols(xb, 0)],
                        ("f", h, d, xb), dev(1, x, zr[d], y), second,
                    )
            for xb in range(e * XB, (e + 1) * XB):
                xf[h, y, :, hcols(xb, 0)] = sh[h, z, :, xb * BLK : (xb + 1) * BLK]

    FW = D // NS

    def fcols(e, part=None):
        if part is None:
            return pl.ds(e * FW, FW)
        return pl.ds(e * FW + part * (FW // 2), FW // 2)

    def finals_one(h, e):
        @when(second)
        def _():
            for d in (1, 3, 2):
                for xb in range(e * XB, (e + 1) * XB):
                    wait(xf.at[h, y, :, hcols(xb, (4 - d) % 4)], ("f", h, d, xb))
            a = lambda: xf.at[h, y, :, fcols(e)]
            send(a, a(), ("q", h, e, 0), dev(1, x, z, yq), second)
            send(a, a(), ("q", h, e, 1), dev(1, x, z, ym), second)
            send(a, a(), ("q", h, e, 4), dev(0, x, z, y), second)

    def finals_two(h, e):
        @when(second)
        def _():
            wait(xf.at[h, ym, :, fcols(e)], ("q", h, e, 0))
            a = lambda: xf.at[h, ym, :, fcols(e, 0)]
            send(a, a(), ("q", h, e, 2), dev(1, x, z, yq), second)
            wait(xf.at[h, yq, :, fcols(e)], ("q", h, e, 1))
            b = lambda: xf.at[h, yq, :, fcols(e, 1)]
            send(b, b(), ("q", h, e, 3), dev(1, x, z, ym), second)
            a2 = lambda: xf.at[h, ym, :, fcols(e)]
            send(a2, a2(), ("q", h, e, 5), dev(0, x, z, y), second)
            b2 = lambda: xf.at[h, yq, :, fcols(e)]
            send(b2, b2(), ("q", h, e, 6), dev(0, x, z, y), second)

    def finals_three(h, e):
        @when(second)
        def _():
            wait(xf.at[h, y2, :, fcols(e, 0)], ("q", h, e, 2))
            wait(xf.at[h, y2, :, fcols(e, 1)], ("q", h, e, 3))
            a = lambda: xf.at[h, y2, :, fcols(e)]
            send(a, a(), ("q", h, e, 7), dev(0, x, z, y), second)

    def finals_here(h):
        @pl.when(first)
        def _():
            for e in range(NS):
                wait(xf.at[h, y, :, fcols(e)], ("q", h, e, 4))
                wait(xf.at[h, ym, :, fcols(e)], ("q", h, e, 5))
                wait(xf.at[h, yq, :, fcols(e)], ("q", h, e, 6))
                wait(xf.at[h, y2, :, fcols(e)], ("q", h, e, 7))

    def final_norm(h, cond):
        def work():
            for q in range(4):
                v = xf[h, q].astype(f32)
                r = lax.rsqrt(jnp.mean(v * v, axis=1, keepdims=True) + epsilon)
                xn[pl.ds((h * 4 + q) * R, R), :] = (v * r * fgain[...]).astype(bf16)

        if cond is None:
            work()
        else:
            pl.when(cond)(work)

    steps = [(h, c) for c in range(NC) for h in range(2)]
    steps += [(h, c) for h in range(2, NH) for c in range(NC)]
    with jax.named_scope("local_weights"):
        ld.start()
        lw.wait()

    n = len(steps)
    slots = {}

    def prefetch(a, b):
        for k in range(a, b):
            ucopy(k).start()


    def at(slot, prio, fn, *args):
        entry = (prio, len(slots.get(slot, ())), fn, args, None)
        slots.setdefault(slot, []).append(entry)

    def at_core(core, slot, prio, fn, *args):
        entry = (prio, len(slots.get(slot, ())), fn, args, core)
        slots.setdefault(slot, []).append(entry)

    for k in range(PRE):
        at(-1, 0, weights_forward, k, second)
    at(-1, 1, near_later, 1)
    at(0, 1, tile_relay_first, 1)
    at(3, 8, ld.wait)
    at(3, 9, prefetch, 0, NSLOT)
    at(-1, 1, tile_relay, 0)
    at(1, 9, tile_relay, 1)
    for h in range(2, NH):
        at(h, 3, near_later, h)
        at(h + 2, 3, tile_relay_first, h)
        at(steps.index((h, 0)) - 1, 9, tile_relay, h)
    for k in range(2 * NC):
        at(WF_SLOT[k], 0 if k == 0 else 2, weights_forward, k, first)
    for k in range(PRE, 2 * NC):
        at(1 + 2 * (k - PRE), 2, weights_forward, k, second)
    last = {}
    for i, (h, c) in enumerate(steps):
        u = i + 1
        if h == 0:
            at(u, 2, weights_last, c)
        if c == 0:
            at(u, 2, tile_ready, h)
        at(u, 2, up_chunk, h, c)
        stage = [u + k * LAG for k in range(1, 5)]
        if h >= NH - 2:
            end = steps.index((h, NC - 1)) + 1
            cap = END[h - NH + 2]
            stage = [min(t, end + d) for t, d in zip(stage, cap)]
        at(stage[0], 3, reduce_one, h, c)
        at(stage[1], 4, reduce_two, h, c)
        at(stage[2], 5, gather_one, h, c)
        slot = max(stage[3], WF_SLOT[NC + c] + 2 + h)
        if h == 0:
            at(slot, 6, weights_last, NC + c)
        if c < NC - 1 or NS == 1:
            at(slot, 6, down_chunk, h, c)
        else:
            at(slot, 6, down_arrived, h, c)
        if c == NC - 1:
            for e in range(NS):
                if NS > 1:
                    at(slot, 7, down_chunk, h, c, e)
                at(slot, 7, y_start, h, e)
        last[h] = slot
    for h in range(NH):
        slot = last[h]
        at_core(first, slot + 1, 2.5, y_mid, h, 0)
        at_core(first, slot + 2, 2.5, y_end, h, 0)
        fns = (y_mid, y_end, finals_one, finals_two, finals_three)
        for lag, fn in zip(LAGS[h], fns):
            early = h == NH - 2 and fn is y_mid
            at_core(second, slot + lag, 5.5 if early else ORDER[h], fn, h, 0)
        if h < NH - 1:
            at(slot + LAGS[h][-1], 13, final_norm, h, second)
    end = max(slots) + 1
    for h in range(NH):
        at(end, h, finals_here, h)
        if h < NH - 1:
            at(end, h, final_norm, h, first)
        else:
            at(end, h, final_norm, h, None)
    for slot in sorted(slots):
        for _, _, fn, args, core in sorted(slots[slot], key=lambda e: e[:2]):
            with jax.named_scope(getattr(fn, "__name__", "copy")):
                if core is None:
                    fn(*args)
                else:
                    turn[0] = core
                    pl.when(core)(lambda: fn(*args))
                    turn[0] = None

    for d in (1, 2, 3):
        wait(cx.at[xr[(4 - d) % 4]], ("cx", d))
    cz[z] = cx[0] + cx[1] + cx[2] + cx[3]
    for d in (1, 2, 3):
        send(cz.at[z], cz.at[z], ("cz", d), dev(p, x, zr[d], y))

    vocab_index = p * 4 + y
    lanes = lax.broadcasted_iota(jnp.int32, (64, 256), 1)
    spread = (lanes % 64 == lax.broadcasted_iota(jnp.int32, (64, 256), 0)).astype(bf16)
    own_row = lax.broadcasted_iota(jnp.int32, (8, 256), 1) // 64 == lax.broadcasted_iota(
        jnp.int32, (8, 256), 0
    )

    def to_row(v):
        r = jnp.dot(v, spread, preferred_element_type=f32)
        return jnp.sum(jnp.where(own_row, r, 0.0), axis=0, keepdims=True)

    idp = jnp.concatenate([ids[...], jnp.zeros((4, 64), jnp.int32)], axis=0)
    high = to_row((idp // 256).astype(f32).astype(bf16))
    low = to_row((idp % 256).astype(f32).astype(bf16))
    id_row = (high * 256.0 + low).astype(jnp.int32) - vocab_index * V_DEV

    m_s[...] = jnp.full_like(m_s, -jnp.inf)
    s_s[...] = jnp.zeros_like(s_s)
    k_s[...] = jnp.zeros_like(k_s)

    def head(k, carry):
        slot = lax.rem(k, NSLOT)
        ucopy(k).wait()
        lt = lax.dot_general(
            ub[slot], xn[...], (((1,), (1,)), ((), ())), preferred_element_type=f32
        )
        m_old = m_s[...]
        m_new = jnp.maximum(m_old, jnp.max(lt, axis=0, keepdims=True))
        rows = lax.broadcasted_iota(jnp.int32, lt.shape, 0) + k * UROWS
        k_s[...] = k_s[...] + jnp.sum(jnp.where(rows == id_row, lt, 0.0), axis=0, keepdims=True)
        s_s[...] = s_s[...] * jnp.exp(m_old - m_new) + jnp.sum(
            jnp.exp(lt - m_new), axis=0, keepdims=True
        )
        m_s[...] = m_new

        @pl.when(k + NSLOT < NU)
        def _():
            ucopy(k + NSLOT).start()

        return carry

    with jax.named_scope("head"):
        lax.fori_loop(0, NU, head, 0)

    st[vocab_index, 0:1] = m_s[...]
    st[vocab_index, 1:2] = s_s[...]
    st[vocab_index, 2:3] = k_s[...]
    mine = st.at[vocab_index]
    for d in range(4):
        yt = yr[d]
        if d > 0:
            send(mine, mine, ("st", 0, d), dev(p, x, z, yt))
        send(mine, mine, ("st", 1, d), dev(other, x, z, yt))
    stat = jax.named_scope("stats_wait")
    stat.__enter__()
    for d in range(4):
        ys = yr[(4 - d) % 4]
        if d > 0:
            wait(st.at[p * 4 + ys], ("st", 0, d))
        wait(st.at[other * 4 + ys], ("st", 1, d))
    stat.__exit__(None, None, None)
    ms = [st[i, 0:1] for i in range(8)]
    top = ms[0]
    for i in range(1, 8):
        top = jnp.maximum(top, ms[i])
    tot = jnp.zeros_like(top)
    pick = jnp.zeros_like(top)
    for i in range(8):
        tot = tot + st[i, 1:2] * jnp.exp(ms[i] - top)
        pick = pick + st[i, 2:3]
    row = pick - top - jnp.log(tot)
    for d in (1, 2, 3):
        wait(cz.at[zr[(4 - d) % 4]], ("cz", d))
    counts = (cz[0] + cz[1] + cz[2] + cz[3])[0:4, 0:1]
    divisor = counts / 16.0
    mv = mask[...].astype(f32)
    tok = jnp.concatenate([row[:, 64 * i : 64 * i + 64] for i in range(4)], axis=0)
    policy = jnp.sum(mv * tok, axis=1, keepdims=True) / divisor
    gaps = policy - jnp.sum(mv * anchor[...], axis=1, keepdims=True) / divisor
    place = lax.broadcasted_iota(jnp.int32, (4, 1), 0)
    side = lax.broadcasted_iota(jnp.int32, (4, 64), 1)
    extra = jnp.broadcast_to(policy, (4, 64))
    for i in range(2):
        chosen = jnp.sum(jnp.where(place == pairing[0, 2 * i], gaps, 0.0))
        rejected = jnp.sum(jnp.where(place == pairing[0, 2 * i + 1], gaps, 0.0))
        diff = chosen - rejected - 0.5 / ipo_tau
        extra = jnp.where(side == i + 1, diff * diff, extra)
    out[0:4, :] = jnp.concatenate([tok, extra], axis=1)
    out[4:8, :] = jnp.zeros((4, 128), f32)

    for src, ssem, cond in pending:
        if cond is None:
            ref = src() if callable(src) else src
            pltpu.make_async_copy(ref, ref, sem(ssem)).wait()
    for which in (first, second):
        @pl.when(which)
        def _():
            for src, ssem, cond in pending:
                if cond is which:
                    ref = src()
                    pltpu.make_async_copy(ref, ref, sem(ssem)).wait()


def run(hs, up, down, lgain, fgain, unemb, ids, mask, anchor, pairing):
    anyspace = pl.BlockSpec(memory_space=pltpu.HBM)
    vm = pl.BlockSpec(memory_space=pltpu.VMEM)
    sm = pl.BlockSpec(memory_space=pltpu.SMEM)
    V = pltpu.VMEM
    return pl.pallas_call(
        body,
        out_shape=(
            jax.ShapeDtypeStruct((8, 128), f32)
        ),
        in_specs=[anyspace, anyspace, anyspace, vm, vm, anyspace, vm, vm, vm, sm],
        out_specs=vm,
        scratch_shapes=[
            V((TILE_D, FF_DEV), bf16),
            V((FF_DEV, TILE_D), bf16),
            V((NH, 4, 4, R, TILE_D), bf16),
            V((NH, 4, 4, R, TILE_D), bf16),
            V((NH, 4, 4, R, FF_DEV), bf16),
            V((NH, 2, 2, R, FF_DEV), bf16),
            V((NH, 2, 4, R, FF_DEV), bf16),
            V((NH, 4, 4, R, FF_DEV), bf16),
            V((NH, 16 * R, TILE_D), f32),
            V((NH, 4, 4, R, TILE_D), bf16),
            V((NH, 2, 2, R, TILE_D), bf16),
            V((NH, 2, 4, R, TILE_D), bf16),
            V((NH, 4, R, TILE_D), bf16),
            V((NH, 4, R, D), bf16),
            V((256, D), bf16),
            V((NSLOT, UROWS, D), bf16),
            V((NH, 4, 8, 128), f32),
            V((NH, 3, 8, 128), f32),
            V((NH, 4 * R, 128), f32),
            V((8, 8, 256), f32),
            V((4, 8, 128), f32),
            V((4, 8, 128), f32),
            V((1, 256), f32),
            V((1, 256), f32),
            V((1, 256), f32),
            pltpu.SemaphoreType.DMA((NSEM,)),
            pltpu.SemaphoreType.DMA((NSLOT,)),
            pltpu.SemaphoreType.REGULAR,
        ],
        compiler_params=pltpu.CompilerParams(
            collective_id=0, has_side_effects=True, vmem_limit_bytes=66_000_000
        ),
        name="relay",
    )(hs, up, down, lgain, fgain, unemb, ids, mask, anchor, pairing)


def unpack(rows, tok, policy, losses):
    tok[...] = rows[0:4, 0:64]
    for i in range(4):
        policy[i] = rows[i, 64]
    for i in range(2):
        losses[i] = rows[0, 65 + i]


def shards(
    hidden_states, up_weight, down_weight, layer_gain, final_gain, unembedding,
    target_ids, response_masks, anchor_logps, pairing,
):
    out = run(
        hidden_states.reshape(NH, 4, R, D),
        up_weight[0],
        down_weight[0],
        layer_gain,
        final_gain.reshape(1, D),
        unembedding,
        target_ids,
        response_masks,
        anchor_logps,
        pairing,
    )
    vm = pl.BlockSpec(memory_space=pltpu.VMEM)
    sm = pl.BlockSpec(memory_space=pltpu.SMEM)
    return pl.pallas_call(
        unpack,
        out_shape=(
            jax.ShapeDtypeStruct((4, 64), f32),
            jax.ShapeDtypeStruct((4,), f32),
            jax.ShapeDtypeStruct((2,), f32),
        ),
        in_specs=[vm],
        out_specs=(vm, sm, sm),
        name="unpack",
    )(out)


def solution(mesh):
    return jax.shard_map(
        shards,
        mesh=mesh,
        in_specs=(
            P("dp", None, None),
            P("pipe", "dp", "mp"),
            P("pipe", "mp", "dp"),
            P("pipe", None),
            P(),
            P(("pipe", "mp"), None),
            P("dp", None),
            P("dp", None),
            P("dp", None),
            P("dp", None),
        ),
        out_specs=(P("dp", None), P("dp"), P("dp")),
        check_vma=False,
    )
```

```python
import jax
import jax.numpy as jnp
from jax import lax
from jax.experimental import pallas as pl
from jax.experimental.pallas import tpu as pltpu
from jax.sharding import PartitionSpec as P

epsilon = 1e-05
ipo_tau = 0.5

NX, NY, NZ = 4, 4, 4
D = 4096
FF_DEV = 1792
BLK = 256
TILE_D = 4 * BLK
NH = 4
R = 32 // (NH // 2)
AHEAD = 2
END = ((2, 3, 4, 6), (1, 2, 3, 4))
LAGS = ((2, 4, 6, 7, 8), (2, 4, 5, 6, 7), (2, 3, 4, 5, 6), (1, 2, 3, 4, 5))
ORDER = (8, 8.1, 7.9, 7.5)
WF_SLOT = (-1, 0, 2, 4, 6, 8, 10, 12)
GATE = 0
PRE = 4
CHUNKS = ((0, 384), (384, 512), (896, 512), (1408, 384))
LAG = 2
NC = len(CHUNKS)
UROWS = 1024
NSLOT = 3
V_DEV = 4096
NU = V_DEV // UROWS
NS = 1
SUB = TILE_D // NS
XB = 4 // NS
NSEM = 1200

f32 = jnp.float32
bf16 = jnp.bfloat16


def body(
    hs, up, down, lgain, fgain, unemb, ids, mask, anchor, pairing,
    out,
    wu, wd, xt, xg, pp, rz1, rz2, ag, yacc, yp, ry1, ry2, sh, xf, xn, ub,
    ssb, ssr, rcol, st, cx, cz, m_s, s_s, k_s,
    sems, usem, gate,
):
    p = lax.axis_index("pipe")
    dp = lax.axis_index("dp")
    y = lax.axis_index("mp")
    x = lax.div(dp, 4)
    z = lax.rem(dp, 4)

    def wrap(v):
        return lax.rem(v + 4, 4)

    xr = [wrap(x + d) for d in range(4)]
    yr = [wrap(y + d) for d in range(4)]
    zr = [wrap(z + d) for d in range(4)]

    def dev(pi, xi, zi, yi):
        return {"pipe": pi, "dp": xi * 4 + zi, "mp": yi}

    names = {}

    def sem(key):
        if key not in names:
            assert len(names) < NSEM
            names[key] = len(names)
        return sems.at[names[key]]

    pending = []
    recorded = set()
    turn = [None]

    def when(core):
        if turn[0] is None:
            return pl.when(core)
        return (lambda fn: fn()) if turn[0] is core else (lambda fn: None)

    def send(src, dst, key, to, cond=None):
        cp = pltpu.make_async_remote_copy(
            src_ref=src() if callable(src) else src, dst_ref=dst, send_sem=sem(("s", key)), recv_sem=sem(("r", key)),
            device_id=to, device_id_type=pl.DeviceIdType.MESH,
        )
        cp.start()
        if (key, id(cond)) not in recorded:
            recorded.add((key, id(cond)))
            pending.append((src, ("s", key), cond))

    def wait(dst, key):
        pltpu.make_async_copy(dst, dst, sem(("r", key))).wait()

    xp, xm, x2 = xr[1], xr[3], xr[2]
    zp, zm, z2 = zr[1], zr[3], zr[2]
    yq, ym, y2 = yr[1], yr[3], yr[2]
    other = 1 - p
    first = p == 0
    second = p == 1

    def ucopy(k):
        slot = lax.rem(k, NSLOT)
        return pltpu.make_async_copy(
            unemb.at[pl.ds(k * UROWS, UROWS)], ub.at[slot], usem.at[slot]
        )

    xrow = pl.ds(pl.multiple_of(x * BLK, BLK), BLK)
    lw = pltpu.make_async_copy(up, wu.at[xrow, :], sem("lwu"))
    lw.start()
    ld = pltpu.make_async_copy(down, wd.at[:, xrow], sem("lwd"))

    cols_of = [
        [pl.ds(pl.multiple_of((xb * 4 + zr[d]) * BLK, BLK), BLK) for d in range(4)]
        for xb in range(4)
    ]

    def hcols(xb, d):
        return cols_of[xb][d]

    cx[...] = jnp.zeros_like(cx)
    cz[...] = jnp.zeros_like(cz)
    st[...] = jnp.zeros_like(st)
    ssb[...] = jnp.zeros_like(ssb)

    bar = pltpu.get_barrier_semaphore()
    peers = []
    for d in (1, 2, 3):
        peers.append(dev(p, xr[d], z, y))
        peers.append(dev(p, x, zr[d], y))
        peers.append(dev(p, x, z, yr[d]))
    for d in range(4):
        peers.append(dev(other, x, z, yr[d]))
    for peer in peers:
        pl.semaphore_signal(bar, inc=1, device_id=peer, device_id_type=pl.DeviceIdType.MESH)
    with jax.named_scope("barrier"):
        pl.semaphore_wait(bar, len(peers))

    items = [("u", c) for c in range(NC)] + [("d", c) for c in range(NC)]

    def own_weights(i):
        kind, c = items[i]
        o, w = CHUNKS[c]
        if kind == "u":
            src = up.at[:, pl.ds(o, w)]
            dst = wu.at[xrow, pl.ds(o, w)]
        else:
            src = down.at[pl.ds(o, w), :]
            dst = wd.at[pl.ds(o, w), xrow]
        return src, dst

    def wslice(i, xb, part=None):
        kind, c = items[i]
        o, w = CHUNKS[c]
        if kind == "u":
            n = BLK if part is None else BLK // 2
            s = xb * BLK + (0 if part is None else part * (BLK // 2))
            return wu.at[pl.ds(pl.multiple_of(s, n), n), pl.ds(o, w)]
        n = w if part is None else w // 2
        s = o + (0 if part is None else part * (w // 2))
        return wd.at[pl.ds(s, n), pl.ds(pl.multiple_of(xb * BLK, BLK), BLK)]

    def weights_own(i, cond=None):
        _, dst = own_weights(i)
        src = lambda: own_weights(i)[0]
        if cond is None:
            src = src()
        send(src, dst, ("w", i, 0), dev(p, xp, z, y), cond)
        send(src, dst, ("w", i, 1), dev(p, xm, z, y), cond)

    def weights_forward(i, cond):
        @pl.when(cond)
        def _():
            wait(wslice(i, xm), ("w", i, 0))
            a = lambda: wslice(i, xm, 0)
            send(a, a(), ("w", i, 2), dev(p, xp, z, y), cond)
            wait(wslice(i, xp), ("w", i, 1))
            b = lambda: wslice(i, xp, 1)
            send(b, b(), ("w", i, 3), dev(p, xm, z, y), cond)
            if cond is first and i == 0:
                for k in range(2, AHEAD):
                    weights_own(k, cond)
            if i + AHEAD < len(items):
                weights_own(i + AHEAD, cond)
            if cond is first and i == len(items) - 1 - GATE:
                pl.semaphore_signal(gate, inc=1, device_id=dev(1, x, z, y),
                                    device_id_type=pl.DeviceIdType.MESH)

    def weights_last(i):
        wait(wslice(i, x2, 0), ("w", i, 2))
        wait(wslice(i, x2, 1), ("w", i, 3))

    def far_tokens(h):
        for xb in range(4):
            part = slice(None) if h == 0 else y
            send(
                lambda h=h, xb=xb, part=part: hs.at[h, part, :, hcols(xb, 2)],
                xt.at[h, part, z, :, pl.ds(xb * BLK, BLK)],
                ("x", h, 2, xb), dev(0, x, z2, y), first,
            )

    def near_tokens(h):
        for d in (1, 3):
            for xb in range(4):
                send(
                    lambda h=h, d=d, xb=xb: hs.at[h, :, :, hcols(xb, d)],
                    xt.at[h, :, z, :, pl.ds(xb * BLK, BLK)],
                    ("x", h, d, xb), dev(0, x, zr[d], y), first,
                )
        for xb in range(4):
            pltpu.make_async_copy(
                hs.at[h, :, :, hcols(xb, 0)], xt.at[h, :, z, :, pl.ds(xb * BLK, BLK)],
                sem(("xl", h, xb)),
            ).start()

    def near_later(h):
        @pl.when(first)
        def _():
            near_tokens(h)

    @pl.when(first)
    def _():
        weights_own(0, first)
        weights_own(1, first)
        far_tokens(0)
        near_tokens(0)
        for h in range(1, NH):
            far_tokens(h)

    own = jnp.sum(mask[...].astype(f32), axis=1, keepdims=True)
    cx[x, 0:4, :] = jnp.broadcast_to(own, (4, 128))
    for d in (1, 2, 3):
        send(cx.at[x], cx.at[x], ("cx", d), dev(p, xr[d], z, y))

    @pl.when(second)
    def _():
        pl.semaphore_wait(gate, 1)
        for i in range(AHEAD):
            weights_own(i, second)

    gz = jnp.concatenate([lgain[:, hcols(xb, 0)] for xb in range(4)], axis=1)

    def tile_arrived(h):
        @pl.when(first)
        def _():
            for xb in range(4):
                pltpu.make_async_copy(
                    hs.at[h, :, :, hcols(xb, 0)], xt.at[h, :, z, :, pl.ds(xb * BLK, BLK)],
                    sem(("xl", h, xb)),
                ).wait()
            for d in (1, 3):
                zs = zr[(4 - d) % 4]
                for xb in range(4):
                    wait(xt.at[h, :, zs, :, pl.ds(xb * BLK, BLK)], ("x", h, d, xb))
            if h == 0:
                for xb in range(4):
                    wait(xt.at[h, :, z2, :, pl.ds(xb * BLK, BLK)], ("x", h, 2, xb))
            else:
                for d in (1, 3, 2):
                    wait(xt.at[h, yr[(4 - d) % 4], z2], ("xy", h, d))

        @pl.when(second)
        def _():
            for e in range(NS):
                es = pl.ds(e * SUB, SUB)
                wait(xt.at[h, y, :, :, es], ("g", h, e, 2))
                wait(xt.at[h, y2, 0:2, :, es], ("g", h, e, 3))
                wait(xt.at[h, y2, 2:4, :, es], ("g", h, e, 4))

    def tile_relay_first(h):
        @pl.when(first)
        def _():
            for xb in range(4):
                wait(xt.at[h, y, z2, :, pl.ds(xb * BLK, BLK)], ("x", h, 2, xb))
            a = lambda: xt.at[h, y, z2]
            for d in (1, 3, 2):
                send(a, a(), ("xy", h, d), dev(0, x, z, yr[d]), first)

    def tile_relay(h):
        @pl.when(second)
        def _():
            for e in range(NS):
                es = pl.ds(e * SUB, SUB)
                wait(xt.at[h, ym, :, :, es], ("g", h, e, 0))
                a = lambda es=es: xt.at[h, ym, 0:2, :, es]
                send(a, a(), ("g", h, e, 3), dev(1, x, z, yq), second)
                wait(xt.at[h, yq, :, :, es], ("g", h, e, 1))
                b = lambda es=es: xt.at[h, yq, 2:4, :, es]
                send(b, b(), ("g", h, e, 4), dev(1, x, z, ym), second)

    def tile_ready(h):
        tile_arrived(h)
        ones = jnp.ones((8, TILE_D), bf16)
        for g in range(4):
            v = xt[h, :, g].reshape(4 * R, TILE_D).astype(f32)
            xg[h, :, g] = (v * gz).astype(bf16).reshape(4, R, TILE_D)
            sq = v * v
            hi = sq.astype(bf16)
            lo = (sq - hi.astype(f32)).astype(bf16)
            dn = (((1,), (1,)), ((), ()))
            ssb[h, g, :, 0 : 4 * R] = lax.dot_general(
                ones, hi, dn, preferred_element_type=f32
            ) + lax.dot_general(ones, lo, dn, preferred_element_type=f32)
        for d in (1, 3, 2):
            zt = zr[d]
            send(ssb.at[h, zt], ssr.at[h, d - 1], ("ss", h, d), dev(p, x, zt, y))

    def row_scale(h):
        for d in (1, 3, 2):
            wait(ssr.at[h, d - 1], ("ss", h, d))
        total = ssb[h, z] + ssr[h, 0] + ssr[h, 1] + ssr[h, 2]
        scale = lax.rsqrt(total * (1.0 / D) + epsilon)
        col = jnp.transpose(scale, (1, 0))[0 : 4 * R, 0:1]
        rcol[h] = jnp.broadcast_to(col, (4 * R, 128))

    def up_chunk(h, c):
        o, w = CHUNKS[c]
        lhs = xg[h].reshape(16 * R, TILE_D)
        r = jnp.dot(lhs, wu[:, o : o + w], preferred_element_type=f32)
        pp[h, :, :, :, o : o + w] = r.astype(bf16).reshape(4, 4, R, w)
        cs = pl.ds(o, w)
        send(pp.at[h, 0:2, z2, :, cs], rz1.at[h, 0, :, :, cs], ("z1", h, c, 0), dev(p, x, zp, y))
        send(pp.at[h, 2:4, z2, :, cs], rz1.at[h, 1, :, :, cs], ("z1", h, c, 1), dev(p, x, zm, y))
        send(pp.at[h, 2:4, zp, :, cs], rz2.at[h, 0, 2:4, :, cs], ("z2", h, c, 0), dev(p, x, zp, y))
        send(pp.at[h, 0:2, zm, :, cs], rz2.at[h, 1, 0:2, :, cs], ("z2", h, c, 1), dev(p, x, zm, y))

    def reduce_one(h, c):
        o, w = CHUNKS[c]
        cs = pl.ds(o, w)
        wait(rz1.at[h, 0, :, :, cs], ("z1", h, c, 0))
        pp[h, 0:2, zp, :, cs] = (
            pp[h, 0:2, zp, :, cs].astype(f32) + rz1[h, 0, :, :, cs].astype(f32)
        ).astype(bf16)
        send(pp.at[h, 0:2, zp, :, cs], rz2.at[h, 0, 0:2, :, cs], ("z2", h, c, 2), dev(p, x, zp, y))
        wait(rz1.at[h, 1, :, :, cs], ("z1", h, c, 1))
        pp[h, 2:4, zm, :, cs] = (
            pp[h, 2:4, zm, :, cs].astype(f32) + rz1[h, 1, :, :, cs].astype(f32)
        ).astype(bf16)
        send(pp.at[h, 2:4, zm, :, cs], rz2.at[h, 1, 2:4, :, cs], ("z2", h, c, 3), dev(p, x, zm, y))

    def reduce_two(h, c):
        o, w = CHUNKS[c]
        cs = pl.ds(o, w)
        if c == 0:
            row_scale(h)
        wait(rz2.at[h, 0, 2:4, :, cs], ("z2", h, c, 0))
        wait(rz2.at[h, 1, 0:2, :, cs], ("z2", h, c, 1))
        wait(rz2.at[h, 0, 0:2, :, cs], ("z2", h, c, 2))
        wait(rz2.at[h, 1, 2:4, :, cs], ("z2", h, c, 3))
        s = (
            pp[h, :, z, :, cs].astype(f32)
            + rz2[h, 0, :, :, cs].astype(f32)
            + rz2[h, 1, :, :, cs].astype(f32)
        ).reshape(4 * R, w)
        v = s * rcol[h][:, 0:1]
        act = v / (1.0 + jnp.exp(-v))
        ag[h, :, z, :, cs] = act.astype(bf16).reshape(4, R, w)
        a = ag.at[h, :, z, :, cs]
        send(a, a, ("a", h, c, 0), dev(p, x, zp, y))
        send(a, a, ("a", h, c, 1), dev(p, x, zm, y))

    def gather_one(h, c):
        o, w = CHUNKS[c]
        cs = pl.ds(o, w)
        wait(ag.at[h, :, zm, :, cs], ("a", h, c, 0))
        a = ag.at[h, 0:2, zm, :, cs]
        send(a, a, ("a", h, c, 2), dev(p, x, zp, y))
        wait(ag.at[h, :, zp, :, cs], ("a", h, c, 1))
        b = ag.at[h, 2:4, zp, :, cs]
        send(b, b, ("a", h, c, 3), dev(p, x, zm, y))

    def down_arrived(h, c):
        cs = pl.ds(*CHUNKS[c])
        wait(ag.at[h, 0:2, z2, :, cs], ("a", h, c, 2))
        wait(ag.at[h, 2:4, z2, :, cs], ("a", h, c, 3))

    def down_chunk(h, c, e=None):
        o, w = CHUNKS[c]
        cs = pl.ds(o, w)
        if e is None:
            down_arrived(h, c)
        lhs = ag[h, :, :, :, cs].reshape(16 * R, w)
        for n in range(0 if e is None else e * SUB, TILE_D if e is None else (e + 1) * SUB, 256):
            r = jnp.dot(lhs, wd[cs, n : n + 256], preferred_element_type=f32)
            if c > 0:
                r = r + yacc[h, :, n : n + 256]
            if c == NC - 1:
                yp[h, :, :, :, n : n + 256] = r.astype(bf16).reshape(4, 4, R, 256)
            else:
                yacc[h, :, n : n + 256] = r

    def y_start(h, e):
        es = pl.ds(e * SUB, SUB)
        send(yp.at[h, y2, 0:2, :, es], ry1.at[h, 0, :, :, es], ("y1", h, e, 0), dev(p, x, z, yq))
        send(yp.at[h, y2, 2:4, :, es], ry1.at[h, 1, :, :, es], ("y1", h, e, 1), dev(p, x, z, ym))
        send(yp.at[h, yq, 2:4, :, es], ry2.at[h, 0, 2:4, :, es], ("y2", h, e, 0), dev(p, x, z, yq))
        send(yp.at[h, ym, 0:2, :, es], ry2.at[h, 1, 0:2, :, es], ("y2", h, e, 1), dev(p, x, z, ym))

    def y_mid(h, e):
        es = pl.ds(e * SUB, SUB)
        wait(ry1.at[h, 0, :, :, es], ("y1", h, e, 0))
        yp[h, yq, 0:2, :, es] = (
            yp[h, yq, 0:2, :, es].astype(f32) + ry1[h, 0, :, :, es].astype(f32)
        ).astype(bf16)
        send(lambda: yp.at[h, yq, 0:2, :, es], ry2.at[h, 0, 0:2, :, es], ("y2", h, e, 2), dev(p, x, z, yq))
        wait(ry1.at[h, 1, :, :, es], ("y1", h, e, 1))
        yp[h, ym, 2:4, :, es] = (
            yp[h, ym, 2:4, :, es].astype(f32) + ry1[h, 1, :, :, es].astype(f32)
        ).astype(bf16)
        send(lambda: yp.at[h, ym, 2:4, :, es], ry2.at[h, 1, 2:4, :, es], ("y2", h, e, 3), dev(p, x, z, ym))

    def y_end(h, e):
        es = pl.ds(e * SUB, SUB)
        wait(ry2.at[h, 0, 2:4, :, es], ("y2", h, e, 0))
        wait(ry2.at[h, 1, 0:2, :, es], ("y2", h, e, 1))
        wait(ry2.at[h, 0, 0:2, :, es], ("y2", h, e, 2))
        wait(ry2.at[h, 1, 2:4, :, es], ("y2", h, e, 3))
        sh[h, :, :, es] = (
            xt[h, y, :, :, es].astype(f32)
            + yp[h, y, :, :, es].astype(f32)
            + ry2[h, 0, :, :, es].astype(f32)
            + ry2[h, 1, :, :, es].astype(f32)
        ).astype(bf16)

        @when(first)
        def _():
            dst = xt.at[h, y, :, :, es]
            src = lambda: sh.at[h, :, :, es]
            send(src, dst, ("g", h, e, 0), dev(1, x, z, yq), first)
            send(src, dst, ("g", h, e, 1), dev(1, x, z, ym), first)
            send(src, dst, ("g", h, e, 2), dev(1, x, z, y), first)

        @when(second)
        def _():
            for d in (1, 3, 2):
                for xb in range(e * XB, (e + 1) * XB):
                    send(
                        lambda d=d, xb=xb: sh.at[h, zr[d], :, pl.ds(xb * BLK, BLK)],
                        xf.at[h, y, :, hcols(xb, 0)],
                        ("f", h, d, xb), dev(1, x, zr[d], y), second,
                    )
            for xb in range(e * XB, (e + 1) * XB):
                xf[h, y, :, hcols(xb, 0)] = sh[h, z, :, xb * BLK : (xb + 1) * BLK]

    FW = D // NS

    def fcols(e, part=None):
        if part is None:
            return pl.ds(e * FW, FW)
        return pl.ds(e * FW + part * (FW // 2), FW // 2)

    def finals_one(h, e):
        @when(second)
        def _():
            for d in (1, 3, 2):
                for xb in range(e * XB, (e + 1) * XB):
                    wait(xf.at[h, y, :, hcols(xb, (4 - d) % 4)], ("f", h, d, xb))
            a = lambda: xf.at[h, y, :, fcols(e)]
            send(a, a(), ("q", h, e, 0), dev(1, x, z, yq), second)
            send(a, a(), ("q", h, e, 1), dev(1, x, z, ym), second)
            send(a, a(), ("q", h, e, 4), dev(0, x, z, y), second)

    def finals_two(h, e):
        @when(second)
        def _():
            wait(xf.at[h, ym, :, fcols(e)], ("q", h, e, 0))
            a = lambda: xf.at[h, ym, :, fcols(e, 0)]
            send(a, a(), ("q", h, e, 2), dev(1, x, z, yq), second)
            wait(xf.at[h, yq, :, fcols(e)], ("q", h, e, 1))
            b = lambda: xf.at[h, yq, :, fcols(e, 1)]
            send(b, b(), ("q", h, e, 3), dev(1, x, z, ym), second)
            a2 = lambda: xf.at[h, ym, :, fcols(e)]
            send(a2, a2(), ("q", h, e, 5), dev(0, x, z, y), second)
            b2 = lambda: xf.at[h, yq, :, fcols(e)]
            send(b2, b2(), ("q", h, e, 6), dev(0, x, z, y), second)

    def finals_three(h, e):
        @when(second)
        def _():
            wait(xf.at[h, y2, :, fcols(e, 0)], ("q", h, e, 2))
            wait(xf.at[h, y2, :, fcols(e, 1)], ("q", h, e, 3))
            a = lambda: xf.at[h, y2, :, fcols(e)]
            send(a, a(), ("q", h, e, 7), dev(0, x, z, y), second)

    def finals_here(h):
        @pl.when(first)
        def _():
            for e in range(NS):
                wait(xf.at[h, y, :, fcols(e)], ("q", h, e, 4))
                wait(xf.at[h, ym, :, fcols(e)], ("q", h, e, 5))
                wait(xf.at[h, yq, :, fcols(e)], ("q", h, e, 6))
                wait(xf.at[h, y2, :, fcols(e)], ("q", h, e, 7))

    def final_norm(h, cond):
        def work():
            for q in range(4):
                v = xf[h, q].astype(f32)
                r = lax.rsqrt(jnp.mean(v * v, axis=1, keepdims=True) + epsilon)
                xn[pl.ds((h * 4 + q) * R, R), :] = (v * r * fgain[...]).astype(bf16)

        if cond is None:
            work()
        else:
            pl.when(cond)(work)

    def sent_before(count):
        batch = pending[:count]
        del pending[:count]
        for src, ssem, cond in batch:
            if cond is None:
                ref = src() if callable(src) else src
                pltpu.make_async_copy(ref, ref, sem(ssem)).wait()
        for which in (first, second):
            @pl.when(which)
            def _():
                for src, ssem, cond in batch:
                    if cond is which:
                        ref = src() if callable(src) else src
                        pltpu.make_async_copy(ref, ref, sem(ssem)).wait()

    steps = [(h, c) for c in range(NC) for h in range(2)]
    steps += [(h, c) for h in range(2, NH) for c in range(NC)]
    with jax.named_scope("local_weights"):
        ld.start()
        lw.wait()

    n = len(steps)
    slots = {}

    def prefetch(a, b):
        for k in range(a, b):
            ucopy(k).start()


    def at(slot, prio, fn, *args):
        entry = (prio, len(slots.get(slot, ())), fn, args, None)
        slots.setdefault(slot, []).append(entry)

    def at_core(core, slot, prio, fn, *args):
        entry = (prio, len(slots.get(slot, ())), fn, args, core)
        slots.setdefault(slot, []).append(entry)

    for k in range(PRE):
        at(-1, 0, weights_forward, k, second)
    at(-1, 1, near_later, 1)
    at(0, 1, tile_relay_first, 1)
    at(3, 8, ld.wait)
    at(3, 9, prefetch, 0, NSLOT)
    at(-1, 1, tile_relay, 0)
    at(1, 9, tile_relay, 1)
    for h in range(2, NH):
        at(h, 3, near_later, h)
        at(h + 2, 3, tile_relay_first, h)
        at(steps.index((h, 0)) - 1, 9, tile_relay, h)
    for k in range(2 * NC):
        at(WF_SLOT[k], 0 if k == 0 else 2, weights_forward, k, first)
    for k in range(PRE, 2 * NC):
        at(1 + 2 * (k - PRE), 2, weights_forward, k, second)
    last = {}
    for i, (h, c) in enumerate(steps):
        u = i + 1
        if h == 0:
            at(u, 2, weights_last, c)
        if c == 0:
            at(u, 2, tile_ready, h)
        at(u, 2, up_chunk, h, c)
        stage = [u + k * LAG for k in range(1, 5)]
        if h >= NH - 2:
            end = steps.index((h, NC - 1)) + 1
            cap = END[h - NH + 2]
            stage = [min(t, end + d) for t, d in zip(stage, cap)]
        at(stage[0], 3, reduce_one, h, c)
        at(stage[1], 4, reduce_two, h, c)
        at(stage[2], 5, gather_one, h, c)
        slot = max(stage[3], WF_SLOT[NC + c] + 2 + h)
        if h == 0:
            at(slot, 6, weights_last, NC + c)
        if c < NC - 1 or NS == 1:
            at(slot, 6, down_chunk, h, c)
        else:
            at(slot, 6, down_arrived, h, c)
        if c == NC - 1:
            for e in range(NS):
                if NS > 1:
                    at(slot, 7, down_chunk, h, c, e)
                at(slot, 7, y_start, h, e)
        last[h] = slot
    for h in range(NH):
        slot = last[h]
        at_core(first, slot + 1, 2.5, y_mid, h, 0)
        at_core(first, slot + 2, 2.5, y_end, h, 0)
        fns = (y_mid, y_end, finals_one, finals_two, finals_three)
        for lag, fn in zip(LAGS[h], fns):
            early = h == NH - 2 and fn is y_mid
            at_core(second, slot + lag, 5.5 if early else ORDER[h], fn, h, 0)
        if h < NH - 1:
            at(slot + LAGS[h][-1], 13, final_norm, h, second)
    share = []

    def old_sends():
        sent_before(share[0])

    end = max(slots) + 1
    for h in range(NH):
        at(end, h, finals_here, h)
        if h < NH - 1:
            at(end, h, final_norm, h, first)
        else:
            at(end, h, final_norm, h, None)
    tail = last[NH - 1]
    for slot in range(tail + 1, tail + 5):
        at(slot, 7.4, old_sends)
    for slot in sorted(slots):
        if slot == tail:
            share.append(len(pending) // 4)
        for _, _, fn, args, core in sorted(slots[slot], key=lambda e: e[:2]):
            with jax.named_scope(getattr(fn, "__name__", "copy")):
                if core is None:
                    fn(*args)
                else:
                    turn[0] = core
                    pl.when(core)(lambda: fn(*args))
                    turn[0] = None

    for d in (1, 2, 3):
        wait(cx.at[xr[(4 - d) % 4]], ("cx", d))
    cz[z] = cx[0] + cx[1] + cx[2] + cx[3]
    for d in (1, 2, 3):
        send(cz.at[z], cz.at[z], ("cz", d), dev(p, x, zr[d], y))

    vocab_index = p * 4 + y
    lanes = lax.broadcasted_iota(jnp.int32, (64, 256), 1)
    spread = (lanes % 64 == lax.broadcasted_iota(jnp.int32, (64, 256), 0)).astype(bf16)
    own_row = lax.broadcasted_iota(jnp.int32, (8, 256), 1) // 64 == lax.broadcasted_iota(
        jnp.int32, (8, 256), 0
    )

    def to_row(v):
        r = jnp.dot(v, spread, preferred_element_type=f32)
        return jnp.sum(jnp.where(own_row, r, 0.0), axis=0, keepdims=True)

    idp = jnp.concatenate([ids[...], jnp.zeros((4, 64), jnp.int32)], axis=0)
    high = to_row((idp // 256).astype(f32).astype(bf16))
    low = to_row((idp % 256).astype(f32).astype(bf16))
    id_row = (high * 256.0 + low).astype(jnp.int32) - vocab_index * V_DEV

    m_s[...] = jnp.full_like(m_s, -jnp.inf)
    s_s[...] = jnp.zeros_like(s_s)
    k_s[...] = jnp.zeros_like(k_s)

    def head(k, carry):
        slot = lax.rem(k, NSLOT)
        ucopy(k).wait()
        lt = lax.dot_general(
            ub[slot], xn[...], (((1,), (1,)), ((), ())), preferred_element_type=f32
        )
        m_old = m_s[...]
        m_new = jnp.maximum(m_old, jnp.max(lt, axis=0, keepdims=True))
        rows = lax.broadcasted_iota(jnp.int32, lt.shape, 0) + k * UROWS
        k_s[...] = k_s[...] + jnp.sum(jnp.where(rows == id_row, lt, 0.0), axis=0, keepdims=True)
        s_s[...] = s_s[...] * jnp.exp(m_old - m_new) + jnp.sum(
            jnp.exp(lt - m_new), axis=0, keepdims=True
        )
        m_s[...] = m_new

        @pl.when(k + NSLOT < NU)
        def _():
            ucopy(k + NSLOT).start()

        return carry

    with jax.named_scope("head"):
        lax.fori_loop(0, NU, head, 0)

    st[vocab_index, 0:1] = m_s[...]
    st[vocab_index, 1:2] = s_s[...]
    st[vocab_index, 2:3] = k_s[...]
    mine = st.at[vocab_index]
    for d in range(4):
        yt = yr[d]
        if d > 0:
            send(mine, mine, ("st", 0, d), dev(p, x, z, yt))
        send(mine, mine, ("st", 1, d), dev(other, x, z, yt))
    stat = jax.named_scope("stats_wait")
    stat.__enter__()
    for d in range(4):
        ys = yr[(4 - d) % 4]
        if d > 0:
            wait(st.at[p * 4 + ys], ("st", 0, d))
        wait(st.at[other * 4 + ys], ("st", 1, d))
    stat.__exit__(None, None, None)
    ms = [st[i, 0:1] for i in range(8)]
    top = ms[0]
    for i in range(1, 8):
        top = jnp.maximum(top, ms[i])
    tot = jnp.zeros_like(top)
    pick = jnp.zeros_like(top)
    for i in range(8):
        tot = tot + st[i, 1:2] * jnp.exp(ms[i] - top)
        pick = pick + st[i, 2:3]
    row = pick - top - jnp.log(tot)
    for d in (1, 2, 3):
        wait(cz.at[zr[(4 - d) % 4]], ("cz", d))
    counts = (cz[0] + cz[1] + cz[2] + cz[3])[0:4, 0:1]
    divisor = counts / 16.0
    mv = mask[...].astype(f32)
    tok = jnp.concatenate([row[:, 64 * i : 64 * i + 64] for i in range(4)], axis=0)
    policy = jnp.sum(mv * tok, axis=1, keepdims=True) / divisor
    gaps = policy - jnp.sum(mv * anchor[...], axis=1, keepdims=True) / divisor
    place = lax.broadcasted_iota(jnp.int32, (4, 1), 0)
    side = lax.broadcasted_iota(jnp.int32, (4, 64), 1)
    extra = jnp.broadcast_to(policy, (4, 64))
    for i in range(2):
        chosen = jnp.sum(jnp.where(place == pairing[0, 2 * i], gaps, 0.0))
        rejected = jnp.sum(jnp.where(place == pairing[0, 2 * i + 1], gaps, 0.0))
        diff = chosen - rejected - 0.5 / ipo_tau
        extra = jnp.where(side == i + 1, diff * diff, extra)
    out[0:4, :] = jnp.concatenate([tok, extra], axis=1)
    out[4:8, :] = jnp.zeros((4, 128), f32)

    sent_before(len(pending))


def run(hs, up, down, lgain, fgain, unemb, ids, mask, anchor, pairing):
    anyspace = pl.BlockSpec(memory_space=pltpu.HBM)
    vm = pl.BlockSpec(memory_space=pltpu.VMEM)
    sm = pl.BlockSpec(memory_space=pltpu.SMEM)
    V = pltpu.VMEM
    return pl.pallas_call(
        body,
        out_shape=(
            jax.ShapeDtypeStruct((8, 128), f32)
        ),
        in_specs=[anyspace, anyspace, anyspace, vm, vm, anyspace, vm, vm, vm, sm],
        out_specs=vm,
        scratch_shapes=[
            V((TILE_D, FF_DEV), bf16),
            V((FF_DEV, TILE_D), bf16),
            V((NH, 4, 4, R, TILE_D), bf16),
            V((NH, 4, 4, R, TILE_D), bf16),
            V((NH, 4, 4, R, FF_DEV), bf16),
            V((NH, 2, 2, R, FF_DEV), bf16),
            V((NH, 2, 4, R, FF_DEV), bf16),
            V((NH, 4, 4, R, FF_DEV), bf16),
            V((NH, 16 * R, TILE_D), f32),
            V((NH, 4, 4, R, TILE_D), bf16),
            V((NH, 2, 2, R, TILE_D), bf16),
            V((NH, 2, 4, R, TILE_D), bf16),
            V((NH, 4, R, TILE_D), bf16),
            V((NH, 4, R, D), bf16),
            V((256, D), bf16),
            V((NSLOT, UROWS, D), bf16),
            V((NH, 4, 8, 128), f32),
            V((NH, 3, 8, 128), f32),
            V((NH, 4 * R, 128), f32),
            V((8, 8, 256), f32),
            V((4, 8, 128), f32),
            V((4, 8, 128), f32),
            V((1, 256), f32),
            V((1, 256), f32),
            V((1, 256), f32),
            pltpu.SemaphoreType.DMA((NSEM,)),
            pltpu.SemaphoreType.DMA((NSLOT,)),
            pltpu.SemaphoreType.REGULAR,
        ],
        compiler_params=pltpu.CompilerParams(
            collective_id=0, has_side_effects=True, vmem_limit_bytes=66_000_000
        ),
        name="relay",
    )(hs, up, down, lgain, fgain, unemb, ids, mask, anchor, pairing)


def unpack(rows, tok, policy, losses):
    tok[...] = rows[0:4, 0:64]
    for i in range(4):
        policy[i] = rows[i, 64]
    for i in range(2):
        losses[i] = rows[0, 65 + i]


def shards(
    hidden_states, up_weight, down_weight, layer_gain, final_gain, unembedding,
    target_ids, response_masks, anchor_logps, pairing,
):
    out = run(
        hidden_states.reshape(NH, 4, R, D),
        up_weight[0],
        down_weight[0],
        layer_gain,
        final_gain.reshape(1, D),
        unembedding,
        target_ids,
        response_masks,
        anchor_logps,
        pairing,
    )
    vm = pl.BlockSpec(memory_space=pltpu.VMEM)
    sm = pl.BlockSpec(memory_space=pltpu.SMEM)
    return pl.pallas_call(
        unpack,
        out_shape=(
            jax.ShapeDtypeStruct((4, 64), f32),
            jax.ShapeDtypeStruct((4,), f32),
            jax.ShapeDtypeStruct((2,), f32),
        ),
        in_specs=[vm],
        out_specs=(vm, sm, sm),
        name="unpack",
    )(out)


def solution(mesh):
    return jax.shard_map(
        shards,
        mesh=mesh,
        in_specs=(
            P("dp", None, None),
            P("pipe", "dp", "mp"),
            P("pipe", "mp", "dp"),
            P("pipe", None),
            P(),
            P(("pipe", "mp"), None),
            P("dp", None),
            P("dp", None),
            P("dp", None),
            P("dp", None),
        ),
        out_specs=(P("dp", None), P("dp"), P("dp")),
        check_vma=False,
    )
```

```python
import jax
import jax.numpy as jnp
from jax import lax
from jax.experimental import pallas as pl
from jax.experimental.pallas import tpu as pltpu
from jax.sharding import PartitionSpec as P

epsilon = 1e-05
ipo_tau = 0.5

NX, NY, NZ = 4, 4, 4
D = 4096
FF_DEV = 1792
BLK = 256
TILE_D = 4 * BLK
NH = 4
R = 32 // (NH // 2)
AHEAD = 2
END = ((2, 3, 4, 6), (1, 2, 3, 4))
LAGS = ((2, 4, 6, 7, 8), (2, 4, 5, 6, 7), (2, 3, 4, 5, 6), (1, 2, 3, 4, 5))
ORDER = (8, 8.1, 7.9, 7.5)
WF_SLOT = (-1, 0, 2, 4, 6, 8, 10, 12)
GATE = 0
PRE = 4
CHUNKS = ((0, 384), (384, 512), (896, 512), (1408, 384))
LAG = 2
NC = len(CHUNKS)
UROWS = 1024
NSLOT = 3
V_DEV = 4096
NU = V_DEV // UROWS
NS = 1
SUB = TILE_D // NS
XB = 4 // NS
NSEM = 814

f32 = jnp.float32
bf16 = jnp.bfloat16


def body(
    hs, up, down, lgain, fgain, unemb, ids, mask, anchor, pairing,
    out,
    wu, wd, xt, xg, pp, rz1, rz2, ag, yacc, yp, ry1, ry2, sh, xf, xn, ub,
    ssb, ssr, rcol, st, cx, cz, m_s, s_s, k_s,
    sems, usem, gate,
):
    p = lax.axis_index("pipe")
    dp = lax.axis_index("dp")
    y = lax.axis_index("mp")
    x = lax.div(dp, 4)
    z = lax.rem(dp, 4)

    def wrap(v):
        return lax.rem(v + 4, 4)

    xr = [wrap(x + d) for d in range(4)]
    yr = [wrap(y + d) for d in range(4)]
    zr = [wrap(z + d) for d in range(4)]

    def dev(pi, xi, zi, yi):
        return {"pipe": pi, "dp": xi * 4 + zi, "mp": yi}

    names = {}

    def sem(key):
        if key not in names:
            assert len(names) < NSEM
            names[key] = len(names)
        return sems.at[names[key]]

    pending = []
    recorded = set()
    turn = [None]

    def when(core):
        if turn[0] is None:
            return pl.when(core)
        return (lambda fn: fn()) if turn[0] is core else (lambda fn: None)

    def send(src, dst, key, to, cond=None):
        cp = pltpu.make_async_remote_copy(
            src_ref=src() if callable(src) else src, dst_ref=dst, send_sem=sem(("s", key)), recv_sem=sem(("r", key)),
            device_id=to, device_id_type=pl.DeviceIdType.MESH,
        )
        cp.start()
        if (key, id(cond)) not in recorded:
            recorded.add((key, id(cond)))
            pending.append((src, ("s", key), cond))

    def wait(dst, key):
        pltpu.make_async_copy(dst, dst, sem(("r", key))).wait()

    xp, xm, x2 = xr[1], xr[3], xr[2]
    zp, zm, z2 = zr[1], zr[3], zr[2]
    yq, ym, y2 = yr[1], yr[3], yr[2]
    other = 1 - p
    first = p == 0
    second = p == 1

    def ucopy(k):
        slot = lax.rem(k, NSLOT)
        return pltpu.make_async_copy(
            unemb.at[pl.ds(k * UROWS, UROWS)], ub.at[slot], usem.at[slot]
        )

    xrow = pl.ds(pl.multiple_of(x * BLK, BLK), BLK)
    lw = pltpu.make_async_copy(up, wu.at[xrow, :], sem("lwu"))
    lw.start()
    ld = pltpu.make_async_copy(down, wd.at[:, xrow], sem("lwd"))

    cols_of = [
        [pl.ds(pl.multiple_of((xb * 4 + zr[d]) * BLK, BLK), BLK) for d in range(4)]
        for xb in range(4)
    ]

    def hcols(xb, d):
        return cols_of[xb][d]

    cx[...] = jnp.zeros_like(cx)
    cz[...] = jnp.zeros_like(cz)
    st[...] = jnp.zeros_like(st)
    ssb[...] = jnp.zeros_like(ssb)

    bar = pltpu.get_barrier_semaphore()
    peers = []
    for d in (1, 2, 3):
        peers.append(dev(p, xr[d], z, y))
        peers.append(dev(p, x, zr[d], y))
        peers.append(dev(p, x, z, yr[d]))
    for d in range(4):
        peers.append(dev(other, x, z, yr[d]))
    for peer in peers:
        pl.semaphore_signal(bar, inc=1, device_id=peer, device_id_type=pl.DeviceIdType.MESH)
    with jax.named_scope("barrier"):
        pl.semaphore_wait(bar, len(peers))

    items = [("u", c) for c in range(NC)] + [("d", c) for c in range(NC)]

    def own_weights(i):
        kind, c = items[i]
        o, w = CHUNKS[c]
        if kind == "u":
            src = up.at[:, pl.ds(o, w)]
            dst = wu.at[xrow, pl.ds(o, w)]
        else:
            src = down.at[pl.ds(o, w), :]
            dst = wd.at[pl.ds(o, w), xrow]
        return src, dst

    def wslice(i, xb, part=None):
        kind, c = items[i]
        o, w = CHUNKS[c]
        if kind == "u":
            n = BLK if part is None else BLK // 2
            s = xb * BLK + (0 if part is None else part * (BLK // 2))
            return wu.at[pl.ds(pl.multiple_of(s, n), n), pl.ds(o, w)]
        n = w if part is None else w // 2
        s = o + (0 if part is None else part * (w // 2))
        return wd.at[pl.ds(s, n), pl.ds(pl.multiple_of(xb * BLK, BLK), BLK)]

    def weights_own(i, cond=None):
        _, dst = own_weights(i)
        src = lambda: own_weights(i)[0]
        if cond is None:
            src = src()
        send(src, dst, ("w", i, 0), dev(p, xp, z, y), cond)
        send(src, dst, ("w", i, 1), dev(p, xm, z, y), cond)

    def weights_forward(i, cond):
        @pl.when(cond)
        def _():
            wait(wslice(i, xm), ("w", i, 0))
            a = lambda: wslice(i, xm, 0)
            send(a, a(), ("w", i, 2), dev(p, xp, z, y), cond)
            wait(wslice(i, xp), ("w", i, 1))
            b = lambda: wslice(i, xp, 1)
            send(b, b(), ("w", i, 3), dev(p, xm, z, y), cond)
            if cond is first and i == 0:
                for k in range(2, AHEAD):
                    weights_own(k, cond)
            if i + AHEAD < len(items):
                weights_own(i + AHEAD, cond)
            if cond is first and i == len(items) - 1 - GATE:
                pl.semaphore_signal(gate, inc=1, device_id=dev(1, x, z, y),
                                    device_id_type=pl.DeviceIdType.MESH)

    def weights_last(i):
        wait(wslice(i, x2, 0), ("w", i, 2))
        wait(wslice(i, x2, 1), ("w", i, 3))

    def far_tokens(h):
        for xb in range(4):
            part = slice(None) if h == 0 else y
            send(
                lambda h=h, xb=xb, part=part: hs.at[h, part, :, hcols(xb, 2)],
                xt.at[h, part, z, :, pl.ds(xb * BLK, BLK)],
                ("x", h, 2, xb), dev(0, x, z2, y), first,
            )

    def near_tokens(h):
        for d in (1, 3):
            for xb in range(4):
                send(
                    lambda h=h, d=d, xb=xb: hs.at[h, :, :, hcols(xb, d)],
                    xt.at[h, :, z, :, pl.ds(xb * BLK, BLK)],
                    ("x", h, d, xb), dev(0, x, zr[d], y), first,
                )
        for xb in range(4):
            pltpu.make_async_copy(
                hs.at[h, :, :, hcols(xb, 0)], xt.at[h, :, z, :, pl.ds(xb * BLK, BLK)],
                sem(("xl", h, xb)),
            ).start()

    def near_later(h):
        @pl.when(first)
        def _():
            near_tokens(h)

    @pl.when(first)
    def _():
        weights_own(0, first)
        weights_own(1, first)
        far_tokens(0)
        near_tokens(0)
        for h in range(1, NH):
            far_tokens(h)

    own = jnp.sum(mask[...].astype(f32), axis=1, keepdims=True)
    cx[x, 0:4, :] = jnp.broadcast_to(own, (4, 128))
    for d in (1, 2, 3):
        send(cx.at[x], cx.at[x], ("cx", d), dev(p, xr[d], z, y))

    @pl.when(second)
    def _():
        pl.semaphore_wait(gate, 1)
        for i in range(AHEAD):
            weights_own(i, second)

    gz = jnp.concatenate([lgain[:, hcols(xb, 0)] for xb in range(4)], axis=1)

    def tile_arrived(h):
        @pl.when(first)
        def _():
            for xb in range(4):
                pltpu.make_async_copy(
                    hs.at[h, :, :, hcols(xb, 0)], xt.at[h, :, z, :, pl.ds(xb * BLK, BLK)],
                    sem(("xl", h, xb)),
                ).wait()
            for d in (1, 3):
                zs = zr[(4 - d) % 4]
                for xb in range(4):
                    wait(xt.at[h, :, zs, :, pl.ds(xb * BLK, BLK)], ("x", h, d, xb))
            if h == 0:
                for xb in range(4):
                    wait(xt.at[h, :, z2, :, pl.ds(xb * BLK, BLK)], ("x", h, 2, xb))
            else:
                for d in (1, 3, 2):
                    wait(xt.at[h, yr[(4 - d) % 4], z2], ("xy", h, d))

        @pl.when(second)
        def _():
            for e in range(NS):
                es = pl.ds(e * SUB, SUB)
                wait(xt.at[h, y, :, :, es], ("g", h, e, 2))
                wait(xt.at[h, y2, 0:2, :, es], ("g", h, e, 3))
                wait(xt.at[h, y2, 2:4, :, es], ("g", h, e, 4))

    def tile_relay_first(h):
        @pl.when(first)
        def _():
            for xb in range(4):
                wait(xt.at[h, y, z2, :, pl.ds(xb * BLK, BLK)], ("x", h, 2, xb))
            a = lambda: xt.at[h, y, z2]
            for d in (1, 3, 2):
                send(a, a(), ("xy", h, d), dev(0, x, z, yr[d]), first)

    def tile_relay(h):
        @pl.when(second)
        def _():
            for e in range(NS):
                es = pl.ds(e * SUB, SUB)
                wait(xt.at[h, ym, :, :, es], ("g", h, e, 0))
                a = lambda es=es: xt.at[h, ym, 0:2, :, es]
                send(a, a(), ("g", h, e, 3), dev(1, x, z, yq), second)
                wait(xt.at[h, yq, :, :, es], ("g", h, e, 1))
                b = lambda es=es: xt.at[h, yq, 2:4, :, es]
                send(b, b(), ("g", h, e, 4), dev(1, x, z, ym), second)

    def tile_ready(h):
        tile_arrived(h)
        ones = jnp.ones((8, TILE_D), bf16)
        for g in range(4):
            v = xt[h, :, g].reshape(4 * R, TILE_D).astype(f32)
            xg[h, :, g] = (v * gz).astype(bf16).reshape(4, R, TILE_D)
            sq = v * v
            hi = sq.astype(bf16)
            lo = (sq - hi.astype(f32)).astype(bf16)
            dn = (((1,), (1,)), ((), ()))
            ssb[h, g, :, 0 : 4 * R] = lax.dot_general(
                ones, hi, dn, preferred_element_type=f32
            ) + lax.dot_general(ones, lo, dn, preferred_element_type=f32)
        for d in (1, 3, 2):
            zt = zr[d]
            send(ssb.at[h, zt], ssr.at[h, d - 1], ("ss", h, d), dev(p, x, zt, y))

    def row_scale(h):
        for d in (1, 3, 2):
            wait(ssr.at[h, d - 1], ("ss", h, d))
        total = ssb[h, z] + ssr[h, 0] + ssr[h, 1] + ssr[h, 2]
        scale = lax.rsqrt(total * (1.0 / D) + epsilon)
        col = jnp.transpose(scale, (1, 0))[0 : 4 * R, 0:1]
        rcol[h] = jnp.broadcast_to(col, (4 * R, 128))

    def up_chunk(h, c):
        o, w = CHUNKS[c]
        lhs = xg[h].reshape(16 * R, TILE_D)
        r = jnp.dot(lhs, wu[:, o : o + w], preferred_element_type=f32)
        pp[h, :, :, :, o : o + w] = r.astype(bf16).reshape(4, 4, R, w)
        cs = pl.ds(o, w)
        send(pp.at[h, 0:2, z2, :, cs], rz1.at[h, 0, :, :, cs], ("z1", h, c, 0), dev(p, x, zp, y))
        send(pp.at[h, 2:4, z2, :, cs], rz1.at[h, 1, :, :, cs], ("z1", h, c, 1), dev(p, x, zm, y))
        send(pp.at[h, 2:4, zp, :, cs], rz2.at[h, 0, 2:4, :, cs], ("z2", h, c, 0), dev(p, x, zp, y))
        send(pp.at[h, 0:2, zm, :, cs], rz2.at[h, 1, 0:2, :, cs], ("z2", h, c, 1), dev(p, x, zm, y))

    def reduce_one(h, c):
        o, w = CHUNKS[c]
        cs = pl.ds(o, w)
        wait(rz1.at[h, 0, :, :, cs], ("z1", h, c, 0))
        pp[h, 0:2, zp, :, cs] = (
            pp[h, 0:2, zp, :, cs].astype(f32) + rz1[h, 0, :, :, cs].astype(f32)
        ).astype(bf16)
        send(pp.at[h, 0:2, zp, :, cs], rz2.at[h, 0, 0:2, :, cs], ("z2", h, c, 2), dev(p, x, zp, y))
        wait(rz1.at[h, 1, :, :, cs], ("z1", h, c, 1))
        pp[h, 2:4, zm, :, cs] = (
            pp[h, 2:4, zm, :, cs].astype(f32) + rz1[h, 1, :, :, cs].astype(f32)
        ).astype(bf16)
        send(pp.at[h, 2:4, zm, :, cs], rz2.at[h, 1, 2:4, :, cs], ("z2", h, c, 3), dev(p, x, zm, y))

    def reduce_two(h, c):
        o, w = CHUNKS[c]
        cs = pl.ds(o, w)
        if c == 0:
            row_scale(h)
        wait(rz2.at[h, 0, 2:4, :, cs], ("z2", h, c, 0))
        wait(rz2.at[h, 1, 0:2, :, cs], ("z2", h, c, 1))
        wait(rz2.at[h, 0, 0:2, :, cs], ("z2", h, c, 2))
        wait(rz2.at[h, 1, 2:4, :, cs], ("z2", h, c, 3))
        s = (
            pp[h, :, z, :, cs].astype(f32)
            + rz2[h, 0, :, :, cs].astype(f32)
            + rz2[h, 1, :, :, cs].astype(f32)
        ).reshape(4 * R, w)
        v = s * rcol[h][:, 0:1]
        act = v / (1.0 + jnp.exp(-v))
        ag[h, :, z, :, cs] = act.astype(bf16).reshape(4, R, w)
        a = ag.at[h, :, z, :, cs]
        send(a, a, ("a", h, c, 0), dev(p, x, zp, y))
        send(a, a, ("a", h, c, 1), dev(p, x, zm, y))

    def gather_one(h, c):
        o, w = CHUNKS[c]
        cs = pl.ds(o, w)
        wait(ag.at[h, :, zm, :, cs], ("a", h, c, 0))
        a = ag.at[h, 0:2, zm, :, cs]
        send(a, a, ("a", h, c, 2), dev(p, x, zp, y))
        wait(ag.at[h, :, zp, :, cs], ("a", h, c, 1))
        b = ag.at[h, 2:4, zp, :, cs]
        send(b, b, ("a", h, c, 3), dev(p, x, zm, y))

    def down_arrived(h, c):
        cs = pl.ds(*CHUNKS[c])
        wait(ag.at[h, 0:2, z2, :, cs], ("a", h, c, 2))
        wait(ag.at[h, 2:4, z2, :, cs], ("a", h, c, 3))

    def down_chunk(h, c, e=None):
        o, w = CHUNKS[c]
        cs = pl.ds(o, w)
        if e is None:
            down_arrived(h, c)
        lhs = ag[h, :, :, :, cs].reshape(16 * R, w)
        for n in range(0 if e is None else e * SUB, TILE_D if e is None else (e + 1) * SUB, 256):
            r = jnp.dot(lhs, wd[cs, n : n + 256], preferred_element_type=f32)
            if c > 0:
                r = r + yacc[h, :, n : n + 256]
            if c == NC - 1:
                yp[h, :, :, :, n : n + 256] = r.astype(bf16).reshape(4, 4, R, 256)
            else:
                yacc[h, :, n : n + 256] = r

    def y_start(h, e):
        es = pl.ds(e * SUB, SUB)
        send(yp.at[h, y2, 0:2, :, es], ry1.at[h, 0, :, :, es], ("y1", h, e, 0), dev(p, x, z, yq))
        send(yp.at[h, y2, 2:4, :, es], ry1.at[h, 1, :, :, es], ("y1", h, e, 1), dev(p, x, z, ym))
        send(yp.at[h, yq, 2:4, :, es], ry2.at[h, 0, 2:4, :, es], ("y2", h, e, 0), dev(p, x, z, yq))
        send(yp.at[h, ym, 0:2, :, es], ry2.at[h, 1, 0:2, :, es], ("y2", h, e, 1), dev(p, x, z, ym))

    def y_mid(h, e):
        es = pl.ds(e * SUB, SUB)
        wait(ry1.at[h, 0, :, :, es], ("y1", h, e, 0))
        yp[h, yq, 0:2, :, es] = (
            yp[h, yq, 0:2, :, es].astype(f32) + ry1[h, 0, :, :, es].astype(f32)
        ).astype(bf16)
        send(lambda: yp.at[h, yq, 0:2, :, es], ry2.at[h, 0, 0:2, :, es], ("y2", h, e, 2), dev(p, x, z, yq))
        wait(ry1.at[h, 1, :, :, es], ("y1", h, e, 1))
        yp[h, ym, 2:4, :, es] = (
            yp[h, ym, 2:4, :, es].astype(f32) + ry1[h, 1, :, :, es].astype(f32)
        ).astype(bf16)
        send(lambda: yp.at[h, ym, 2:4, :, es], ry2.at[h, 1, 2:4, :, es], ("y2", h, e, 3), dev(p, x, z, ym))

    def y_end(h, e):
        es = pl.ds(e * SUB, SUB)
        wait(ry2.at[h, 0, 2:4, :, es], ("y2", h, e, 0))
        wait(ry2.at[h, 1, 0:2, :, es], ("y2", h, e, 1))
        wait(ry2.at[h, 0, 0:2, :, es], ("y2", h, e, 2))
        wait(ry2.at[h, 1, 2:4, :, es], ("y2", h, e, 3))
        sh[h, :, :, es] = (
            xt[h, y, :, :, es].astype(f32)
            + yp[h, y, :, :, es].astype(f32)
            + ry2[h, 0, :, :, es].astype(f32)
            + ry2[h, 1, :, :, es].astype(f32)
        ).astype(bf16)

        @when(first)
        def _():
            dst = xt.at[h, y, :, :, es]
            src = lambda: sh.at[h, :, :, es]
            send(src, dst, ("g", h, e, 0), dev(1, x, z, yq), first)
            send(src, dst, ("g", h, e, 1), dev(1, x, z, ym), first)
            send(src, dst, ("g", h, e, 2), dev(1, x, z, y), first)

        @when(second)
        def _():
            for d in (1, 3, 2):
                for xb in range(e * XB, (e + 1) * XB):
                    send(
                        lambda d=d, xb=xb: sh.at[h, zr[d], :, pl.ds(xb * BLK, BLK)],
                        xf.at[h, y, :, hcols(xb, 0)],
                        ("f", h, d, xb), dev(1, x, zr[d], y), second,
                    )
            for xb in range(e * XB, (e + 1) * XB):
                xf[h, y, :, hcols(xb, 0)] = sh[h, z, :, xb * BLK : (xb + 1) * BLK]

    FW = D // NS

    def fcols(e, part=None):
        if part is None:
            return pl.ds(e * FW, FW)
        return pl.ds(e * FW + part * (FW // 2), FW // 2)

    def finals_one(h, e):
        @when(second)
        def _():
            for d in (1, 3, 2):
                for xb in range(e * XB, (e + 1) * XB):
                    wait(xf.at[h, y, :, hcols(xb, (4 - d) % 4)], ("f", h, d, xb))
            a = lambda: xf.at[h, y, :, fcols(e)]
            send(a, a(), ("q", h, e, 0), dev(1, x, z, yq), second)
            send(a, a(), ("q", h, e, 1), dev(1, x, z, ym), second)
            send(a, a(), ("q", h, e, 4), dev(0, x, z, y), second)

    def finals_two(h, e):
        @when(second)
        def _():
            wait(xf.at[h, ym, :, fcols(e)], ("q", h, e, 0))
            a = lambda: xf.at[h, ym, :, fcols(e, 0)]
            send(a, a(), ("q", h, e, 2), dev(1, x, z, yq), second)
            wait(xf.at[h, yq, :, fcols(e)], ("q", h, e, 1))
            b = lambda: xf.at[h, yq, :, fcols(e, 1)]
            send(b, b(), ("q", h, e, 3), dev(1, x, z, ym), second)
            a2 = lambda: xf.at[h, ym, :, fcols(e)]
            send(a2, a2(), ("q", h, e, 5), dev(0, x, z, y), second)
            b2 = lambda: xf.at[h, yq, :, fcols(e)]
            send(b2, b2(), ("q", h, e, 6), dev(0, x, z, y), second)

    def finals_three(h, e):
        @when(second)
        def _():
            wait(xf.at[h, y2, :, fcols(e, 0)], ("q", h, e, 2))
            wait(xf.at[h, y2, :, fcols(e, 1)], ("q", h, e, 3))
            a = lambda: xf.at[h, y2, :, fcols(e)]
            send(a, a(), ("q", h, e, 7), dev(0, x, z, y), second)

    def finals_here(h):
        @pl.when(first)
        def _():
            for e in range(NS):
                wait(xf.at[h, y, :, fcols(e)], ("q", h, e, 4))
                wait(xf.at[h, ym, :, fcols(e)], ("q", h, e, 5))
                wait(xf.at[h, yq, :, fcols(e)], ("q", h, e, 6))
                wait(xf.at[h, y2, :, fcols(e)], ("q", h, e, 7))

    def final_norm(h, cond):
        def work():
            for q in range(4):
                v = xf[h, q].astype(f32)
                r = lax.rsqrt(jnp.mean(v * v, axis=1, keepdims=True) + epsilon)
                xn[pl.ds((h * 4 + q) * R, R), :] = (v * r * fgain[...]).astype(bf16)

        if cond is None:
            work()
        else:
            pl.when(cond)(work)

    def sent_before(count):
        batch = pending[:count]
        del pending[:count]
        for src, ssem, cond in batch:
            if cond is None:
                ref = src() if callable(src) else src
                pltpu.make_async_copy(ref, ref, sem(ssem)).wait()
        for which in (first, second):
            @pl.when(which)
            def _():
                for src, ssem, cond in batch:
                    if cond is which:
                        ref = src() if callable(src) else src
                        pltpu.make_async_copy(ref, ref, sem(ssem)).wait()

    steps = [(h, c) for c in range(NC) for h in range(2)]
    steps += [(h, c) for h in range(2, NH) for c in range(NC)]
    with jax.named_scope("local_weights"):
        ld.start()
        lw.wait()

    n = len(steps)
    slots = {}

    def prefetch(a, b):
        for k in range(a, b):
            ucopy(k).start()


    def at(slot, prio, fn, *args):
        entry = (prio, len(slots.get(slot, ())), fn, args, None)
        slots.setdefault(slot, []).append(entry)

    def at_core(core, slot, prio, fn, *args):
        entry = (prio, len(slots.get(slot, ())), fn, args, core)
        slots.setdefault(slot, []).append(entry)

    for k in range(PRE):
        at(-1, 0, weights_forward, k, second)
    at(-1, 1, near_later, 1)
    at(0, 1, tile_relay_first, 1)
    at(3, 8, ld.wait)
    at(3, 9, prefetch, 0, NSLOT)
    at(-1, 1, tile_relay, 0)
    at(1, 9, tile_relay, 1)
    for h in range(2, NH):
        at(h, 3, near_later, h)
        at(h + 2, 3, tile_relay_first, h)
        at(steps.index((h, 0)) - 1, 9, tile_relay, h)
    for k in range(2 * NC):
        at(WF_SLOT[k], 0 if k == 0 else 2, weights_forward, k, first)
    for k in range(PRE, 2 * NC):
        at(1 + 2 * (k - PRE), 2, weights_forward, k, second)
    last = {}
    for i, (h, c) in enumerate(steps):
        u = i + 1
        if h == 0:
            at(u, 2, weights_last, c)
        if c == 0:
            at(u, 2, tile_ready, h)
        at(u, 2, up_chunk, h, c)
        stage = [u + k * LAG for k in range(1, 5)]
        if h >= NH - 2:
            end = steps.index((h, NC - 1)) + 1
            cap = END[h - NH + 2]
            stage = [min(t, end + d) for t, d in zip(stage, cap)]
        at(stage[0], 3, reduce_one, h, c)
        at(stage[1], 4, reduce_two, h, c)
        at(stage[2], 5, gather_one, h, c)
        slot = max(stage[3], WF_SLOT[NC + c] + 2 + h)
        if h == 0:
            at(slot, 6, weights_last, NC + c)
        if c < NC - 1 or NS == 1:
            at(slot, 6, down_chunk, h, c)
        else:
            at(slot, 6, down_arrived, h, c)
        if c == NC - 1:
            for e in range(NS):
                if NS > 1:
                    at(slot, 7, down_chunk, h, c, e)
                at(slot, 7, y_start, h, e)
        last[h] = slot
    for h in range(NH):
        slot = last[h]
        at_core(first, slot + 1, 2.5, y_mid, h, 0)
        at_core(first, slot + 2, 2.5, y_end, h, 0)
        fns = (y_mid, y_end, finals_one, finals_two, finals_three)
        for lag, fn in zip(LAGS[h], fns):
            early = h == NH - 2 and fn is y_mid
            at_core(second, slot + lag, 5.5 if early else ORDER[h], fn, h, 0)
        if h < NH - 1:
            at(slot + LAGS[h][-1], 13, final_norm, h, second)
    share = []

    def old_sends():
        sent_before(share[0])

    end = max(slots) + 1
    for h in range(NH):
        at(end, h, finals_here, h)
        if h < NH - 1:
            at(end, h, final_norm, h, first)
        else:
            at(end, h, final_norm, h, None)
    tail = last[NH - 1]
    for slot in range(tail + 1, tail + 5):
        at(slot, 7.4, old_sends)
    for slot in sorted(slots):
        if slot == tail:
            share.append(len(pending) // 4)
        for _, _, fn, args, core in sorted(slots[slot], key=lambda e: e[:2]):
            with jax.named_scope(getattr(fn, "__name__", "copy")):
                if core is None:
                    fn(*args)
                else:
                    turn[0] = core
                    pl.when(core)(lambda: fn(*args))
                    turn[0] = None

    for d in (1, 2, 3):
        wait(cx.at[xr[(4 - d) % 4]], ("cx", d))
    cz[z] = cx[0] + cx[1] + cx[2] + cx[3]
    for d in (1, 2, 3):
        send(cz.at[z], cz.at[z], ("cz", d), dev(p, x, zr[d], y))

    vocab_index = p * 4 + y
    lanes = lax.broadcasted_iota(jnp.int32, (64, 256), 1)
    spread = (lanes % 64 == lax.broadcasted_iota(jnp.int32, (64, 256), 0)).astype(bf16)
    own_row = lax.broadcasted_iota(jnp.int32, (8, 256), 1) // 64 == lax.broadcasted_iota(
        jnp.int32, (8, 256), 0
    )

    def to_row(v):
        r = jnp.dot(v, spread, preferred_element_type=f32)
        return jnp.sum(jnp.where(own_row, r, 0.0), axis=0, keepdims=True)

    idp = jnp.concatenate([ids[...], jnp.zeros((4, 64), jnp.int32)], axis=0)
    high = to_row((idp // 256).astype(f32).astype(bf16))
    low = to_row((idp % 256).astype(f32).astype(bf16))
    id_row = (high * 256.0 + low).astype(jnp.int32) - vocab_index * V_DEV

    m_s[...] = jnp.full_like(m_s, -jnp.inf)
    s_s[...] = jnp.zeros_like(s_s)
    k_s[...] = jnp.zeros_like(k_s)

    def head(k, carry):
        slot = lax.rem(k, NSLOT)
        ucopy(k).wait()
        lt = lax.dot_general(
            ub[slot], xn[...], (((1,), (1,)), ((), ())), preferred_element_type=f32
        )
        m_old = m_s[...]
        m_new = jnp.maximum(m_old, jnp.max(lt, axis=0, keepdims=True))
        rows = lax.broadcasted_iota(jnp.int32, lt.shape, 0) + k * UROWS
        k_s[...] = k_s[...] + jnp.sum(jnp.where(rows == id_row, lt, 0.0), axis=0, keepdims=True)
        s_s[...] = s_s[...] * jnp.exp(m_old - m_new) + jnp.sum(
            jnp.exp(lt - m_new), axis=0, keepdims=True
        )
        m_s[...] = m_new

        @pl.when(k + NSLOT < NU)
        def _():
            ucopy(k + NSLOT).start()

        return carry

    with jax.named_scope("head"):
        lax.fori_loop(0, NU, head, 0)

    st[vocab_index, 0:1] = m_s[...]
    st[vocab_index, 1:2] = s_s[...]
    st[vocab_index, 2:3] = k_s[...]
    mine = st.at[vocab_index]
    for d in range(4):
        yt = yr[d]
        if d > 0:
            send(mine, mine, ("st", 0, d), dev(p, x, z, yt))
        send(mine, mine, ("st", 1, d), dev(other, x, z, yt))
    stat = jax.named_scope("stats_wait")
    stat.__enter__()
    for d in range(4):
        ys = yr[(4 - d) % 4]
        if d > 0:
            wait(st.at[p * 4 + ys], ("st", 0, d))
        wait(st.at[other * 4 + ys], ("st", 1, d))
    stat.__exit__(None, None, None)
    ms = [st[i, 0:1] for i in range(8)]
    top = ms[0]
    for i in range(1, 8):
        top = jnp.maximum(top, ms[i])
    tot = jnp.zeros_like(top)
    pick = jnp.zeros_like(top)
    for i in range(8):
        tot = tot + st[i, 1:2] * jnp.exp(ms[i] - top)
        pick = pick + st[i, 2:3]
    row = pick - top - jnp.log(tot)
    for d in (1, 2, 3):
        wait(cz.at[zr[(4 - d) % 4]], ("cz", d))
    counts = (cz[0] + cz[1] + cz[2] + cz[3])[0:4, 0:1]
    divisor = counts / 16.0
    mv = mask[...].astype(f32)
    tok = jnp.concatenate([row[:, 64 * i : 64 * i + 64] for i in range(4)], axis=0)
    policy = jnp.sum(mv * tok, axis=1, keepdims=True) / divisor
    gaps = policy - jnp.sum(mv * anchor[...], axis=1, keepdims=True) / divisor
    place = lax.broadcasted_iota(jnp.int32, (4, 1), 0)
    side = lax.broadcasted_iota(jnp.int32, (4, 64), 1)
    extra = jnp.broadcast_to(policy, (4, 64))
    for i in range(2):
        chosen = jnp.sum(jnp.where(place == pairing[0, 2 * i], gaps, 0.0))
        rejected = jnp.sum(jnp.where(place == pairing[0, 2 * i + 1], gaps, 0.0))
        diff = chosen - rejected - 0.5 / ipo_tau
        extra = jnp.where(side == i + 1, diff * diff, extra)
    out[0:4, :] = jnp.concatenate([tok, extra], axis=1)
    out[4:8, :] = jnp.zeros((4, 128), f32)

    sent_before(len(pending))


def run(hs, up, down, lgain, fgain, unemb, ids, mask, anchor, pairing):
    anyspace = pl.BlockSpec(memory_space=pltpu.HBM)
    vm = pl.BlockSpec(memory_space=pltpu.VMEM)
    sm = pl.BlockSpec(memory_space=pltpu.SMEM)
    V = pltpu.VMEM
    return pl.pallas_call(
        body,
        out_shape=(
            jax.ShapeDtypeStruct((8, 128), f32)
        ),
        in_specs=[anyspace, anyspace, anyspace, vm, vm, anyspace, vm, vm, vm, sm],
        out_specs=vm,
        scratch_shapes=[
            V((TILE_D, FF_DEV), bf16),
            V((FF_DEV, TILE_D), bf16),
            V((NH, 4, 4, R, TILE_D), bf16),
            V((NH, 4, 4, R, TILE_D), bf16),
            V((NH, 4, 4, R, FF_DEV), bf16),
            V((NH, 2, 2, R, FF_DEV), bf16),
            V((NH, 2, 4, R, FF_DEV), bf16),
            V((NH, 4, 4, R, FF_DEV), bf16),
            V((NH, 16 * R, TILE_D), f32),
            V((NH, 4, 4, R, TILE_D), bf16),
            V((NH, 2, 2, R, TILE_D), bf16),
            V((NH, 2, 4, R, TILE_D), bf16),
            V((NH, 4, R, TILE_D), bf16),
            V((NH, 4, R, D), bf16),
            V((256, D), bf16),
            V((NSLOT, UROWS, D), bf16),
            V((NH, 4, 8, 128), f32),
            V((NH, 3, 8, 128), f32),
            V((NH, 4 * R, 128), f32),
            V((8, 8, 256), f32),
            V((4, 8, 128), f32),
            V((4, 8, 128), f32),
            V((1, 256), f32),
            V((1, 256), f32),
            V((1, 256), f32),
            pltpu.SemaphoreType.DMA((NSEM,)),
            pltpu.SemaphoreType.DMA((NSLOT,)),
            pltpu.SemaphoreType.REGULAR,
        ],
        compiler_params=pltpu.CompilerParams(
            collective_id=0, has_side_effects=True, vmem_limit_bytes=66_000_000
        ),
        name="relay",
    )(hs, up, down, lgain, fgain, unemb, ids, mask, anchor, pairing)


def unpack(rows, tok, policy, losses):
    tok[...] = rows[0:4, 0:64]
    for i in range(4):
        policy[i] = rows[i, 64]
    for i in range(2):
        losses[i] = rows[0, 65 + i]


def shards(
    hidden_states, up_weight, down_weight, layer_gain, final_gain, unembedding,
    target_ids, response_masks, anchor_logps, pairing,
):
    out = run(
        hidden_states.reshape(NH, 4, R, D),
        up_weight[0],
        down_weight[0],
        layer_gain,
        final_gain.reshape(1, D),
        unembedding,
        target_ids,
        response_masks,
        anchor_logps,
        pairing,
    )
    vm = pl.BlockSpec(memory_space=pltpu.VMEM)
    sm = pl.BlockSpec(memory_space=pltpu.SMEM)
    return pl.pallas_call(
        unpack,
        out_shape=(
            jax.ShapeDtypeStruct((4, 64), f32),
            jax.ShapeDtypeStruct((4,), f32),
            jax.ShapeDtypeStruct((2,), f32),
        ),
        in_specs=[vm],
        out_specs=(vm, sm, sm),
        name="unpack",
    )(out)


def solution(mesh):
    return jax.shard_map(
        shards,
        mesh=mesh,
        in_specs=(
            P("dp", None, None),
            P("pipe", "dp", "mp"),
            P("pipe", "mp", "dp"),
            P("pipe", None),
            P(),
            P(("pipe", "mp"), None),
            P("dp", None),
            P("dp", None),
            P("dp", None),
            P("dp", None),
        ),
        out_specs=(P("dp", None), P("dp"), P("dp")),
        check_vma=False,
    )
```
